32 devices in a mesh: tp: 4 (over z), ep: 8 (over y, x, core).
Axes of the slice: x: 2, y: 2, z: 4, core: 2. Of those that a mesh axis runs over, the one named last changes fastest.
Arguments:
- tokens: bfloat16 [3072, 2048], P('ep', 'tp'), may hold values from -6 to 6
- norm_gain: float32 [2048], replicated, may hold values from 0.25 to 1.75
- shared_gate: bfloat16 [2048, 2816], P('ep', 'tp'), may hold values from -0.125 to 0.125
- shared_up: bfloat16 [2048, 2816], P('ep', 'tp'), may hold values from -0.125 to 0.125
- shared_down: bfloat16 [2816, 2048], P('tp', 'ep'), may hold values from -0.15625 to 0.15625
- expert_gate: bfloat16 [4, 8, 704, 2048], P('tp', 'ep'), may hold values from -0.125 to 0.125
- expert_up: bfloat16 [4, 8, 704, 2048], P('tp', 'ep'), may hold values from -0.125 to 0.125
- expert_down: bfloat16 [16, 1408, 2048], P('ep', None, 'tp'), may hold values from -0.15625 to 0.15625
- chosen: int32 [16, 384], P('ep'), may hold values from 0 to 3071, as said below
- gates: float32 [16, 384], P('ep'), may hold values from 0.1 to 1
Outputs:
- mixed: bfloat16 [3072, 2048], P('ep', 'tp')
The draws below stay inside these ranges and needn't reach their ends.
Inputs may be any that keep to these rules, and one draw needn't show every extreme that they name: Each row of chosen holds 384 different token indices in rising order. Of one row, at most 96 lie among the 384 tokens of one index of ep (tokens s * 384 to (s + 1) * 384 - 1), and in every row exactly 96 lie among those of some index.
All inputs are finite; a program needn't handle non-finite values.
Results may differ from the reference program's by a relative error of at most 0.012.
Values may be sent and summed in bfloat16 or wider, within the bound.
A program may use at most 64 MiB of HBM per device.

```python
import jax
import jax.numpy as jnp
from jax import lax

D = 2048
FS = 2816
F = 1408
EXP_DEV = 2
TOK_DEV = 384
TOKENS = 3072
EXPERTS = 16
SPLIT = 2
CAP = 384
N_TP = 4
N_EP = 8


def expert_choices(expert_key):
    key_pair, key_shift, key_rank = jax.random.split(expert_key, 3)
    halves = N_EP // 2
    average = CAP // N_EP
    pairing = jax.random.permutation(key_pair, N_EP)
    shifts = jax.random.randint(key_shift, (halves,), 0, average + 1).astype(jnp.int32)
    shifts = shifts.at[0].set(average)
    counts = jnp.full((N_EP,), average, jnp.int32)
    counts = counts.at[pairing[:halves]].add(shifts).at[pairing[halves:]].add(-shifts)
    rank_keys = jax.random.split(key_rank, N_EP)
    rankings = jax.vmap(source_ranking)(rank_keys)
    flags = (rankings < counts[:, None]).reshape(-1).astype(jnp.int32)
    places = jnp.cumsum(flags) - 1
    places = jnp.where(flags > 0, places, CAP)
    token_ids = jnp.arange(N_EP * TOK_DEV, dtype=jnp.int32)
    return jnp.zeros((CAP,), jnp.int32).at[places].set(token_ids, mode='drop')


def source_ranking(rank_key):
    return jax.random.permutation(rank_key, TOK_DEV).astype(jnp.int32)


def draw_chosen(key, part):
    expert_keys = jax.random.split(jax.random.fold_in(key, 11), EXPERTS)
    return jax.vmap(expert_choices)(expert_keys)


def strengthened(array, own_key, source, target, shards_of, factor):
    owner, partner = [(jnp.arange(array.shape[position]) // (array.shape[position] // shards_of)).reshape([-1 if axis == position else 1 for axis in range(array.ndim)]) for position in (source, target)]
    chosen = jax.random.permutation(own_key, shards_of)[partner]
    strong = (owner == chosen) | (owner == (partner + shards_of // 2) % shards_of)
    return jnp.where(strong, factor * array, array)


def levels(stream_key, dims, cuts, low, top_value):
    def one(axis_at, shards_of):
        draws = jax.random.uniform(jax.random.fold_in(jax.random.fold_in(stream_key, 6), axis_at), (shards_of,), jnp.float32, low / len(cuts), top_value / len(cuts))
        return jnp.repeat(jnp.exp(draws), dims[axis_at] // shards_of).reshape((-1,) + (1,) * (len(dims) - axis_at - 1))

    level = one(*cuts[0])
    for cut in cuts[1:]:
        level = level * one(*cut)
    return level


def normal_values(key, shape, scale, most, cuts=(), held_as=jnp.bfloat16):
    entries = jax.random.normal(key, shape, jnp.float32) * scale
    if len(cuts) > 0:
        entries = levels(key, shape, cuts, -0.22, 0.18) * entries
    return jnp.clip(entries, min=-most, max=most).astype(held_as)


def bell_draw_with(own_key, extent, scale, reach, cuts, heavy, held_as=jnp.bfloat16):
    entries = scale * jax.random.normal(own_key, extent, jnp.float32)
    if cuts:
        entries = entries * levels(own_key, extent, cuts, -0.22, 0.18)
    return jnp.clip(strengthened(entries, jax.random.fold_in(own_key, 3), *heavy), -reach, reach).astype(held_as)


def setup_inputs(seed: int = 0) -> dict:
    key_list = jax.random.split(jax.random.key(seed), 11)
    tokens = normal_values(key_list[0], (TOKENS, D), 1.0, 6.0, ((0, 8), (1, 4)))
    norm_gain = jnp.clip(1.0 + 0.15 * jax.random.normal(key_list[1], (D,), jnp.float32), 0.25, 1.75)
    shared_gate = normal_values(key_list[2], (D, FS), D ** -0.5, 0.125, ((0, 8), (1, 4)))
    shared_up = normal_values(key_list[3], (D, FS), D ** -0.5, 0.125, ((0, 8), (1, 4)))
    shared_down = bell_draw_with(key_list[4], (FS, D), FS ** -0.5, 0.15625, ((0, 4), (1, 8)), (0, 1, 8, 2.0))
    expert_gate = normal_values(key_list[5], (N_TP, N_EP, F // SPLIT, D), D ** -0.5, 0.125, ((0, 4), (1, 8)))
    expert_up = normal_values(key_list[6], (N_TP, N_EP, F // SPLIT, D), D ** -0.5, 0.125, ((0, 4), (1, 8)))
    expert_down = normal_values(key_list[7], (EXPERTS, F, D), F ** -0.5, 0.15625, ((0, 8), (2, 4)))
    chosen = draw_chosen(jax.random.fold_in(key_list[10], 71), 0)
    gates = jnp.clip(0.1 + 0.9 * jax.random.uniform(key_list[9], (EXPERTS, CAP), jnp.float32) ** levels(key_list[9], (EXPERTS, CAP), ((0, 8),), -0.2, 0.2), 0.1, 1.0)
    return dict(tokens=tokens, norm_gain=norm_gain, shared_gate=shared_gate, shared_up=shared_up, shared_down=shared_down, expert_gate=expert_gate, expert_up=expert_up, expert_down=expert_down, chosen=chosen, gates=gates)


norm_eps = 1e-06

def reference(tokens, norm_gain, shared_gate, shared_up, shared_down, expert_gate, expert_up, expert_down, chosen, gates):
    widened = tokens.astype(jnp.float32)
    inv_scale = lax.rsqrt(lax.optimization_barrier(jnp.mean(widened * widened, axis=1, keepdims=True)) + norm_eps)
    normed = (widened * inv_scale * norm_gain.astype(jnp.float32)).astype(jnp.bfloat16)
    gate_sum = jnp.dot(normed, shared_gate, preferred_element_type=jnp.float32)
    up_sum = jnp.dot(normed, shared_up, preferred_element_type=jnp.float32)
    shared_hidden = (jax.nn.silu(gate_sum) * up_sum).astype(jnp.bfloat16)
    shared_out = jnp.dot(shared_hidden, shared_down, preferred_element_type=jnp.float32)
    split_count = N_TP // EXP_DEV

    def expert_term(expert_index):
        ep_column = (expert_index // EXP_DEV).astype(jnp.int32)
        expert_slot = (expert_index % EXP_DEV).astype(jnp.int32)

        def weight_of(weights):
            picked = lax.dynamic_index_in_dim(weights, ep_column, 1, keepdims=False)
            picked = lax.dynamic_slice_in_dim(picked, expert_slot * split_count, split_count, 0)
            return jnp.transpose(picked.reshape(F, D))
        token_ids = lax.dynamic_index_in_dim(chosen, expert_index, 0, keepdims=False)
        token_rows = jnp.take(normed, token_ids, axis=0)
        gate_values = jnp.dot(token_rows, weight_of(expert_gate), preferred_element_type=jnp.float32)
        up_values = jnp.dot(token_rows, weight_of(expert_up), preferred_element_type=jnp.float32)
        hidden = (jax.nn.silu(gate_values) * up_values).astype(jnp.bfloat16)
        down_weight = lax.dynamic_index_in_dim(expert_down, expert_index, 0, keepdims=False)
        outputs = jnp.dot(hidden, down_weight, preferred_element_type=jnp.float32)
        gate_row = lax.dynamic_index_in_dim(gates, expert_index, 0, keepdims=False).astype(jnp.float32)
        return (gate_row[:, None] * outputs).astype(jnp.bfloat16)
    weighted = lax.map(expert_term, jnp.arange(EXPERTS, dtype=jnp.int32))
    routed = jnp.zeros((TOKENS, D), jnp.float32).at[chosen.reshape(-1)].add(weighted.reshape(-1, D).astype(jnp.float32))
    return (shared_out + routed).astype(jnp.bfloat16)
```

```python
import functools

import jax
import jax.numpy as jnp
from jax import lax
from jax.experimental import pallas as pl
from jax.experimental.pallas import tpu as pltpu
from jax.sharding import PartitionSpec as P

norm_eps = 1e-06
MESH = pl.DeviceIdType.MESH


def flip(index, mask):
    bit = 1
    result = index
    while bit <= mask:
        if mask & bit:
            result = result + bit - 2 * bit * ((index // bit) % 2)
        bit *= 2
    return result


def bits_below(count):
    return [1 << i for i in range(count.bit_length() - 1)]


def half_orders(count):
    bits = bits_below(count)
    upper = bits[1:]
    return [upper + bits[:1], upper[::-1] + bits[:1]]


def later_hops(mask, order):
    last = max([i for i, b in enumerate(order) if mask & b], default=-1)
    return order[last + 1 :]


def masks_by_level(count):
    return sorted(range(1, count), key=lambda m: (bin(m).count("1"), -m))


def levels(count):
    found = {}
    for m in masks_by_level(count):
        found.setdefault(bin(m).count("1"), []).append(m)
    return [found[k] for k in sorted(found)]


def column_of(row, count):
    same = lax.broadcasted_iota(jnp.int32, (count, count), 0) == lax.broadcasted_iota(
        jnp.int32, (count, count), 1
    )
    return jnp.sum(jnp.where(same, row, 0.0), axis=1, keepdims=True)


def normalise(rows, gain):
    widened = rows.astype(jnp.float32)
    inv_scale = lax.rsqrt(jnp.mean(widened * widened, axis=1, keepdims=True) + norm_eps)
    return (widened * inv_scale * gain).astype(jnp.bfloat16)


def layer_kernel(
    n_tp,
    n_ep,
    slot_most,
    tok_hbm,
    gain_ref,
    sg_hbm,
    su_hbm,
    sd_hbm,
    eg_hbm,
    eu_hbm,
    down_hbm,
    chosen_ref,
    gates_ref,
    out_ref,
    tok_all,
    own_rows,
    used_rows,
    sel,
    sg_in,
    su_in,
    sd_in,
    eg_ref,
    eu_ref,
    down_ref,
    hidden,
    acc,
    parts,
    in_up,
    in_down,
    stage,
    back,
    picker,
    ids_out,
    ids_in,
    chosen_col,
    gates_col,
    place_row,
    ep_send,
    ep_recv,
    tp_send,
    tp_recv,
    disp_send,
    disp_recv,
    hid_send,
    hid_recv,
    up_send,
    up_recv,
    down_send,
    down_recv,
    ret_send,
    ret_recv,
    ids_send_sem,
    ids_recv_sem,
    local_sem,
    *flat,
):
    tp = lax.axis_index("tp")
    ep = lax.axis_index("ep")
    f32, bf16, i32 = jnp.float32, jnp.bfloat16, jnp.int32
    n_exp, cap = chosen_ref.shape
    n_tok, width = tok_hbm.shape
    n_hid = eg_ref.shape[0]
    slot_pad = back.shape[2]
    split = n_tp // n_exp
    slot = tp // split
    orders = half_orders(n_ep)
    high_masks = [k * split for k in range(1, n_exp)]
    tp_order = bits_below(n_tp)[::-1]
    ep_levels = levels(n_ep)
    cut = max(128, cap * 2 // 3 // 128 * 128)
    chunks = [(0, cut), (cut, cap - cut)]
    parts_of = range(len(chunks))

    own_loads = [
        (tok_hbm, tok_all.at[ep]),
        (sg_hbm, sg_in),
        (su_hbm, su_in),
        (sd_hbm, sd_in),
    ]

    def block_of(out, block, rows):
        if len(out.shape) == 3:
            return out.at[block, rows, :]
        cols = out.shape[1] // n_ep
        return out.at[rows, pl.ds(pl.multiple_of(block * cols, cols), cols)]

    def columns(ref, block):
        return ref.at[:, pl.ds(pl.multiple_of(block * width, width), width)]

    loads = []
    for i, (source, target) in enumerate(own_loads):
        if i > 0:
            target = block_of(target, ep, pl.ds(0, source.shape[0]))
        loads.append(pltpu.make_async_copy(source, target, local_sem.at[i]))
    loads.append(pltpu.make_async_copy(tok_hbm, columns(own_rows, tp), local_sem.at[4]))
    for i, (source, target) in enumerate(((eg_hbm, eg_ref), (eu_hbm, eu_ref), (down_hbm, down_ref))):
        loads.append(pltpu.make_async_copy(source, target, local_sem.at[5 + i]))
    for load in loads:
        load.start()

    barrier = pltpu.get_barrier_semaphore()
    for mask in range(1, n_tp):
        pl.semaphore_signal(barrier, inc=1, device_id={"tp": flip(tp, mask)}, device_id_type=MESH)
    for mask in range(1, n_ep):
        pl.semaphore_signal(barrier, inc=1, device_id={"ep": flip(ep, mask)}, device_id_type=MESH)
    back[...] = jnp.zeros_like(back)
    ids_out[...] = jnp.zeros_like(ids_out)
    acc[...] = jnp.zeros_like(acc)
    pl.semaphore_wait(barrier, n_tp + n_ep - 2)

    def piece(w, block, h):
        half = own_loads[w][0].shape[0] // 2
        rows = pl.ds(h * half, half)
        if w == 0:
            return tok_all.at[block, rows, :]
        return block_of([None, sg_in, su_in, sd_in][w], block, rows)

    def remote(source, target, send, recv, axis, place):
        return pltpu.make_async_remote_copy(
            src_ref=source,
            dst_ref=target,
            send_sem=send,
            recv_sem=recv,
            device_id={axis: place},
            device_id_type=MESH,
        )

    def ep_copy(w, h, mask, hop):
        ref = piece(w, flip(ep, mask), h)
        sem = (w, h, mask | hop)
        return remote(ref, ref, ep_send.at[sem], ep_recv.at[sem], "ep", flip(ep, hop))

    def ep_wait(w, h, mask):
        hop = [b for b in orders[h] if mask & b][-1]
        ref = piece(w, flip(ep, mask), h)
        sem = (w, h, mask)
        remote(ref, ref, ep_send.at[sem], ep_recv.at[sem], "ep", flip(ep, hop)).wait_recv()

    def ep_start(w):
        for position in range(len(orders[0])):
            for h in (0, 1):
                ep_copy(w, h, 0, orders[h][position]).start()

    def ep_level(w, masks):
        for mask in masks:
            for h in (0, 1):
                ep_wait(w, h, mask)
                for hop in later_hops(mask, orders[h]):
                    ep_copy(w, h, mask, hop).start()

    def tp_copy(mask, hop):
        ref = columns(own_rows, flip(tp, mask))
        source = tok_all.at[ep] if mask == 0 else ref
        sem = mask | hop
        return remote(source, ref, tp_send.at[sem], tp_recv.at[sem], "tp", flip(tp, hop))

    def tp_wait(mask):
        ref = columns(own_rows, flip(tp, mask))
        remote(ref, ref, tp_send.at[mask], tp_recv.at[mask], "tp", flip(tp, mask)).wait_recv()

    def used_piece(mask, h):
        cols = pl.ds(pl.multiple_of(flip(tp, mask) * width, width), width)
        return used_rows.at[pl.ds(*chunks[h]), cols]

    def disp_copy(mask, hop, h):
        source = used_piece(mask, h)
        if mask == 0:
            source = sel.at[flip(tp, hop) // split, pl.ds(*chunks[h]), :]
        sem = (mask | hop, h)
        return remote(
            source, used_piece(mask, h), disp_send.at[sem], disp_recv.at[sem], "tp", flip(tp, hop)
        )

    def disp_wait(mask, h):
        ref = used_piece(mask, h)
        sem = (mask, h)
        remote(ref, ref, disp_send.at[sem], disp_recv.at[sem], "tp", flip(tp, mask)).wait_recv()

    def low_hops(mask):
        return [b for b in bits_below(split) if b > mask % split]

    def hid_copy(mask, hop, h):
        ref = hidden.at[flip(tp, mask), :, pl.ds(*chunks[h])]
        sem = (mask | hop, h)
        return remote(ref, ref, hid_send.at[sem], hid_recv.at[sem], "tp", flip(tp, hop))

    def hid_wait(mask, h):
        ref = hidden.at[flip(tp, mask), :, pl.ds(*chunks[h])]
        sem = (mask, h)
        remote(ref, ref, hid_send.at[sem], hid_recv.at[sem], "tp", flip(tp, mask)).wait_recv()

    def up_copy(d):
        return remote(parts.at[d], in_up.at[d], up_send.at[d], up_recv.at[d], "tp", tp + 1)

    def down_copy(d):
        return remote(parts.at[d], in_down.at[d], down_send.at[d], down_recv.at[d], "tp", tp - 1)

    def up_wait(d):
        ref = in_up.at[d]
        remote(ref, ref, up_send.at[d], up_recv.at[d], "tp", tp - 1).wait_recv()

    def down_wait(d):
        ref = in_down.at[d]
        remote(ref, ref, down_send.at[d], down_recv.at[d], "tp", tp + 1).wait_recv()

    def ret_slot(k):
        return flip(tp, k * split) // split

    def ret_copy(mask, k):
        rows = pl.ds(0, slot_most)
        return remote(
            stage.at[k, flip(ep, mask)],
            back.at[k, ep, rows, :],
            ret_send.at[mask, k],
            ret_recv.at[mask, k],
            "ep",
            flip(ep, mask),
        )

    def ret_wait(mask, k):
        ref = back.at[k, flip(ep, mask), pl.ds(0, slot_most), :]
        sem = (mask, k)
        remote(ref, ref, ret_send.at[sem], ret_recv.at[sem], "ep", flip(ep, mask)).wait_recv()

    def ids_copy(mask):
        return remote(
            ids_out.at[flip(ep, mask)],
            ids_in.at[ep],
            ids_send_sem.at[mask],
            ids_recv_sem.at[mask],
            "ep",
            flip(ep, mask),
        )

    def ids_wait(mask):
        ref = ids_in.at[flip(ep, mask)]
        remote(
            ref, ref, ids_send_sem.at[mask], ids_recv_sem.at[mask], "ep", flip(ep, mask)
        ).wait_recv()

    loads[0].wait()
    ep_start(0)
    for hop in tp_order:
        tp_copy(0, hop).start()

    for s in range(n_exp):
        row = chosen_ref[pl.ds(s, 1), :]
        col = column_of(row.astype(f32), cap).astype(i32)
        chosen_col[s] = col
        gates_col[s] = column_of(gates_ref[pl.ds(s, 1), :], cap)
        row_from = jnp.zeros_like(row)
        col_from = jnp.zeros_like(col)
        for d in range(1, n_ep):
            row_from += jnp.where(row >= d * n_tok, 1, 0)
            col_from += jnp.where(col >= d * n_tok, 1, 0)
        ahead = jnp.where(col < row_from * n_tok, 1.0, 0.0)
        run_row = jnp.sum(ahead, axis=0, keepdims=True).astype(i32)
        ahead = jnp.where(row < col_from * n_tok, 1.0, 0.0)
        run_col = jnp.sum(ahead, axis=1, keepdims=True).astype(i32)
        lanes = lax.broadcasted_iota(i32, (1, cap), 1)
        rows = lax.broadcasted_iota(i32, (cap, 1), 0)
        place_row[s] = row_from * slot_most + lanes - run_row
        within = rows - run_col

        def slot_ids(d, carry):
            slots = lax.broadcasted_iota(i32, (cap, slot_pad), 1)
            wanted = jnp.where(col_from == d, within, -1)
            value = (col - d * n_tok + 1).astype(f32)
            total = jnp.sum(jnp.where(slots == wanted, value, 0.0), axis=0, keepdims=True)
            ids_out[d, pl.ds(s, 1), :] = total.astype(i32) - 1
            return carry

        lax.fori_loop(0, n_ep, slot_ids, 0)

    def select(e):
        def one(s, carry):
            ids = lax.broadcasted_iota(i32, (cap, n_tok), 1) + e * n_tok
            hits = jnp.where(chosen_col[s] == ids, 1.0, 0.0).astype(bf16)
            acc[s] += jnp.dot(hits, tok_all[e], preferred_element_type=f32)
            return carry

        lax.fori_loop(0, n_exp, one, 0)

    select(ep)
    ep_level(0, ep_levels[0])
    for load in loads[1:4]:
        load.wait()
    for w in (1, 2, 3):
        ep_start(w)
    ep_masks = sorted(range(1, n_ep), key=lambda m: -bin(m >> 1).count("1"))
    for mask in ep_masks:
        ids_copy(mask).start()
    ids_in[ep] = ids_out[ep]
    for mask in ep_levels[0]:
        select(flip(ep, mask))
    for masks in ep_levels[1:]:
        ep_level(0, masks)
        for mask in masks:
            select(flip(ep, mask))
    for s in range(n_exp):
        sel[s] = acc[s].astype(bf16)
    for h in parts_of:
        for hop in high_masks + low_hops(0):
            disp_copy(0, hop, h).start()
    own_used = pltpu.make_async_copy(sel.at[slot], columns(used_rows, tp), local_sem.at[8])
    own_used.start()
    acc[...] = jnp.zeros_like(acc)

    ep_level(1, ep_levels[0])
    for mask in high_masks:
        for h in parts_of:
            disp_wait(mask, h)
            for hop in low_hops(mask):
                disp_copy(mask, hop, h).start()
    ep_level(2, ep_levels[0])
    tp_rank = sorted(
        range(1, n_tp), key=lambda m: [tp_order.index(b) for b in tp_order if m & b][::-1]
    )
    first_tp = [m for m in tp_rank if m == tp_order[0]]
    for mask in first_tp:
        tp_wait(mask)
        for hop in later_hops(mask, tp_order):
            tp_copy(mask, hop).start()
    for mask in ep_masks:
        ids_wait(mask)
    for k in range(n_exp):
        for e in range(n_ep):
            ids = ids_in[e, pl.ds(ret_slot(k), 1), :]
            match = lax.broadcasted_iota(i32, (n_tok, slot_pad), 0) == ids
            picker[k, :, e * slot_pad : (e + 1) * slot_pad] = jnp.where(match, 1.0, 0.0).astype(bf16)
    ep_level(3, ep_levels[0])
    own_used.wait()
    loads[5].wait()
    loads[6].wait()
    low_masks = [m for m in range(1, n_tp) if m not in high_masks]
    for h in parts_of:
        for mask in low_masks:
            disp_wait(mask, h)
            for hop in low_hops(mask):
                disp_copy(mask, hop, h).start()
        used = normalise(used_rows[pl.ds(*chunks[h]), :], gain_ref[...])
        contract = (((1,), (1,)), ((), ()))
        gate = lax.dot_general(eg_ref[...], used, contract, preferred_element_type=f32)
        up = lax.dot_general(eu_ref[...], used, contract, preferred_element_type=f32)
        hidden[tp, :, pl.ds(*chunks[h])] = (jax.nn.silu(gate) * up).astype(bf16)
        for hop in tp_order[::-1]:
            hid_copy(0, hop, h).start()

    for masks in ep_levels[1:]:
        for w in (1, 2, 3):
            ep_level(w, masks)
    loads[4].wait()
    for mask in tp_rank:
        if mask not in first_tp:
            tp_wait(mask)
            for hop in later_hops(mask, tp_order):
                tp_copy(mask, hop).start()

    if flat:
        weights = flat
        cols = sg_hbm.shape[1]
        group = 128 // cols
        for ref, out in zip((sg_in, su_in, sd_in), flat):
            for j in range(n_ep // group):
                joined = jnp.concatenate([ref[j * group + i] for i in range(group)], axis=1)
                out[:, j * 128 : (j + 1) * 128] = joined
    else:
        weights = (sg_in, su_in, sd_in)
    sg_ref, su_ref, sd_ref = weights
    chunk = n_tok // 2

    def shared_rows(i, carry):
        rows = pl.ds(pl.multiple_of(i * chunk, chunk), chunk)
        x = normalise(own_rows[rows, :], gain_ref[...])
        contract = (((1,), (1,)), ((), ()))
        gate = lax.dot_general(x, sg_ref[...], contract, preferred_element_type=f32)
        up = lax.dot_general(x, su_ref[...], contract, preferred_element_type=f32)
        mid = (jax.nn.silu(gate) * up).astype(bf16)
        for block in range(n_tp):
            cols = pl.ds(block * width, width)
            parts[block, rows, :] = jnp.dot(
                mid, sd_ref[:, cols], preferred_element_type=f32
            ).astype(bf16)
        return carry

    lax.fori_loop(0, 2, shared_rows, 0)

    def sums_ends(j):
        @pl.when(tp == 0)
        def _():
            up_copy(n_tp - 1 - j).start()

        @pl.when(tp == n_tp - 1)
        def _():
            down_copy(j).start()

    def sums_middle(j):
        d = n_tp - 1 - j

        @pl.when(jnp.logical_and(tp > 0, tp < d))
        def _():
            up_wait(d)
            parts[d] = (parts[d].astype(f32) + in_up[d].astype(f32)).astype(bf16)
            up_copy(d).start()

        @pl.when(jnp.logical_and(tp < n_tp - 1, tp > j))
        def _():
            down_wait(j)
            parts[j] = (parts[j].astype(f32) + in_down[j].astype(f32)).astype(bf16)
            down_copy(j).start()

    def add_block(mask):
        block = flip(tp, mask)
        acc[block // split] += lax.dot_general(
            hidden[block], down_ref[block], (((0,), (0,)), ((), ())), preferred_element_type=f32
        )

    def give_back(k):
        s = ret_slot(k)
        weighted = (gates_col[s] * acc[s]).astype(bf16)
        slots = n_ep * slot_most
        placer = lax.broadcasted_iota(i32, (slots, cap), 0) == place_row[s]
        placer = jnp.where(placer, 1.0, 0.0).astype(bf16)
        placed = jnp.dot(placer, weighted, preferred_element_type=f32)
        stage[k] = placed.reshape(n_ep, slot_most, width).astype(bf16)
        for mask in ep_masks:
            ret_copy(mask, k).start()
        back[k, ep, :slot_most, :] = stage[k, ep]

    loads[7].wait()
    sums_ends(0)
    hid_masks = sorted(
        range(1, n_tp), key=lambda m: [tp_order.index(b) for b in tp_order if m & b][::-1]
    )
    hid_first = [m for m in hid_masks if m == tp_order[0]]
    for mask in hid_first:
        for h in parts_of:
            hid_wait(mask, h)
            for hop in later_hops(mask, tp_order):
                hid_copy(mask, hop, h).start()
    add_block(0)
    for k in range(n_exp):
        group = [m for m in hid_masks if m // split == k]
        for mask in group:
            if mask not in hid_first:
                for h in parts_of:
                    hid_wait(mask, h)
                    for hop in later_hops(mask, tp_order):
                        hid_copy(mask, hop, h).start()
            add_block(mask)
            if k > 0 and mask == group[0] and k == 1:
                for j in range(1, n_tp - 1):
                    sums_middle(j)
        give_back(k)
        if k == 0:
            for j in range(n_tp - 1):
                if j == 0:
                    sums_middle(0)
                if j > 0:
                    sums_ends(j)

    acc[0] = parts[tp].astype(f32)

    @pl.when(tp > 0)
    def _():
        up_wait(tp)
        acc[0] += in_up[tp].astype(f32)

    @pl.when(tp < n_tp - 1)
    def _():
        down_wait(tp)
        acc[0] += in_down[tp].astype(f32)

    for k in range(n_exp):
        for mask in ep_masks:
            ret_wait(mask, k)
        value = acc[0] + jnp.dot(
            picker[k], back[k].reshape(n_ep * slot_pad, width), preferred_element_type=f32
        )
        if k < n_exp - 1:
            acc[0] = value
        else:
            out_ref[...] = value.astype(bf16)

    for w in range(4):
        for h in (0, 1):
            for mask in range(n_ep):
                for hop in later_hops(mask, orders[h]):
                    ep_copy(w, h, mask, hop).wait_send()
    for mask in range(n_tp):
        for hop in later_hops(mask, tp_order):
            tp_copy(mask, hop).wait_send()
            for h in parts_of:
                hid_copy(mask, hop, h).wait_send()
    for mask in range(n_tp):
        hops = low_hops(mask)
        if mask == 0:
            hops = high_masks + hops
        for hop in hops:
            for h in parts_of:
                disp_copy(mask, hop, h).wait_send()
    for mask in ep_masks:
        ids_copy(mask).wait_send()
        for k in range(n_exp):
            ret_copy(mask, k).wait_send()
    for d in range(n_tp):

        @pl.when(tp < d)
        def _():
            up_copy(d).wait_send()

        @pl.when(tp > d)
        def _():
            down_copy(d).wait_send()


def on_device(
    tokens,
    norm_gain,
    shared_gate,
    shared_up,
    shared_down,
    expert_gate,
    expert_up,
    expert_down,
    chosen,
    gates,
):
    n_tp = lax.axis_size("tp")
    n_ep = lax.axis_size("ep")
    n_exp, cap = chosen.shape
    n_tok, width = tokens.shape
    model = n_tp * width
    bf16, f32, i32 = jnp.bfloat16, jnp.float32, jnp.int32
    slot_most = 2 * cap // n_ep
    slot_pad = -(-slot_most // 128) * 128
    n_hid = expert_gate.shape[2]
    sg, su, sd = shared_gate.T, shared_up.T, shared_down
    rows, cols = sg.shape
    if cols % 128 == 0:
        joined, flat = (rows, n_ep * cols), []
    else:
        joined = (n_ep, rows, cols)
        flat = [pltpu.VMEM((rows, n_ep * cols), bf16)] * 3
    vmem = pl.BlockSpec(memory_space=pltpu.VMEM)
    hbm = pl.BlockSpec(memory_space=pl.ANY)
    dma = pltpu.SemaphoreType.DMA
    return pl.pallas_call(
        functools.partial(layer_kernel, n_tp, n_ep, slot_most),
        out_shape=jax.ShapeDtypeStruct((n_tok, width), bf16),
        in_specs=[hbm, vmem] + [hbm] * 6 + [vmem] * 2,
        out_specs=vmem,
        scratch_shapes=[
            pltpu.VMEM((n_ep, n_tok, width), bf16),
            pltpu.VMEM((n_tok, model), bf16),
            pltpu.VMEM((cap, model), bf16),
            pltpu.VMEM((n_exp, cap, width), bf16),
            pltpu.VMEM(joined, bf16),
            pltpu.VMEM(joined, bf16),
            pltpu.VMEM(joined, bf16),
            pltpu.VMEM((n_hid, model), bf16),
            pltpu.VMEM((n_hid, model), bf16),
            pltpu.VMEM((n_tp, n_hid, width), bf16),
            pltpu.VMEM((n_tp, n_hid, cap), bf16),
            pltpu.VMEM((n_exp, cap, width), f32),
            pltpu.VMEM((n_tp, n_tok, width), bf16),
            pltpu.VMEM((n_tp, n_tok, width), bf16),
            pltpu.VMEM((n_tp, n_tok, width), bf16),
            pltpu.VMEM((n_exp, n_ep, slot_most, width), bf16),
            pltpu.VMEM((n_exp, n_ep, slot_pad, width), bf16),
            pltpu.VMEM((n_exp, n_tok, n_ep * slot_pad), bf16),
            pltpu.VMEM((n_ep, 8, slot_pad), i32),
            pltpu.VMEM((n_ep, 8, slot_pad), i32),
            pltpu.VMEM((n_exp, cap, 1), i32),
            pltpu.VMEM((n_exp, cap, 1), f32),
            pltpu.VMEM((n_exp, 1, cap), i32),
            dma((4, 2, n_ep)),
            dma((4, 2, n_ep)),
            dma((n_tp,)),
            dma((n_tp,)),
            dma((n_tp, 2)),
            dma((n_tp, 2)),
            dma((n_tp, 2)),
            dma((n_tp, 2)),
            dma((n_tp,)),
            dma((n_tp,)),
            dma((n_tp,)),
            dma((n_tp,)),
            dma((n_ep, n_exp)),
            dma((n_ep, n_exp)),
            dma((n_ep,)),
            dma((n_ep,)),
            dma((9,)),
        ]
        + flat,
        compiler_params=pltpu.CompilerParams(
            collective_id=0, has_side_effects=True, vmem_limit_bytes=62 * 1024 * 1024
        ),
    )(
        tokens,
        norm_gain.reshape(1, -1),
        sg,
        su,
        sd,
        expert_gate.reshape(n_hid, model),
        expert_up.reshape(n_hid, model),
        expert_down.reshape(n_tp, n_hid, width),
        chosen,
        gates,
    )


def solution(mesh):
    return jax.shard_map(
        on_device,
        mesh=mesh,
        in_specs=(
            P("ep", "tp"),
            P(),
            P("ep", "tp"),
            P("ep", "tp"),
            P("tp", "ep"),
            P("tp", "ep", None, None),
            P("tp", "ep", None, None),
            P("ep", None, "tp"),
            P("ep", None),
            P("ep", None),
        ),
        out_specs=P("ep", "tp"),
        check_vma=False,
    )
```

```python
import functools

import jax
import jax.numpy as jnp
from jax import lax
from jax.experimental import pallas as pl
from jax.experimental.pallas import tpu as pltpu
from jax.sharding import PartitionSpec as P

norm_eps = 1e-06
MESH = pl.DeviceIdType.MESH


def flip(index, mask):
    bit = 1
    result = index
    while bit <= mask:
        if mask & bit:
            result = result + bit - 2 * bit * ((index // bit) % 2)
        bit *= 2
    return result


def bits_below(count):
    return [1 << i for i in range(count.bit_length() - 1)]


def half_orders(count):
    bits = bits_below(count)
    upper = bits[1:]
    return [upper + bits[:1], upper[::-1] + bits[:1]]


def later_hops(mask, order):
    last = max([i for i, b in enumerate(order) if mask & b], default=-1)
    return order[last + 1 :]


def masks_by_level(count):
    return sorted(range(1, count), key=lambda m: (bin(m).count("1"), -m))


def levels(count):
    found = {}
    for m in masks_by_level(count):
        found.setdefault(bin(m).count("1"), []).append(m)
    return [found[k] for k in sorted(found)]


def column_of(row, count):
    same = lax.broadcasted_iota(jnp.int32, (count, count), 0) == lax.broadcasted_iota(
        jnp.int32, (count, count), 1
    )
    return jnp.sum(jnp.where(same, row, 0.0), axis=1, keepdims=True)


def normalise(rows, gain):
    widened = rows.astype(jnp.float32)
    inv_scale = lax.rsqrt(jnp.mean(widened * widened, axis=1, keepdims=True) + norm_eps)
    return (widened * inv_scale * gain).astype(jnp.bfloat16)


def layer_kernel(
    n_tp,
    n_ep,
    slot_most,
    tok_hbm,
    gain_ref,
    sg_hbm,
    su_hbm,
    sd_hbm,
    eg_hbm,
    eu_hbm,
    down_hbm,
    chosen_ref,
    gates_ref,
    out_ref,
    tok_all,
    own_rows,
    used_rows,
    sel,
    sg_in,
    su_in,
    sd_in,
    eg_ref,
    eu_ref,
    down_ref,
    hidden,
    acc,
    parts,
    in_up,
    in_down,
    stage,
    back,
    picker,
    ids_out,
    ids_in,
    chosen_col,
    gates_col,
    place_row,
    ep_send,
    ep_recv,
    tp_send,
    tp_recv,
    disp_send,
    disp_recv,
    far_send,
    hid_send,
    hid_recv,
    up_send,
    up_recv,
    down_send,
    down_recv,
    ret_send,
    ret_recv,
    ids_send_sem,
    ids_recv_sem,
    local_sem,
    *flat,
):
    tp = lax.axis_index("tp")
    ep = lax.axis_index("ep")
    f32, bf16, i32 = jnp.float32, jnp.bfloat16, jnp.int32
    n_exp, cap = chosen_ref.shape
    n_tok, width = tok_hbm.shape
    n_hid = eg_ref.shape[0]
    slot_pad = back.shape[2]
    split = n_tp // n_exp
    slot = tp // split
    orders = half_orders(n_ep)
    ep_levels = levels(n_ep)
    cut = max(128, cap * 2 // 3 // 128 * 128)
    chunks = [(0, cut), (cut, cap - cut)]
    parts_of = range(len(chunks))

    own_loads = [
        (tok_hbm, tok_all.at[ep]),
        (sg_hbm, sg_in),
        (su_hbm, su_in),
        (sd_hbm, sd_in),
    ]

    def block_of(out, block, rows):
        if len(out.shape) == 3:
            return out.at[block, rows, :]
        cols = out.shape[1] // n_ep
        return out.at[rows, pl.ds(pl.multiple_of(block * cols, cols), cols)]

    def columns(ref, block):
        return ref.at[:, pl.ds(pl.multiple_of(block * width, width), width)]

    loads = []
    for i, (source, target) in enumerate(own_loads):
        if i > 0:
            target = block_of(target, ep, pl.ds(0, source.shape[0]))
        loads.append(pltpu.make_async_copy(source, target, local_sem.at[i]))
    loads.append(pltpu.make_async_copy(tok_hbm, columns(own_rows, tp), local_sem.at[4]))
    for i, (source, target) in enumerate(((eg_hbm, eg_ref), (eu_hbm, eu_ref), (down_hbm, down_ref))):
        loads.append(pltpu.make_async_copy(source, target, local_sem.at[5 + i]))
    for load in loads:
        load.start()

    barrier = pltpu.get_barrier_semaphore()
    for mask in range(1, n_tp):
        pl.semaphore_signal(barrier, inc=1, device_id={"tp": flip(tp, mask)}, device_id_type=MESH)
    for mask in range(1, n_ep):
        pl.semaphore_signal(barrier, inc=1, device_id={"ep": flip(ep, mask)}, device_id_type=MESH)
    back[...] = jnp.zeros_like(back)
    ids_out[...] = jnp.zeros_like(ids_out)
    acc[...] = jnp.zeros_like(acc)
    pl.semaphore_wait(barrier, n_tp + n_ep - 2)

    def piece(w, block, h):
        half = own_loads[w][0].shape[0] // 2
        rows = pl.ds(h * half, half)
        if w == 0:
            return tok_all.at[block, rows, :]
        return block_of([None, sg_in, su_in, sd_in][w], block, rows)

    def remote(source, target, send, recv, axis, place):
        return pltpu.make_async_remote_copy(
            src_ref=source,
            dst_ref=target,
            send_sem=send,
            recv_sem=recv,
            device_id={axis: place},
            device_id_type=MESH,
        )

    def ep_copy(w, h, mask, hop):
        ref = piece(w, flip(ep, mask), h)
        sem = (w, h, mask | hop)
        return remote(ref, ref, ep_send.at[sem], ep_recv.at[sem], "ep", flip(ep, hop))

    def ep_wait(w, h, mask):
        hop = [b for b in orders[h] if mask & b][-1]
        ref = piece(w, flip(ep, mask), h)
        sem = (w, h, mask)
        remote(ref, ref, ep_send.at[sem], ep_recv.at[sem], "ep", flip(ep, hop)).wait_recv()

    def ep_start(w):
        for position in range(len(orders[0])):
            for h in (0, 1):
                ep_copy(w, h, 0, orders[h][position]).start()

    def ep_level(w, masks):
        for mask in masks:
            for h in (0, 1):
                ep_wait(w, h, mask)
                for hop in later_hops(mask, orders[h]):
                    ep_copy(w, h, mask, hop).start()

    def known(up, j):
        return tp >= j if up else tp < n_tp - j

    def ahead(up):
        return tp < n_tp - 1 if up else tp > 0

    def at_distance(up, j):
        return tp - j if up else tp + j

    def tok_ref(ref, block, h):
        half = n_tok // 2
        cols = pl.ds(pl.multiple_of(block * width, width), width)
        return ref.at[pl.ds(h * half, half), cols]

    def tok_copy(up, j, h):
        ref = tok_ref(own_rows, at_distance(up, j), h)
        source = tok_all.at[ep, pl.ds(h * (n_tok // 2), n_tok // 2), :] if j == 0 else ref
        sem = (up, j, h)
        return remote(
            source, ref, tp_send.at[sem], tp_recv.at[sem], "tp", at_distance(1 - up, 1)
        )

    def tok_wait(up, j, h):
        ref = tok_ref(own_rows, at_distance(up, j), h)
        sem = (up, j - 1, h)
        remote(ref, ref, tp_send.at[sem], tp_recv.at[sem], "tp", at_distance(up, 1)).wait_recv()

    def hid_copy(up, j, h):
        ref = hidden.at[at_distance(up, j), :, pl.ds(*chunks[h])]
        sem = (up, j, h)
        return remote(
            ref, ref, hid_send.at[sem], hid_recv.at[sem], "tp", at_distance(1 - up, 1)
        )

    def hid_wait(up, j, h):
        ref = hidden.at[at_distance(up, j), :, pl.ds(*chunks[h])]
        sem = (up, j - 1, h)
        remote(ref, ref, hid_send.at[sem], hid_recv.at[sem], "tp", at_distance(up, 1)).wait_recv()

    def line_start(copy, *rest):
        for up in (0, 1):

            @pl.when(ahead(up))
            def _():
                copy(up, 0, *rest).start()

    def line_pass(copy, wait, j, *rest, side=None):
        for up in (0, 1):
            here = known(up, j)
            if side is not None:
                near = tp < n_tp // 2 if up == side else tp >= n_tp // 2
                here = jnp.logical_and(here, near)

            @pl.when(here)
            def _():
                wait(up, j, *rest)

                @pl.when(ahead(up))
                def _():
                    copy(up, j, *rest).start()

    def hid_pass(j, side):
        for h in parts_of:
            line_pass(hid_copy, hid_wait, j, h, side=side)

    def tok_pass(j, h):
        line_pass(tok_copy, tok_wait, j, h)

    def ret_slot(k):
        return flip(tp, k * split) // split

    low = slot * split
    top = low + split - 1

    def in_group(up):
        return tp < top if up else tp > low

    def used_piece(block, h):
        cols = pl.ds(pl.multiple_of(block * width, width), width)
        return used_rows.at[pl.ds(*chunks[h]), cols]

    def disp_copy(up, j, h):
        block = at_distance(up, j)
        ref = used_piece(block, h)
        source = sel.at[slot, pl.ds(*chunks[h]), :] if j == 0 else ref
        return remote(
            source,
            ref,
            disp_send.at[up, j, h],
            disp_recv.at[block, h],
            "tp",
            at_distance(1 - up, 1),
        )

    def disp_wait(up, j, h):
        block = at_distance(up, j)
        ref = used_piece(block, h)
        remote(
            ref, ref, disp_send.at[up, j, h], disp_recv.at[block, h], "tp", at_distance(up, 1)
        ).wait_recv()

    def far_copy(k, h, entry):
        return remote(
            sel.at[ret_slot(k), pl.ds(*chunks[h]), :],
            used_piece(tp, h),
            far_send.at[k, h],
            disp_recv.at[tp, h],
            "tp",
            entry,
        )

    def far_each(act, h):
        for k in range(1, n_exp):
            s = ret_slot(k)

            @pl.when(s > slot)
            def _():
                act(far_copy(k, h, s * split))

            @pl.when(s < slot)
            def _():
                act(far_copy(k, h, s * split + split - 1))

    def disp_start(h):
        far_each(lambda copy: copy.start(), h)
        for up in (0, 1):

            @pl.when(in_group(up))
            def _():
                disp_copy(up, 0, h).start()

    def disp_pass(j, h):
        for up in (0, 1):

            @pl.when(jnp.logical_and(known(up, j), in_group(up)))
            def _():
                disp_wait(up, j, h)
                disp_copy(up, j, h).start()

    def disp_rest(h):
        for j in range(1, n_tp):
            for up in (0, 1):

                @pl.when(jnp.logical_and(known(up, j), jnp.logical_not(in_group(up))))
                def _():
                    disp_wait(up, j, h)

    def up_copy(d):
        return remote(parts.at[d], in_up.at[d], up_send.at[d], up_recv.at[d], "tp", tp + 1)

    def down_copy(d):
        return remote(parts.at[d], in_down.at[d], down_send.at[d], down_recv.at[d], "tp", tp - 1)

    def up_wait(d):
        ref = in_up.at[d]
        remote(ref, ref, up_send.at[d], up_recv.at[d], "tp", tp - 1).wait_recv()

    def down_wait(d):
        ref = in_down.at[d]
        remote(ref, ref, down_send.at[d], down_recv.at[d], "tp", tp + 1).wait_recv()

    def ret_copy(mask, k):
        rows = pl.ds(0, slot_most)
        return remote(
            stage.at[k, flip(ep, mask)],
            back.at[k, ep, rows, :],
            ret_send.at[mask, k],
            ret_recv.at[mask, k],
            "ep",
            flip(ep, mask),
        )

    def ret_wait(mask, k):
        ref = back.at[k, flip(ep, mask), pl.ds(0, slot_most), :]
        sem = (mask, k)
        remote(ref, ref, ret_send.at[sem], ret_recv.at[sem], "ep", flip(ep, mask)).wait_recv()

    def ids_copy(mask):
        return remote(
            ids_out.at[flip(ep, mask)],
            ids_in.at[ep],
            ids_send_sem.at[mask],
            ids_recv_sem.at[mask],
            "ep",
            flip(ep, mask),
        )

    def ids_wait(mask):
        ref = ids_in.at[flip(ep, mask)]
        remote(
            ref, ref, ids_send_sem.at[mask], ids_recv_sem.at[mask], "ep", flip(ep, mask)
        ).wait_recv()

    loads[0].wait()
    ep_start(0)
    for h in (0, 1):
        line_start(tok_copy, h)

    for s in range(n_exp):
        row = chosen_ref[pl.ds(s, 1), :]
        col = column_of(row.astype(f32), cap).astype(i32)
        chosen_col[s] = col
        gates_col[s] = column_of(gates_ref[pl.ds(s, 1), :], cap)
        row_from = jnp.zeros_like(row)
        col_from = jnp.zeros_like(col)
        for d in range(1, n_ep):
            row_from += jnp.where(row >= d * n_tok, 1, 0)
            col_from += jnp.where(col >= d * n_tok, 1, 0)
        before = jnp.where(col < row_from * n_tok, 1.0, 0.0)
        run_row = jnp.sum(before, axis=0, keepdims=True).astype(i32)
        before = jnp.where(row < col_from * n_tok, 1.0, 0.0)
        run_col = jnp.sum(before, axis=1, keepdims=True).astype(i32)
        lanes = lax.broadcasted_iota(i32, (1, cap), 1)
        rows = lax.broadcasted_iota(i32, (cap, 1), 0)
        place_row[s] = row_from * slot_most + lanes - run_row
        within = rows - run_col

        def slot_ids(d, carry):
            slots = lax.broadcasted_iota(i32, (cap, slot_pad), 1)
            wanted = jnp.where(col_from == d, within, -1)
            value = (col - d * n_tok + 1).astype(f32)
            total = jnp.sum(jnp.where(slots == wanted, value, 0.0), axis=0, keepdims=True)
            ids_out[d, pl.ds(s, 1), :] = total.astype(i32) - 1
            return carry

        lax.fori_loop(0, n_ep, slot_ids, 0)

    def select(e):
        def one(s, carry):
            ids = lax.broadcasted_iota(i32, (cap, n_tok), 1) + e * n_tok
            hits = jnp.where(chosen_col[s] == ids, 1.0, 0.0).astype(bf16)
            acc[s] += jnp.dot(hits, tok_all[e], preferred_element_type=f32)
            return carry

        lax.fori_loop(0, n_exp, one, 0)

    select(ep)
    if n_tp > 2:
        tok_pass(1, 0)
    ep_level(0, ep_levels[0])
    for load in loads[1:4]:
        load.wait()
    for w in (1, 2, 3):
        ep_start(w)
    ep_masks = sorted(range(1, n_ep), key=lambda m: -bin(m >> 1).count("1"))
    for mask in ep_masks:
        ids_copy(mask).start()
    ids_in[ep] = ids_out[ep]
    if n_tp > 2:
        tok_pass(1, 1)
    for mask in ep_levels[0]:
        select(flip(ep, mask))
    if n_tp > 3:
        tok_pass(2, 0)
    for masks in ep_levels[1:]:
        for mask in sorted(masks, key=lambda m: -(m % 2)):
            ep_level(0, [mask])
            select(flip(ep, mask))
    for s in range(n_exp):
        sel[s] = acc[s].astype(bf16)
    disp_start(0)
    own_used = pltpu.make_async_copy(sel.at[slot], columns(used_rows, tp), local_sem.at[8])
    own_used.start()
    acc[...] = jnp.zeros_like(acc)
    if n_tp > 3:
        tok_pass(2, 1)
    for j in range(3, n_tp - 1):
        for h in (0, 1):
            tok_pass(j, h)
    ep_level(1, ep_levels[0])
    disp_start(1)
    for j in range(1, n_tp):
        disp_pass(j, 0)
    ep_level(2, ep_levels[0])
    for j in range(1, n_tp):
        disp_pass(j, 1)
    for mask in ep_masks:
        ids_wait(mask)
    for k in range(n_exp):
        for e in range(n_ep):
            ids = ids_in[e, pl.ds(ret_slot(k), 1), :]
            match = lax.broadcasted_iota(i32, (n_tok, slot_pad), 0) == ids
            picker[k, :, e * slot_pad : (e + 1) * slot_pad] = jnp.where(match, 1.0, 0.0).astype(bf16)
    ep_level(3, ep_levels[0])
    own_used.wait()
    loads[5].wait()
    loads[6].wait()
    for h in parts_of:
        disp_rest(h)
        used = normalise(used_rows[pl.ds(*chunks[h]), :], gain_ref[...])
        contract = (((1,), (1,)), ((), ()))
        gate = lax.dot_general(eg_ref[...], used, contract, preferred_element_type=f32)
        up = lax.dot_general(eu_ref[...], used, contract, preferred_element_type=f32)
        hidden[tp, :, pl.ds(*chunks[h])] = (jax.nn.silu(gate) * up).astype(bf16)
        line_start(hid_copy, h)
    for masks in ep_levels[1:]:
        for w in (1, 2, 3):
            ep_level(w, masks)
    loads[4].wait()
    for h in (0, 1):
        tok_pass(n_tp - 1, h)
    hid_pass(1, 0)
    if flat:
        weights = flat
        cols = sg_hbm.shape[1]
        group = 128 // cols
        for ref, out in zip((sg_in, su_in, sd_in), flat):
            for j in range(n_ep // group):
                joined = jnp.concatenate([ref[j * group + i] for i in range(group)], axis=1)
                out[:, j * 128 : (j + 1) * 128] = joined
    else:
        weights = (sg_in, su_in, sd_in)
    sg_ref, su_ref, sd_ref = weights
    chunk = n_tok // 2

    def shared_rows(i, carry):
        rows = pl.ds(pl.multiple_of(i * chunk, chunk), chunk)
        x = normalise(own_rows[rows, :], gain_ref[...])
        contract = (((1,), (1,)), ((), ()))
        gate = lax.dot_general(x, sg_ref[...], contract, preferred_element_type=f32)
        up = lax.dot_general(x, su_ref[...], contract, preferred_element_type=f32)
        mid = (jax.nn.silu(gate) * up).astype(bf16)
        for block in range(n_tp):
            cols = pl.ds(block * width, width)
            parts[block, rows, :] = jnp.dot(
                mid, sd_ref[:, cols], preferred_element_type=f32
            ).astype(bf16)
        return carry

    lax.fori_loop(0, 2, shared_rows, 0)

    def sums_ends(j):
        @pl.when(tp == 0)
        def _():
            up_copy(n_tp - 1 - j).start()

        @pl.when(tp == n_tp - 1)
        def _():
            down_copy(j).start()

    def sums_middle(j):
        d = n_tp - 1 - j

        @pl.when(jnp.logical_and(tp > 0, tp < d))
        def _():
            up_wait(d)
            parts[d] = (parts[d].astype(f32) + in_up[d].astype(f32)).astype(bf16)
            up_copy(d).start()

        @pl.when(jnp.logical_and(tp < n_tp - 1, tp > j))
        def _():
            down_wait(j)
            parts[j] = (parts[j].astype(f32) + in_down[j].astype(f32)).astype(bf16)
            down_copy(j).start()

    def add_block(mask):
        block = flip(tp, mask)
        acc[block // split] += lax.dot_general(
            hidden[block], down_ref[block], (((0,), (0,)), ((), ())), preferred_element_type=f32
        )

    def give_back(k):
        s = ret_slot(k)
        weighted = (gates_col[s] * acc[s]).astype(bf16)
        slots = n_ep * slot_most
        placer = lax.broadcasted_iota(i32, (slots, cap), 0) == place_row[s]
        placer = jnp.where(placer, 1.0, 0.0).astype(bf16)
        placed = jnp.dot(placer, weighted, preferred_element_type=f32)
        stage[k] = placed.reshape(n_ep, slot_most, width).astype(bf16)
        for mask in ep_masks:
            ret_copy(mask, k).start()
        back[k, ep, :slot_most, :] = stage[k, ep]

    loads[7].wait()
    sums_ends(0)
    add_block(0)
    hid_pass(1, 1)
    for j in range(1, n_tp):
        if j > 1:
            hid_pass(j, 0)
            hid_pass(j, 1)
        add_block(j)
        if (j + 1) % split == 0:
            give_back(j // split)
        if j > 1:
            sums_middle(j - 2)
        if j < n_tp - 1:
            sums_ends(j)
    sums_middle(n_tp - 2)
    acc[0] = parts[tp].astype(f32)

    @pl.when(tp > 0)
    def _():
        up_wait(tp)
        acc[0] += in_up[tp].astype(f32)

    @pl.when(tp < n_tp - 1)
    def _():
        down_wait(tp)
        acc[0] += in_down[tp].astype(f32)

    for k in range(n_exp):
        for mask in ep_masks:
            ret_wait(mask, k)
        value = acc[0] + jnp.dot(
            picker[k], back[k].reshape(n_ep * slot_pad, width), preferred_element_type=f32
        )
        if k < n_exp - 1:
            acc[0] = value
        else:
            out_ref[...] = value.astype(bf16)

    for w in range(4):
        for h in (0, 1):
            for mask in range(n_ep):
                for hop in later_hops(mask, orders[h]):
                    ep_copy(w, h, mask, hop).wait_send()
    for h in parts_of:
        far_each(lambda copy: copy.wait_send(), h)
    for up in (0, 1):
        for j in range(n_tp - 1):

            @pl.when(jnp.logical_and(known(up, j), ahead(up)))
            def _():
                for h in parts_of:
                    tok_copy(up, j, h).wait_send()
                    hid_copy(up, j, h).wait_send()

        for j in range(n_tp):

            @pl.when(jnp.logical_and(known(up, j), in_group(up)))
            def _():
                for h in parts_of:
                    disp_copy(up, j, h).wait_send()

    for mask in ep_masks:
        ids_copy(mask).wait_send()
        for k in range(n_exp):
            ret_copy(mask, k).wait_send()
    for d in range(n_tp):

        @pl.when(tp < d)
        def _():
            up_copy(d).wait_send()

        @pl.when(tp > d)
        def _():
            down_copy(d).wait_send()


def on_device(
    tokens,
    norm_gain,
    shared_gate,
    shared_up,
    shared_down,
    expert_gate,
    expert_up,
    expert_down,
    chosen,
    gates,
):
    n_tp = lax.axis_size("tp")
    n_ep = lax.axis_size("ep")
    n_exp, cap = chosen.shape
    n_tok, width = tokens.shape
    model = n_tp * width
    bf16, f32, i32 = jnp.bfloat16, jnp.float32, jnp.int32
    slot_most = 2 * cap // n_ep
    slot_pad = -(-slot_most // 128) * 128
    n_hid = expert_gate.shape[2]
    sg, su, sd = shared_gate.T, shared_up.T, shared_down
    rows, cols = sg.shape
    if cols % 128 == 0:
        joined, flat = (rows, n_ep * cols), []
    else:
        joined = (n_ep, rows, cols)
        flat = [pltpu.VMEM((rows, n_ep * cols), bf16)] * 3
    vmem = pl.BlockSpec(memory_space=pltpu.VMEM)
    hbm = pl.BlockSpec(memory_space=pl.ANY)
    dma = pltpu.SemaphoreType.DMA
    return pl.pallas_call(
        functools.partial(layer_kernel, n_tp, n_ep, slot_most),
        out_shape=jax.ShapeDtypeStruct((n_tok, width), bf16),
        in_specs=[hbm, vmem] + [hbm] * 6 + [vmem] * 2,
        out_specs=vmem,
        scratch_shapes=[
            pltpu.VMEM((n_ep, n_tok, width), bf16),
            pltpu.VMEM((n_tok, model), bf16),
            pltpu.VMEM((cap, model), bf16),
            pltpu.VMEM((n_exp, cap, width), bf16),
            pltpu.VMEM(joined, bf16),
            pltpu.VMEM(joined, bf16),
            pltpu.VMEM(joined, bf16),
            pltpu.VMEM((n_hid, model), bf16),
            pltpu.VMEM((n_hid, model), bf16),
            pltpu.VMEM((n_tp, n_hid, width), bf16),
            pltpu.VMEM((n_tp, n_hid, cap), bf16),
            pltpu.VMEM((n_exp, cap, width), f32),
            pltpu.VMEM((n_tp, n_tok, width), bf16),
            pltpu.VMEM((n_tp, n_tok, width), bf16),
            pltpu.VMEM((n_tp, n_tok, width), bf16),
            pltpu.VMEM((n_exp, n_ep, slot_most, width), bf16),
            pltpu.VMEM((n_exp, n_ep, slot_pad, width), bf16),
            pltpu.VMEM((n_exp, n_tok, n_ep * slot_pad), bf16),
            pltpu.VMEM((n_ep, 8, slot_pad), i32),
            pltpu.VMEM((n_ep, 8, slot_pad), i32),
            pltpu.VMEM((n_exp, cap, 1), i32),
            pltpu.VMEM((n_exp, cap, 1), f32),
            pltpu.VMEM((n_exp, 1, cap), i32),
            dma((4, 2, n_ep)),
            dma((4, 2, n_ep)),
            dma((2, n_tp, 2)),
            dma((2, n_tp, 2)),
            dma((2, n_tp, 2)),
            dma((n_tp, 2)),
            dma((n_exp, 2)),
            dma((2, n_tp, 2)),
            dma((2, n_tp, 2)),
            dma((n_tp,)),
            dma((n_tp,)),
            dma((n_tp,)),
            dma((n_tp,)),
            dma((n_ep, n_exp)),
            dma((n_ep, n_exp)),
            dma((n_ep,)),
            dma((n_ep,)),
            dma((9,)),
        ]
        + flat,
        compiler_params=pltpu.CompilerParams(
            collective_id=0, has_side_effects=True, vmem_limit_bytes=62 * 1024 * 1024
        ),
    )(
        tokens,
        norm_gain.reshape(1, -1),
        sg,
        su,
        sd,
        expert_gate.reshape(n_hid, model),
        expert_up.reshape(n_hid, model),
        expert_down.reshape(n_tp, n_hid, width),
        chosen,
        gates,
    )


def solution(mesh):
    return jax.shard_map(
        on_device,
        mesh=mesh,
        in_specs=(
            P("ep", "tp"),
            P(),
            P("ep", "tp"),
            P("ep", "tp"),
            P("tp", "ep"),
            P("tp", "ep", None, None),
            P("tp", "ep", None, None),
            P("ep", None, "tp"),
            P("ep", None),
            P("ep", None),
        ),
        out_specs=P("ep", "tp"),
        check_vma=False,
    )
```

```python
import functools

import jax
import jax.numpy as jnp
from jax import lax
from jax.experimental import pallas as pl
from jax.experimental.pallas import tpu as pltpu
from jax.sharding import PartitionSpec as P

norm_eps = 1e-06
MESH = pl.DeviceIdType.MESH


def flip(index, mask):
    bit = 1
    result = index
    while bit <= mask:
        if mask & bit:
            result = result + bit - 2 * bit * ((index // bit) % 2)
        bit *= 2
    return result


def bits_below(count):
    return [1 << i for i in range(count.bit_length() - 1)]


def half_orders(count):
    bits = bits_below(count)
    upper = bits[1:]
    return [upper + bits[:1], upper[::-1] + bits[:1]]


def later_hops(mask, order):
    last = max([i for i, b in enumerate(order) if mask & b], default=-1)
    return order[last + 1 :]


def masks_by_level(count):
    return sorted(range(1, count), key=lambda m: (bin(m).count("1"), -m))


def levels(count):
    found = {}
    for m in masks_by_level(count):
        found.setdefault(bin(m).count("1"), []).append(m)
    return [found[k] for k in sorted(found)]


def column_of(row, count):
    same = lax.broadcasted_iota(jnp.int32, (count, count), 0) == lax.broadcasted_iota(
        jnp.int32, (count, count), 1
    )
    return jnp.sum(jnp.where(same, row, 0.0), axis=1, keepdims=True)


def normalise(rows, gain):
    widened = rows.astype(jnp.float32)
    inv_scale = lax.rsqrt(jnp.mean(widened * widened, axis=1, keepdims=True) + norm_eps)
    return (widened * inv_scale * gain).astype(jnp.bfloat16)


def layer_kernel(
    n_tp,
    n_ep,
    slot_most,
    tok_hbm,
    gain_ref,
    sg_hbm,
    su_hbm,
    sd_hbm,
    eg_hbm,
    eu_hbm,
    down_hbm,
    chosen_ref,
    gates_ref,
    out_ref,
    tok_all,
    own_rows,
    used_rows,
    sel,
    sg_in,
    su_in,
    sd_in,
    eg_ref,
    eu_ref,
    down_ref,
    hidden,
    acc,
    parts,
    in_up,
    in_down,
    stage,
    back,
    picker,
    ids_out,
    ids_in,
    chosen_col,
    gates_col,
    place_row,
    ep_send,
    ep_recv,
    tp_send,
    tp_recv,
    disp_send,
    disp_recv,
    far_send,
    hid_send,
    hid_recv,
    up_send,
    up_recv,
    down_send,
    down_recv,
    ret_send,
    ret_recv,
    ids_send_sem,
    ids_recv_sem,
    local_sem,
    *flat,
):
    tp = lax.axis_index("tp")
    ep = lax.axis_index("ep")
    f32, bf16, i32 = jnp.float32, jnp.bfloat16, jnp.int32
    n_exp, cap = chosen_ref.shape
    n_tok, width = tok_hbm.shape
    n_hid = eg_ref.shape[0]
    slot_pad = back.shape[2]
    split = n_tp // n_exp
    slot = tp // split
    orders = half_orders(n_ep)
    ep_levels = levels(n_ep)
    cut = max(128, cap * 2 // 3 // 128 * 128)
    chunks = [(0, cut), (cut, cap - cut)]
    parts_of = range(len(chunks))

    own_loads = [
        (tok_hbm, tok_all.at[ep]),
        (sg_hbm, sg_in),
        (su_hbm, su_in),
        (sd_hbm, sd_in),
    ]

    def block_of(out, block, rows):
        if len(out.shape) == 3:
            return out.at[block, rows, :]
        cols = out.shape[1] // n_ep
        return out.at[rows, pl.ds(pl.multiple_of(block * cols, cols), cols)]

    def columns(ref, block):
        return ref.at[:, pl.ds(pl.multiple_of(block * width, width), width)]

    loads = []
    for i, (source, target) in enumerate(own_loads):
        if i > 0:
            target = block_of(target, ep, pl.ds(0, source.shape[0]))
        loads.append(pltpu.make_async_copy(source, target, local_sem.at[i]))
    loads.append(pltpu.make_async_copy(tok_hbm, columns(own_rows, tp), local_sem.at[4]))
    for i, (source, target) in enumerate(((eg_hbm, eg_ref), (eu_hbm, eu_ref), (down_hbm, down_ref))):
        loads.append(pltpu.make_async_copy(source, target, local_sem.at[5 + i]))
    for load in loads:
        load.start()

    barrier = pltpu.get_barrier_semaphore()
    for mask in range(1, n_tp):
        pl.semaphore_signal(barrier, inc=1, device_id={"tp": flip(tp, mask)}, device_id_type=MESH)
    for mask in range(1, n_ep):
        pl.semaphore_signal(barrier, inc=1, device_id={"ep": flip(ep, mask)}, device_id_type=MESH)
    back[...] = jnp.zeros_like(back)
    ids_out[...] = jnp.zeros_like(ids_out)
    acc[...] = jnp.zeros_like(acc)
    pl.semaphore_wait(barrier, n_tp + n_ep - 2)

    def piece(w, block, h):
        half = own_loads[w][0].shape[0] // 2
        rows = pl.ds(h * half, half)
        if w == 0:
            return tok_all.at[block, rows, :]
        return block_of([None, sg_in, su_in, sd_in][w], block, rows)

    def remote(source, target, send, recv, axis, place):
        return pltpu.make_async_remote_copy(
            src_ref=source,
            dst_ref=target,
            send_sem=send,
            recv_sem=recv,
            device_id={axis: place},
            device_id_type=MESH,
        )

    def ep_copy(w, h, mask, hop):
        ref = piece(w, flip(ep, mask), h)
        sem = (w, h, mask | hop)
        return remote(ref, ref, ep_send.at[sem], ep_recv.at[sem], "ep", flip(ep, hop))

    def ep_wait(w, h, mask):
        hop = [b for b in orders[h] if mask & b][-1]
        ref = piece(w, flip(ep, mask), h)
        sem = (w, h, mask)
        remote(ref, ref, ep_send.at[sem], ep_recv.at[sem], "ep", flip(ep, hop)).wait_recv()

    def ep_start(w):
        for position in range(len(orders[0])):
            for h in (0, 1):
                ep_copy(w, h, 0, orders[h][position]).start()

    def ep_level(w, masks):
        for mask in masks:
            for h in (0, 1):
                ep_wait(w, h, mask)
                for hop in later_hops(mask, orders[h]):
                    ep_copy(w, h, mask, hop).start()

    def known(up, j):
        return tp >= j if up else tp < n_tp - j

    def ahead(up):
        return tp < n_tp - 1 if up else tp > 0

    def at_distance(up, j):
        return tp - j if up else tp + j

    def tok_ref(ref, block, h):
        half = n_tok // 2
        cols = pl.ds(pl.multiple_of(block * width, width), width)
        return ref.at[pl.ds(h * half, half), cols]

    def tok_copy(up, j, h):
        ref = tok_ref(own_rows, at_distance(up, j), h)
        source = tok_all.at[ep, pl.ds(h * (n_tok // 2), n_tok // 2), :] if j == 0 else ref
        sem = (up, j, h)
        return remote(
            source, ref, tp_send.at[sem], tp_recv.at[sem], "tp", at_distance(1 - up, 1)
        )

    def tok_wait(up, j, h):
        ref = tok_ref(own_rows, at_distance(up, j), h)
        sem = (up, j - 1, h)
        remote(ref, ref, tp_send.at[sem], tp_recv.at[sem], "tp", at_distance(up, 1)).wait_recv()

    def hid_copy(up, j, h):
        ref = hidden.at[at_distance(up, j), :, pl.ds(*chunks[h])]
        sem = (up, j, h)
        return remote(
            ref, ref, hid_send.at[sem], hid_recv.at[sem], "tp", at_distance(1 - up, 1)
        )

    def hid_wait(up, j, h):
        ref = hidden.at[at_distance(up, j), :, pl.ds(*chunks[h])]
        sem = (up, j - 1, h)
        remote(ref, ref, hid_send.at[sem], hid_recv.at[sem], "tp", at_distance(up, 1)).wait_recv()

    def line_start(copy, *rest):
        for up in (0, 1):

            @pl.when(ahead(up))
            def _():
                copy(up, 0, *rest).start()

    def line_pass(copy, wait, j, *rest, side=None):
        for up in (0, 1):
            here = known(up, j)
            if side is not None:
                near = tp < n_tp // 2 if up == side else tp >= n_tp // 2
                here = jnp.logical_and(here, near)

            @pl.when(here)
            def _():
                wait(up, j, *rest)

                @pl.when(ahead(up))
                def _():
                    copy(up, j, *rest).start()

    def hid_pass(j, side):
        for h in parts_of:
            line_pass(hid_copy, hid_wait, j, h, side=side)

    def tok_pass(j, h):
        line_pass(tok_copy, tok_wait, j, h)

    def ret_slot(k):
        return flip(tp, k * split) // split

    low = slot * split
    top = low + split - 1

    def in_group(up):
        return tp < top if up else tp > low

    def used_piece(block, h):
        cols = pl.ds(pl.multiple_of(block * width, width), width)
        return used_rows.at[pl.ds(*chunks[h]), cols]

    def disp_copy(up, j, h):
        block = at_distance(up, j)
        ref = used_piece(block, h)
        source = sel.at[slot, pl.ds(*chunks[h]), :] if j == 0 else ref
        return remote(
            source,
            ref,
            disp_send.at[up, j, h],
            disp_recv.at[block, h],
            "tp",
            at_distance(1 - up, 1),
        )

    def disp_wait(up, j, h):
        block = at_distance(up, j)
        ref = used_piece(block, h)
        remote(
            ref, ref, disp_send.at[up, j, h], disp_recv.at[block, h], "tp", at_distance(up, 1)
        ).wait_recv()

    def far_copy(k, h, entry):
        return remote(
            sel.at[ret_slot(k), pl.ds(*chunks[h]), :],
            used_piece(tp, h),
            far_send.at[k, h],
            disp_recv.at[tp, h],
            "tp",
            entry,
        )

    def far_each(act, h):
        for k in range(1, n_exp):
            s = ret_slot(k)

            @pl.when(s > slot)
            def _():
                act(far_copy(k, h, s * split))

            @pl.when(s < slot)
            def _():
                act(far_copy(k, h, s * split + split - 1))

    def disp_start(h):
        far_each(lambda copy: copy.start(), h)
        for up in (0, 1):

            @pl.when(in_group(up))
            def _():
                disp_copy(up, 0, h).start()

    def disp_pass(j, h):
        for up in (0, 1):

            @pl.when(jnp.logical_and(known(up, j), in_group(up)))
            def _():
                disp_wait(up, j, h)
                disp_copy(up, j, h).start()

    def disp_rest(h):
        for j in range(1, n_tp):
            for up in (0, 1):

                @pl.when(jnp.logical_and(known(up, j), jnp.logical_not(in_group(up))))
                def _():
                    disp_wait(up, j, h)

    def up_copy(d):
        return remote(parts.at[d], in_up.at[d], up_send.at[d], up_recv.at[d], "tp", tp + 1)

    def down_copy(d):
        return remote(parts.at[d], in_down.at[d], down_send.at[d], down_recv.at[d], "tp", tp - 1)

    def up_wait(d):
        ref = in_up.at[d]
        remote(ref, ref, up_send.at[d], up_recv.at[d], "tp", tp - 1).wait_recv()

    def down_wait(d):
        ref = in_down.at[d]
        remote(ref, ref, down_send.at[d], down_recv.at[d], "tp", tp + 1).wait_recv()

    def ret_copy(mask, k):
        rows = pl.ds(0, slot_most)
        return remote(
            stage.at[k, flip(ep, mask)],
            back.at[k, ep, rows, :],
            ret_send.at[mask, k],
            ret_recv.at[mask, k],
            "ep",
            flip(ep, mask),
        )

    def ret_wait(mask, k):
        ref = back.at[k, flip(ep, mask), pl.ds(0, slot_most), :]
        sem = (mask, k)
        remote(ref, ref, ret_send.at[sem], ret_recv.at[sem], "ep", flip(ep, mask)).wait_recv()

    def ids_copy(mask):
        return remote(
            ids_out.at[flip(ep, mask)],
            ids_in.at[ep],
            ids_send_sem.at[mask],
            ids_recv_sem.at[mask],
            "ep",
            flip(ep, mask),
        )

    def ids_wait(mask):
        ref = ids_in.at[flip(ep, mask)]
        remote(
            ref, ref, ids_send_sem.at[mask], ids_recv_sem.at[mask], "ep", flip(ep, mask)
        ).wait_recv()

    loads[0].wait()
    ep_start(0)
    for h in (0, 1):
        line_start(tok_copy, h)

    for s in range(n_exp):
        row = chosen_ref[pl.ds(s, 1), :]
        col = column_of(row.astype(f32), cap).astype(i32)
        chosen_col[s] = col
        gates_col[s] = column_of(gates_ref[pl.ds(s, 1), :], cap)
        row_from = jnp.zeros_like(row)
        col_from = jnp.zeros_like(col)
        for d in range(1, n_ep):
            row_from += jnp.where(row >= d * n_tok, 1, 0)
            col_from += jnp.where(col >= d * n_tok, 1, 0)
        before = jnp.where(col < row_from * n_tok, 1.0, 0.0)
        run_row = jnp.sum(before, axis=0, keepdims=True).astype(i32)
        before = jnp.where(row < col_from * n_tok, 1.0, 0.0)
        run_col = jnp.sum(before, axis=1, keepdims=True).astype(i32)
        lanes = lax.broadcasted_iota(i32, (1, cap), 1)
        rows = lax.broadcasted_iota(i32, (cap, 1), 0)
        place_row[s] = row_from * slot_most + lanes - run_row
        within = rows - run_col

        def slot_ids(d, carry):
            slots = lax.broadcasted_iota(i32, (cap, slot_pad), 1)
            wanted = jnp.where(col_from == d, within, -1)
            value = (col - d * n_tok + 1).astype(f32)
            total = jnp.sum(jnp.where(slots == wanted, value, 0.0), axis=0, keepdims=True)
            ids_out[d, pl.ds(s, 1), :] = total.astype(i32) - 1
            return carry

        lax.fori_loop(0, n_ep, slot_ids, 0)

    def select(e):
        def one(s, carry):
            ids = lax.broadcasted_iota(i32, (cap, n_tok), 1) + e * n_tok
            hits = jnp.where(chosen_col[s] == ids, 1.0, 0.0).astype(bf16)
            acc[s] += jnp.dot(hits, tok_all[e], preferred_element_type=f32)
            return carry

        lax.fori_loop(0, n_exp, one, 0)

    select(ep)
    if n_tp > 2:
        tok_pass(1, 0)
    ep_level(0, ep_levels[0])
    for load in loads[1:4]:
        load.wait()
    for w in (1, 2, 3):
        ep_start(w)
    ep_masks = sorted(range(1, n_ep), key=lambda m: -bin(m >> 1).count("1"))
    for mask in ep_masks:
        ids_copy(mask).start()
    ids_in[ep] = ids_out[ep]
    if n_tp > 2:
        tok_pass(1, 1)
    for mask in ep_levels[0]:
        select(flip(ep, mask))
    if n_tp > 3:
        tok_pass(2, 0)
    for masks in ep_levels[1:]:
        for mask in sorted(masks, key=lambda m: -(m % 2)):
            ep_level(0, [mask])
            select(flip(ep, mask))
    for s in range(n_exp):
        sel[s] = acc[s].astype(bf16)
    disp_start(0)
    own_used = pltpu.make_async_copy(sel.at[slot], columns(used_rows, tp), local_sem.at[8])
    own_used.start()
    acc[...] = jnp.zeros_like(acc)
    if n_tp > 3:
        tok_pass(2, 1)
    for j in range(3, n_tp - 1):
        for h in (0, 1):
            tok_pass(j, h)
    ep_level(1, ep_levels[0])
    disp_start(1)
    for j in range(1, n_tp):
        disp_pass(j, 0)
    ep_level(2, ep_levels[0])
    for j in range(1, n_tp):
        disp_pass(j, 1)
    for mask in ep_masks:
        ids_wait(mask)
    for k in range(n_exp):
        for e in range(n_ep):
            ids = ids_in[e, pl.ds(ret_slot(k), 1), :]
            match = lax.broadcasted_iota(i32, (n_tok, slot_pad), 0) == ids
            picker[k, :, e * slot_pad : (e + 1) * slot_pad] = jnp.where(match, 1.0, 0.0).astype(bf16)
    ep_level(3, ep_levels[0])
    own_used.wait()
    loads[5].wait()
    loads[6].wait()
    for h in parts_of:
        disp_rest(h)
        used = normalise(used_rows[pl.ds(*chunks[h]), :], gain_ref[...])
        contract = (((1,), (1,)), ((), ()))
        gate = lax.dot_general(eg_ref[...], used, contract, preferred_element_type=f32)
        up = lax.dot_general(eu_ref[...], used, contract, preferred_element_type=f32)
        hidden[tp, :, pl.ds(*chunks[h])] = (jax.nn.silu(gate) * up).astype(bf16)
        line_start(hid_copy, h)
    for masks in ep_levels[1:]:
        for w in (1, 2, 3):
            ep_level(w, masks)
    loads[4].wait()
    for h in (0, 1):
        tok_pass(n_tp - 1, h)
    if flat:
        weights = flat
        cols = sg_hbm.shape[1]
        group = 128 // cols
        for ref, out in zip((sg_in, su_in, sd_in), flat):
            for j in range(n_ep // group):
                joined = jnp.concatenate([ref[j * group + i] for i in range(group)], axis=1)
                out[:, j * 128 : (j + 1) * 128] = joined
    else:
        weights = (sg_in, su_in, sd_in)
    sg_ref, su_ref, sd_ref = weights
    chunk = n_tok // 2

    def shared_rows(i, carry):
        rows = pl.ds(pl.multiple_of(i * chunk, chunk), chunk)
        x = normalise(own_rows[rows, :], gain_ref[...])
        contract = (((1,), (1,)), ((), ()))
        gate = lax.dot_general(x, sg_ref[...], contract, preferred_element_type=f32)
        up = lax.dot_general(x, su_ref[...], contract, preferred_element_type=f32)
        mid = (jax.nn.silu(gate) * up).astype(bf16)
        for block in range(n_tp):
            cols = pl.ds(block * width, width)
            parts[block, rows, :] = jnp.dot(
                mid, sd_ref[:, cols], preferred_element_type=f32
            ).astype(bf16)
        return carry

    lax.fori_loop(0, 2, shared_rows, 0)

    def sums_ends(j):
        @pl.when(tp == 0)
        def _():
            up_copy(n_tp - 1 - j).start()

        @pl.when(tp == n_tp - 1)
        def _():
            down_copy(j).start()

    def sums_up(j):
        d = n_tp - 1 - j

        @pl.when(jnp.logical_and(tp > 0, tp < d))
        def _():
            up_wait(d)
            parts[d] = (parts[d].astype(f32) + in_up[d].astype(f32)).astype(bf16)
            up_copy(d).start()

    def sums_down(j):
        @pl.when(jnp.logical_and(tp < n_tp - 1, tp > j))
        def _():
            down_wait(j)
            parts[j] = (parts[j].astype(f32) + in_down[j].astype(f32)).astype(bf16)
            down_copy(j).start()

    def sums_middle(j):
        @pl.when(tp < n_tp // 2)
        def _():
            sums_up(j)
            sums_down(j)

        @pl.when(tp >= n_tp // 2)
        def _():
            sums_down(j)
            sums_up(j)

    def add_block(mask):
        block = flip(tp, mask)
        acc[block // split] += lax.dot_general(
            hidden[block], down_ref[block], (((0,), (0,)), ((), ())), preferred_element_type=f32
        )

    def give_back(k):
        s = ret_slot(k)
        weighted = (gates_col[s] * acc[s]).astype(bf16)
        slots = n_ep * slot_most
        placer = lax.broadcasted_iota(i32, (slots, cap), 0) == place_row[s]
        placer = jnp.where(placer, 1.0, 0.0).astype(bf16)
        placed = jnp.dot(placer, weighted, preferred_element_type=f32)
        stage[k] = placed.reshape(n_ep, slot_most, width).astype(bf16)
        for mask in ep_masks:
            ret_copy(mask, k).start()
        back[k, ep, :slot_most, :] = stage[k, ep]

    loads[7].wait()
    sums_ends(0)
    add_block(0)
    hid_pass(1, 0)
    hid_pass(1, 1)
    for j in range(1, n_tp):
        if j > 1:
            hid_pass(j, 0)
            hid_pass(j, 1)
        add_block(j)
        if (j + 1) % split == 0:
            give_back(j // split)
        if j > 1:
            sums_middle(j - 2)
        if j < n_tp - 1:
            sums_ends(j)
    sums_middle(n_tp - 2)
    acc[0] = parts[tp].astype(f32)

    @pl.when(tp > 0)
    def _():
        up_wait(tp)
        acc[0] += in_up[tp].astype(f32)

    @pl.when(tp < n_tp - 1)
    def _():
        down_wait(tp)
        acc[0] += in_down[tp].astype(f32)

    for k in range(n_exp):
        for mask in ep_masks:
            ret_wait(mask, k)
        value = acc[0] + jnp.dot(
            picker[k], back[k].reshape(n_ep * slot_pad, width), preferred_element_type=f32
        )
        if k < n_exp - 1:
            acc[0] = value
        else:
            out_ref[...] = value.astype(bf16)

    for w in range(4):
        for h in (0, 1):
            for mask in range(n_ep):
                for hop in later_hops(mask, orders[h]):
                    ep_copy(w, h, mask, hop).wait_send()
    for h in parts_of:
        far_each(lambda copy: copy.wait_send(), h)
    for up in (0, 1):
        for j in range(n_tp - 1):

            @pl.when(jnp.logical_and(known(up, j), ahead(up)))
            def _():
                for h in parts_of:
                    tok_copy(up, j, h).wait_send()
                    hid_copy(up, j, h).wait_send()

        for j in range(n_tp):

            @pl.when(jnp.logical_and(known(up, j), in_group(up)))
            def _():
                for h in parts_of:
                    disp_copy(up, j, h).wait_send()

    for mask in ep_masks:
        ids_copy(mask).wait_send()
        for k in range(n_exp):
            ret_copy(mask, k).wait_send()
    for d in range(n_tp):

        @pl.when(tp < d)
        def _():
            up_copy(d).wait_send()

        @pl.when(tp > d)
        def _():
            down_copy(d).wait_send()


def on_device(
    tokens,
    norm_gain,
    shared_gate,
    shared_up,
    shared_down,
    expert_gate,
    expert_up,
    expert_down,
    chosen,
    gates,
):
    n_tp = lax.axis_size("tp")
    n_ep = lax.axis_size("ep")
    n_exp, cap = chosen.shape
    n_tok, width = tokens.shape
    model = n_tp * width
    bf16, f32, i32 = jnp.bfloat16, jnp.float32, jnp.int32
    slot_most = 2 * cap // n_ep
    slot_pad = -(-slot_most // 128) * 128
    n_hid = expert_gate.shape[2]
    sg, su, sd = shared_gate.T, shared_up.T, shared_down
    rows, cols = sg.shape
    if cols % 128 == 0:
        joined, flat = (rows, n_ep * cols), []
    else:
        joined = (n_ep, rows, cols)
        flat = [pltpu.VMEM((rows, n_ep * cols), bf16)] * 3
    vmem = pl.BlockSpec(memory_space=pltpu.VMEM)
    hbm = pl.BlockSpec(memory_space=pl.ANY)
    dma = pltpu.SemaphoreType.DMA
    return pl.pallas_call(
        functools.partial(layer_kernel, n_tp, n_ep, slot_most),
        out_shape=jax.ShapeDtypeStruct((n_tok, width), bf16),
        in_specs=[hbm, vmem] + [hbm] * 6 + [vmem] * 2,
        out_specs=vmem,
        scratch_shapes=[
            pltpu.VMEM((n_ep, n_tok, width), bf16),
            pltpu.VMEM((n_tok, model), bf16),
            pltpu.VMEM((cap, model), bf16),
            pltpu.VMEM((n_exp, cap, width), bf16),
            pltpu.VMEM(joined, bf16),
            pltpu.VMEM(joined, bf16),
            pltpu.VMEM(joined, bf16),
            pltpu.VMEM((n_hid, model), bf16),
            pltpu.VMEM((n_hid, model), bf16),
            pltpu.VMEM((n_tp, n_hid, width), bf16),
            pltpu.VMEM((n_tp, n_hid, cap), bf16),
            pltpu.VMEM((n_exp, cap, width), f32),
            pltpu.VMEM((n_tp, n_tok, width), bf16),
            pltpu.VMEM((n_tp, n_tok, width), bf16),
            pltpu.VMEM((n_tp, n_tok, width), bf16),
            pltpu.VMEM((n_exp, n_ep, slot_most, width), bf16),
            pltpu.VMEM((n_exp, n_ep, slot_pad, width), bf16),
            pltpu.VMEM((n_exp, n_tok, n_ep * slot_pad), bf16),
            pltpu.VMEM((n_ep, 8, slot_pad), i32),
            pltpu.VMEM((n_ep, 8, slot_pad), i32),
            pltpu.VMEM((n_exp, cap, 1), i32),
            pltpu.VMEM((n_exp, cap, 1), f32),
            pltpu.VMEM((n_exp, 1, cap), i32),
            dma((4, 2, n_ep)),
            dma((4, 2, n_ep)),
            dma((2, n_tp, 2)),
            dma((2, n_tp, 2)),
            dma((2, n_tp, 2)),
            dma((n_tp, 2)),
            dma((n_exp, 2)),
            dma((2, n_tp, 2)),
            dma((2, n_tp, 2)),
            dma((n_tp,)),
            dma((n_tp,)),
            dma((n_tp,)),
            dma((n_tp,)),
            dma((n_ep, n_exp)),
            dma((n_ep, n_exp)),
            dma((n_ep,)),
            dma((n_ep,)),
            dma((9,)),
        ]
        + flat,
        compiler_params=pltpu.CompilerParams(
            collective_id=0, has_side_effects=True, vmem_limit_bytes=62 * 1024 * 1024
        ),
    )(
        tokens,
        norm_gain.reshape(1, -1),
        sg,
        su,
        sd,
        expert_gate.reshape(n_hid, model),
        expert_up.reshape(n_hid, model),
        expert_down.reshape(n_tp, n_hid, width),
        chosen,
        gates,
    )


def solution(mesh):
    return jax.shard_map(
        on_device,
        mesh=mesh,
        in_specs=(
            P("ep", "tp"),
            P(),
            P("ep", "tp"),
            P("ep", "tp"),
            P("tp", "ep"),
            P("tp", "ep", None, None),
            P("tp", "ep", None, None),
            P("ep", None, "tp"),
            P("ep", None),
            P("ep", None),
        ),
        out_specs=P("ep", "tp"),
        check_vma=False,
    )
```

```python
import functools

import jax
import jax.numpy as jnp
from jax import lax
from jax.experimental import pallas as pl
from jax.experimental.pallas import tpu as pltpu
from jax.sharding import PartitionSpec as P

norm_eps = 1e-06
MESH = pl.DeviceIdType.MESH


def flip(index, mask):
    bit = 1
    result = index
    while bit <= mask:
        if mask & bit:
            result = result + bit - 2 * bit * ((index // bit) % 2)
        bit *= 2
    return result


def bits_below(count):
    return [1 << i for i in range(count.bit_length() - 1)]


def half_orders(count):
    bits = bits_below(count)
    upper = bits[1:]
    return [upper + bits[:1], upper[::-1] + bits[:1]]


def later_hops(mask, order):
    last = max([i for i, b in enumerate(order) if mask & b], default=-1)
    return order[last + 1 :]


def masks_by_level(count):
    return sorted(range(1, count), key=lambda m: (bin(m).count("1"), -m))


def levels(count):
    found = {}
    for m in masks_by_level(count):
        found.setdefault(bin(m).count("1"), []).append(m)
    return [found[k] for k in sorted(found)]


def column_of(row, count):
    same = lax.broadcasted_iota(jnp.int32, (count, count), 0) == lax.broadcasted_iota(
        jnp.int32, (count, count), 1
    )
    return jnp.sum(jnp.where(same, row, 0.0), axis=1, keepdims=True)


def normalise(rows, gain):
    widened = rows.astype(jnp.float32)
    inv_scale = lax.rsqrt(jnp.mean(widened * widened, axis=1, keepdims=True) + norm_eps)
    return (widened * inv_scale * gain).astype(jnp.bfloat16)


def layer_kernel(
    n_tp,
    n_ep,
    slot_most,
    tok_hbm,
    gain_hbm,
    sg_hbm,
    su_hbm,
    sd_hbm,
    eg_hbm,
    eu_hbm,
    down_hbm,
    chosen_hbm,
    gates_hbm,
    out_hbm,
    out_ref,
    gain_ref,
    chosen_ref,
    gates_ref,
    tok_all,
    own_rows,
    used_rows,
    sel,
    sg_in,
    su_in,
    sd_in,
    eg_ref,
    eu_ref,
    down_ref,
    hidden,
    acc,
    parts,
    in_up,
    in_down,
    stage,
    back,
    picker,
    ids_out,
    ids_in,
    chosen_col,
    gates_col,
    place_row,
    ep_send,
    ep_recv,
    tp_send,
    tp_recv,
    disp_send,
    disp_recv,
    far_send,
    hid_send,
    hid_recv,
    up_send,
    up_recv,
    down_send,
    down_recv,
    ret_send,
    ret_recv,
    ids_send_sem,
    ids_recv_sem,
    local_sem,
    *flat,
):
    tp = lax.axis_index("tp")
    ep = lax.axis_index("ep")
    f32, bf16, i32 = jnp.float32, jnp.bfloat16, jnp.int32
    n_exp, cap = chosen_ref.shape
    n_tok, width = tok_hbm.shape
    n_hid = eg_ref.shape[0]
    slot_pad = back.shape[2]
    split = n_tp // n_exp
    slot = tp // split
    orders = half_orders(n_ep)
    ep_levels = levels(n_ep)
    cut = max(128, cap * 2 // 3 // 128 * 128)
    chunks = [(0, cut), (cut, cap - cut)]
    parts_of = range(len(chunks))

    own_loads = [
        (tok_hbm, tok_all.at[ep]),
        (sg_hbm, sg_in),
        (su_hbm, su_in),
        (sd_hbm, sd_in),
    ]

    def block_of(out, block, rows):
        if len(out.shape) == 3:
            return out.at[block, rows, :]
        cols = out.shape[1] // n_ep
        return out.at[rows, pl.ds(pl.multiple_of(block * cols, cols), cols)]

    def columns(ref, block):
        return ref.at[:, pl.ds(pl.multiple_of(block * width, width), width)]

    loads = []
    for i, (source, target) in enumerate(own_loads):
        if i > 0:
            target = block_of(target, ep, pl.ds(0, source.shape[0]))
        loads.append(pltpu.make_async_copy(source, target, local_sem.at[i]))
    loads.append(pltpu.make_async_copy(tok_hbm, columns(own_rows, tp), local_sem.at[4]))
    for i, (source, target) in enumerate(((eg_hbm, eg_ref), (eu_hbm, eu_ref), (down_hbm, down_ref))):
        loads.append(pltpu.make_async_copy(source, target, local_sem.at[5 + i]))
    small = ((chosen_hbm, chosen_ref), (gates_hbm, gates_ref), (gain_hbm, gain_ref))
    for i, (source, target) in enumerate(small):
        loads.append(pltpu.make_async_copy(source, target, local_sem.at[10 + i]))
    for load in loads:
        load.start()

    barrier = pltpu.get_barrier_semaphore()
    for mask in range(1, n_tp):
        pl.semaphore_signal(barrier, inc=1, device_id={"tp": flip(tp, mask)}, device_id_type=MESH)
    for mask in range(1, n_ep):
        pl.semaphore_signal(barrier, inc=1, device_id={"ep": flip(ep, mask)}, device_id_type=MESH)
    back[...] = jnp.zeros_like(back)
    ids_out[...] = jnp.zeros_like(ids_out)
    acc[...] = jnp.zeros_like(acc)
    pl.semaphore_wait(barrier, n_tp + n_ep - 2)

    def piece(w, block, h):
        half = own_loads[w][0].shape[0] // 2
        rows = pl.ds(h * half, half)
        if w == 0:
            return tok_all.at[block, rows, :]
        return block_of([None, sg_in, su_in, sd_in][w], block, rows)

    def remote(source, target, send, recv, axis, place):
        return pltpu.make_async_remote_copy(
            src_ref=source,
            dst_ref=target,
            send_sem=send,
            recv_sem=recv,
            device_id={axis: place},
            device_id_type=MESH,
        )

    def ep_copy(w, h, mask, hop):
        ref = piece(w, flip(ep, mask), h)
        sem = (w, h, (mask | hop) - 1)
        return remote(ref, ref, ep_send.at[w], ep_recv.at[sem], "ep", flip(ep, hop))

    def ep_wait(w, h, mask):
        hop = [b for b in orders[h] if mask & b][-1]
        ref = piece(w, flip(ep, mask), h)
        sem = (w, h, mask - 1)
        remote(ref, ref, ep_send.at[w], ep_recv.at[sem], "ep", flip(ep, hop)).wait_recv()

    def ep_start(w):
        for position in range(len(orders[0])):
            for h in (0, 1):
                ep_copy(w, h, 0, orders[h][position]).start()

    def ep_level(w, masks):
        for mask in masks:
            for h in (0, 1):
                ep_wait(w, h, mask)
                for hop in later_hops(mask, orders[h]):
                    ep_copy(w, h, mask, hop).start()

    def known(up, j):
        return tp >= j if up else tp < n_tp - j

    def ahead(up):
        return tp < n_tp - 1 if up else tp > 0

    def at_distance(up, j):
        return tp - j if up else tp + j

    def tok_ref(ref, block, h):
        half = n_tok // 2
        cols = pl.ds(pl.multiple_of(block * width, width), width)
        return ref.at[pl.ds(h * half, half), cols]

    def tok_copy(up, j, h):
        ref = tok_ref(own_rows, at_distance(up, j), h)
        source = tok_all.at[ep, pl.ds(h * (n_tok // 2), n_tok // 2), :] if j == 0 else ref
        sem = (up, j, h)
        return remote(
            source, ref, tp_send.at[up], tp_recv.at[sem], "tp", at_distance(1 - up, 1)
        )

    def tok_wait(up, j, h):
        ref = tok_ref(own_rows, at_distance(up, j), h)
        sem = (up, j - 1, h)
        remote(ref, ref, tp_send.at[up], tp_recv.at[sem], "tp", at_distance(up, 1)).wait_recv()

    def hid_copy(up, j, h):
        ref = hidden.at[at_distance(up, j), :, pl.ds(*chunks[h])]
        sem = (up, j, h)
        return remote(
            ref, ref, hid_send.at[up], hid_recv.at[sem], "tp", at_distance(1 - up, 1)
        )

    def hid_wait(up, j, h):
        ref = hidden.at[at_distance(up, j), :, pl.ds(*chunks[h])]
        sem = (up, j - 1, h)
        remote(ref, ref, hid_send.at[up], hid_recv.at[sem], "tp", at_distance(up, 1)).wait_recv()

    def line_start(copy, *rest):
        for up in (0, 1):

            @pl.when(ahead(up))
            def _():
                copy(up, 0, *rest).start()

    def line_pass(copy, wait, j, *rest, side=None):
        for up in (0, 1):
            here = known(up, j)
            if side is not None:
                near = tp < n_tp // 2 if up == side else tp >= n_tp // 2
                here = jnp.logical_and(here, near)

            @pl.when(here)
            def _():
                wait(up, j, *rest)

                @pl.when(ahead(up))
                def _():
                    copy(up, j, *rest).start()

    def hid_pass(j, side):
        for h in parts_of:
            line_pass(hid_copy, hid_wait, j, h, side=side)

    def tok_pass(j, h):
        line_pass(tok_copy, tok_wait, j, h)

    def ret_slot(k):
        return flip(tp, k * split) // split

    low = slot * split
    top = low + split - 1

    def in_group(up):
        return tp < top if up else tp > low

    def used_piece(block, h):
        cols = pl.ds(pl.multiple_of(block * width, width), width)
        return used_rows.at[pl.ds(*chunks[h]), cols]

    def disp_copy(up, j, h):
        block = at_distance(up, j)
        ref = used_piece(block, h)
        source = sel.at[slot, pl.ds(*chunks[h]), :] if j == 0 else ref
        return remote(
            source,
            ref,
            disp_send.at[up],
            disp_recv.at[block, h],
            "tp",
            at_distance(1 - up, 1),
        )

    def disp_wait(up, j, h):
        block = at_distance(up, j)
        ref = used_piece(block, h)
        remote(
            ref, ref, disp_send.at[up], disp_recv.at[block, h], "tp", at_distance(up, 1)
        ).wait_recv()

    def far_copy(k, h, entry):
        return remote(
            sel.at[ret_slot(k), pl.ds(*chunks[h]), :],
            used_piece(tp, h),
            far_send.at[0],
            disp_recv.at[tp, h],
            "tp",
            entry,
        )

    def far_each(act, h):
        for k in range(1, n_exp):
            s = ret_slot(k)

            @pl.when(s > slot)
            def _():
                act(far_copy(k, h, s * split))

            @pl.when(s < slot)
            def _():
                act(far_copy(k, h, s * split + split - 1))

    def disp_start(h):
        far_each(lambda copy: copy.start(), h)
        for up in (0, 1):

            @pl.when(in_group(up))
            def _():
                disp_copy(up, 0, h).start()

    def disp_pass(j, h):
        for up in (0, 1):

            @pl.when(jnp.logical_and(known(up, j), in_group(up)))
            def _():
                disp_wait(up, j, h)
                disp_copy(up, j, h).start()

    def disp_rest(h):
        for j in range(1, n_tp):
            for up in (0, 1):

                @pl.when(jnp.logical_and(known(up, j), jnp.logical_not(in_group(up))))
                def _():
                    disp_wait(up, j, h)

    def up_copy(d):
        return remote(parts.at[d], in_up.at[d], up_send.at[0], up_recv.at[d], "tp", tp + 1)

    def down_copy(d):
        return remote(parts.at[d], in_down.at[d], down_send.at[0], down_recv.at[d], "tp", tp - 1)

    def up_wait(d):
        ref = in_up.at[d]
        remote(ref, ref, up_send.at[0], up_recv.at[d], "tp", tp - 1).wait_recv()

    def down_wait(d):
        ref = in_down.at[d]
        remote(ref, ref, down_send.at[0], down_recv.at[d], "tp", tp + 1).wait_recv()

    def ret_copy(mask, k):
        rows = pl.ds(0, slot_most)
        return remote(
            stage.at[k, flip(ep, mask)],
            back.at[k, ep, rows, :],
            ret_send.at[k],
            ret_recv.at[k],
            "ep",
            flip(ep, mask),
        )

    def local_wait(ref, sem):
        pltpu.make_async_copy(ref, ref, sem).wait()

    def ret_wait(k):
        local_wait(back.at[k, pl.ds(0, n_ep - 1), pl.ds(0, slot_most), :], ret_recv.at[k])

    def ids_copy(mask):
        return remote(
            ids_out.at[flip(ep, mask)],
            ids_in.at[ep],
            ids_send_sem.at[0],
            ids_recv_sem.at[0],
            "ep",
            flip(ep, mask),
        )

    def ids_wait():
        local_wait(ids_in.at[pl.ds(0, n_ep - 1)], ids_recv_sem.at[0])

    loads[0].wait()
    ep_start(0)
    for h in (0, 1):
        line_start(tok_copy, h)

    for load in loads[8:11]:
        load.wait()
    for s in range(n_exp):
        row = chosen_ref[pl.ds(s, 1), :]
        col = column_of(row.astype(f32), cap).astype(i32)
        chosen_col[s] = col
        gates_col[s] = column_of(gates_ref[pl.ds(s, 1), :], cap)
        row_from = jnp.zeros_like(row)
        col_from = jnp.zeros_like(col)
        for d in range(1, n_ep):
            row_from += jnp.where(row >= d * n_tok, 1, 0)
            col_from += jnp.where(col >= d * n_tok, 1, 0)
        before = jnp.where(col < row_from * n_tok, 1.0, 0.0)
        run_row = jnp.sum(before, axis=0, keepdims=True).astype(i32)
        before = jnp.where(row < col_from * n_tok, 1.0, 0.0)
        run_col = jnp.sum(before, axis=1, keepdims=True).astype(i32)
        lanes = lax.broadcasted_iota(i32, (1, cap), 1)
        rows = lax.broadcasted_iota(i32, (cap, 1), 0)
        place_row[s] = row_from * slot_most + lanes - run_row
        within = rows - run_col

        def slot_ids(d, carry):
            slots = lax.broadcasted_iota(i32, (cap, slot_pad), 1)
            wanted = jnp.where(col_from == d, within, -1)
            value = (col - d * n_tok + 1).astype(f32)
            total = jnp.sum(jnp.where(slots == wanted, value, 0.0), axis=0, keepdims=True)
            ids_out[d, pl.ds(s, 1), :] = total.astype(i32) - 1
            return carry

        lax.fori_loop(0, n_ep, slot_ids, 0)

    def select(e):
        def one(s, carry):
            ids = lax.broadcasted_iota(i32, (cap, n_tok), 1) + e * n_tok
            hits = jnp.where(chosen_col[s] == ids, 1.0, 0.0).astype(bf16)
            acc[s] += jnp.dot(hits, tok_all[e], preferred_element_type=f32)
            return carry

        lax.fori_loop(0, n_exp, one, 0)

    select(ep)
    if n_tp > 2:
        tok_pass(1, 0)
    ep_level(0, ep_levels[0])
    for load in loads[1:4]:
        load.wait()
    for w in (1, 2, 3):
        ep_start(w)
    ep_masks = sorted(range(1, n_ep), key=lambda m: -bin(m >> 1).count("1"))
    for mask in ep_masks:
        ids_copy(mask).start()
    ids_in[ep] = ids_out[ep]
    if n_tp > 2:
        tok_pass(1, 1)
    for mask in ep_levels[0]:
        select(flip(ep, mask))
    if n_tp > 3:
        tok_pass(2, 0)
    for masks in ep_levels[1:]:
        for mask in sorted(masks, key=lambda m: -(m % 2)):
            ep_level(0, [mask])
            select(flip(ep, mask))
    for s in range(n_exp):
        sel[s] = acc[s].astype(bf16)
    disp_start(0)
    own_used = pltpu.make_async_copy(sel.at[slot], columns(used_rows, tp), local_sem.at[8])
    own_used.start()
    acc[...] = jnp.zeros_like(acc)
    if n_tp > 3:
        tok_pass(2, 1)
    for j in range(3, n_tp - 1):
        for h in (0, 1):
            tok_pass(j, h)
    ep_level(1, ep_levels[0])
    disp_start(1)
    for j in range(1, n_tp):
        disp_pass(j, 0)
    ep_level(2, ep_levels[0])
    for j in range(1, n_tp):
        disp_pass(j, 1)
    ids_wait()
    for k in range(n_exp):
        for e in range(n_ep):
            ids = ids_in[e, pl.ds(ret_slot(k), 1), :]
            match = lax.broadcasted_iota(i32, (n_tok, slot_pad), 0) == ids
            picker[k, :, e * slot_pad : (e + 1) * slot_pad] = jnp.where(match, 1.0, 0.0).astype(bf16)
    ep_level(3, ep_levels[0])
    own_used.wait()
    loads[5].wait()
    loads[6].wait()
    for h in parts_of:
        disp_rest(h)
        used = normalise(used_rows[pl.ds(*chunks[h]), :], gain_ref[...])
        contract = (((1,), (1,)), ((), ()))
        gate = lax.dot_general(eg_ref[...], used, contract, preferred_element_type=f32)
        up = lax.dot_general(eu_ref[...], used, contract, preferred_element_type=f32)
        hidden[tp, :, pl.ds(*chunks[h])] = (jax.nn.silu(gate) * up).astype(bf16)
        line_start(hid_copy, h)
    for masks in ep_levels[1:]:
        for w in (1, 2, 3):
            ep_level(w, masks)
    loads[4].wait()
    for h in (0, 1):
        tok_pass(n_tp - 1, h)
    if flat:
        weights = flat
        cols = sg_hbm.shape[1]
        group = 128 // cols
        for ref, out in zip((sg_in, su_in, sd_in), flat):
            for j in range(n_ep // group):
                joined = jnp.concatenate([ref[j * group + i] for i in range(group)], axis=1)
                out[:, j * 128 : (j + 1) * 128] = joined
    else:
        weights = (sg_in, su_in, sd_in)
    sg_ref, su_ref, sd_ref = weights
    chunk = n_tok // 2

    def shared_rows(i, carry):
        rows = pl.ds(pl.multiple_of(i * chunk, chunk), chunk)
        x = normalise(own_rows[rows, :], gain_ref[...])
        contract = (((1,), (1,)), ((), ()))
        gate = lax.dot_general(x, sg_ref[...], contract, preferred_element_type=f32)
        up = lax.dot_general(x, su_ref[...], contract, preferred_element_type=f32)
        mid = (jax.nn.silu(gate) * up).astype(bf16)
        for block in range(n_tp):
            cols = pl.ds(block * width, width)
            parts[block, rows, :] = jnp.dot(
                mid, sd_ref[:, cols], preferred_element_type=f32
            ).astype(bf16)
        return carry

    lax.fori_loop(0, 2, shared_rows, 0)

    def sums_ends(j):
        @pl.when(tp == 0)
        def _():
            up_copy(n_tp - 1 - j).start()

        @pl.when(tp == n_tp - 1)
        def _():
            down_copy(j).start()

    def sums_up(j):
        d = n_tp - 1 - j

        @pl.when(jnp.logical_and(tp > 0, tp < d))
        def _():
            up_wait(d)
            parts[d] = (parts[d].astype(f32) + in_up[d].astype(f32)).astype(bf16)
            up_copy(d).start()

    def sums_down(j):
        @pl.when(jnp.logical_and(tp < n_tp - 1, tp > j))
        def _():
            down_wait(j)
            parts[j] = (parts[j].astype(f32) + in_down[j].astype(f32)).astype(bf16)
            down_copy(j).start()

    def sums_middle(j):
        @pl.when(tp < n_tp // 2)
        def _():
            sums_up(j)
            sums_down(j)

        @pl.when(tp >= n_tp // 2)
        def _():
            sums_down(j)
            sums_up(j)

    def add_block(mask):
        block = flip(tp, mask)
        acc[block // split] += lax.dot_general(
            hidden[block], down_ref[block], (((0,), (0,)), ((), ())), preferred_element_type=f32
        )

    def give_back(k):
        s = ret_slot(k)
        weighted = (gates_col[s] * acc[s]).astype(bf16)
        slots = n_ep * slot_most
        placer = lax.broadcasted_iota(i32, (slots, cap), 0) == place_row[s]
        placer = jnp.where(placer, 1.0, 0.0).astype(bf16)
        placed = jnp.dot(placer, weighted, preferred_element_type=f32)
        stage[k] = placed.reshape(n_ep, slot_most, width).astype(bf16)
        for mask in ep_masks:
            ret_copy(mask, k).start()
        back[k, ep, :slot_most, :] = stage[k, ep]

    loads[7].wait()
    sums_ends(0)
    add_block(0)
    hid_pass(1, 0)
    hid_pass(1, 1)
    for j in range(1, n_tp):
        if j > 1:
            hid_pass(j, 0)
            hid_pass(j, 1)
        add_block(j)
        if (j + 1) % split == 0:
            give_back(j // split)
        if j > 1:
            sums_middle(j - 2)
        if j < n_tp - 1:
            sums_ends(j)
    sums_middle(n_tp - 2)
    acc[0] = parts[tp].astype(f32)

    @pl.when(tp > 0)
    def _():
        up_wait(tp)
        acc[0] += in_up[tp].astype(f32)

    @pl.when(tp < n_tp - 1)
    def _():
        down_wait(tp)
        acc[0] += in_down[tp].astype(f32)

    for k in range(n_exp):
        ret_wait(k)
        value = acc[0] + jnp.dot(
            picker[k], back[k].reshape(n_ep * slot_pad, width), preferred_element_type=f32
        )
        if k < n_exp - 1:
            acc[0] = value
        else:
            out_ref[...] = value.astype(bf16)

    result = pltpu.make_async_copy(out_ref, out_hbm, local_sem.at[9])
    result.start()
    for w in range(4):
        if w == 0 or len(sg_in.shape) == 3:
            sent = [tok_all, sg_in, su_in, sd_in][w].at[pl.ds(0, n_ep - 1)]
        else:
            cols = sg_hbm.shape[1] * (n_ep - 1)
            sent = [None, sg_in, su_in, sd_in][w].at[:, pl.ds(0, cols)]
        local_wait(sent, ep_send.at[w])
    local_wait(sel.at[pl.ds(0, n_exp - 1)], far_send.at[0])
    local_wait(ids_out.at[pl.ds(0, n_ep - 1)], ids_send_sem.at[0])
    for k in range(n_exp):
        local_wait(stage.at[k, pl.ds(0, n_ep - 1)], ret_send.at[k])
    for place in range(n_tp):
        for up in (0, 1):
            blocks = place + 1 if up else n_tp - place
            last = n_tp - 1 if up else 0
            if place != last:

                @pl.when(tp == place)
                def _():
                    local_wait(own_rows.at[:, pl.ds(0, blocks * width)], tp_send.at[up])
                    local_wait(hidden.at[pl.ds(0, blocks)], hid_send.at[up])
                    sums = up_send if up else down_send
                    local_wait(parts.at[pl.ds(0, n_tp - blocks)], sums.at[0])

            edge = place % split == (split - 1 if up else 0)
            if not edge:

                @pl.when(tp == place)
                def _():
                    local_wait(used_rows.at[:, pl.ds(0, blocks * width)], disp_send.at[up])

    result.wait()


def on_device(
    tokens,
    norm_gain,
    shared_gate,
    shared_up,
    shared_down,
    expert_gate,
    expert_up,
    expert_down,
    chosen,
    gates,
):
    n_tp = lax.axis_size("tp")
    n_ep = lax.axis_size("ep")
    n_exp, cap = chosen.shape
    n_tok, width = tokens.shape
    model = n_tp * width
    bf16, f32, i32 = jnp.bfloat16, jnp.float32, jnp.int32
    slot_most = 2 * cap // n_ep
    slot_pad = -(-slot_most // 128) * 128
    n_hid = expert_gate.shape[2]
    sg, su, sd = shared_gate.T, shared_up.T, shared_down
    rows, cols = sg.shape
    if cols % 128 == 0:
        joined, flat = (rows, n_ep * cols), []
    else:
        joined = (n_ep, rows, cols)
        flat = [pltpu.VMEM((rows, n_ep * cols), bf16)] * 3
    hbm = pl.BlockSpec(memory_space=pltpu.HBM)
    anywhere = pl.BlockSpec(memory_space=pl.ANY)
    dma = pltpu.SemaphoreType.DMA
    return pl.pallas_call(
        functools.partial(layer_kernel, n_tp, n_ep, slot_most),
        out_shape=jax.ShapeDtypeStruct((n_tok, width), bf16),
        in_specs=[hbm] * 10,
        out_specs=anywhere,
        scratch_shapes=[
            pltpu.VMEM((n_tok, width), bf16),
            pltpu.VMEM((1, model), f32),
            pltpu.VMEM(chosen.shape, i32),
            pltpu.VMEM(gates.shape, f32),
            pltpu.VMEM((n_ep, n_tok, width), bf16),
            pltpu.VMEM((n_tok, model), bf16),
            pltpu.VMEM((cap, model), bf16),
            pltpu.VMEM((n_exp, cap, width), bf16),
            pltpu.VMEM(joined, bf16),
            pltpu.VMEM(joined, bf16),
            pltpu.VMEM(joined, bf16),
            pltpu.VMEM((n_hid, model), bf16),
            pltpu.VMEM((n_hid, model), bf16),
            pltpu.VMEM((n_tp, n_hid, width), bf16),
            pltpu.VMEM((n_tp, n_hid, cap), bf16),
            pltpu.VMEM((n_exp, cap, width), f32),
            pltpu.VMEM((n_tp, n_tok, width), bf16),
            pltpu.VMEM((n_tp, n_tok, width), bf16),
            pltpu.VMEM((n_tp, n_tok, width), bf16),
            pltpu.VMEM((n_exp, n_ep, slot_most, width), bf16),
            pltpu.VMEM((n_exp, n_ep, slot_pad, width), bf16),
            pltpu.VMEM((n_exp, n_tok, n_ep * slot_pad), bf16),
            pltpu.VMEM((n_ep, 8, slot_pad), i32),
            pltpu.VMEM((n_ep, 8, slot_pad), i32),
            pltpu.VMEM((n_exp, cap, 1), i32),
            pltpu.VMEM((n_exp, cap, 1), f32),
            pltpu.VMEM((n_exp, 1, cap), i32),
            dma((4,)),
            dma((4, 2, n_ep - 1)),
            dma((2,)),
            dma((2, n_tp - 1, 2)),
            dma((2,)),
            dma((n_tp, 2)),
            dma((1,)),
            dma((2,)),
            dma((2, n_tp - 1, 2)),
            dma((1,)),
            dma((n_tp,)),
            dma((1,)),
            dma((n_tp,)),
            dma((n_exp,)),
            dma((n_exp,)),
            dma((1,)),
            dma((1,)),
            dma((13,)),
        ]
        + flat,
        compiler_params=pltpu.CompilerParams(
            collective_id=0, has_side_effects=True, vmem_limit_bytes=62 * 1024 * 1024
        ),
    )(
        tokens,
        norm_gain.reshape(1, -1),
        sg,
        su,
        sd,
        expert_gate.reshape(n_hid, model),
        expert_up.reshape(n_hid, model),
        expert_down.reshape(n_tp, n_hid, width),
        chosen,
        gates,
    )


def solution(mesh):
    return jax.shard_map(
        on_device,
        mesh=mesh,
        in_specs=(
            P("ep", "tp"),
            P(),
            P("ep", "tp"),
            P("ep", "tp"),
            P("tp", "ep"),
            P("tp", "ep", None, None),
            P("tp", "ep", None, None),
            P("ep", None, "tp"),
            P("ep", None),
            P("ep", None),
        ),
        out_specs=P("ep", "tp"),
        check_vma=False,
    )
```

```python
import functools

import jax
import jax.numpy as jnp
from jax import lax
from jax.experimental import pallas as pl
from jax.experimental.pallas import tpu as pltpu
from jax.sharding import PartitionSpec as P

norm_eps = 1e-06
MESH = pl.DeviceIdType.MESH


def flip(index, mask):
    bit = 1
    result = index
    while bit <= mask:
        if mask & bit:
            result = result + bit - 2 * bit * ((index // bit) % 2)
        bit *= 2
    return result


def bits_below(count):
    return [1 << i for i in range(count.bit_length() - 1)]


def half_orders(count):
    bits = bits_below(count)
    upper = bits[1:]
    return [upper + bits[:1], upper[::-1] + bits[:1]]


def later_hops(mask, order):
    last = max([i for i, b in enumerate(order) if mask & b], default=-1)
    return order[last + 1 :]


def masks_by_level(count):
    return sorted(range(1, count), key=lambda m: (bin(m).count("1"), -m))


def levels(count):
    found = {}
    for m in masks_by_level(count):
        found.setdefault(bin(m).count("1"), []).append(m)
    return [found[k] for k in sorted(found)]


def column_of(row, count):
    same = lax.broadcasted_iota(jnp.int32, (count, count), 0) == lax.broadcasted_iota(
        jnp.int32, (count, count), 1
    )
    return jnp.sum(jnp.where(same, row, 0.0), axis=1, keepdims=True)


def normalise(rows, gain):
    widened = rows.astype(jnp.float32)
    inv_scale = lax.rsqrt(jnp.mean(widened * widened, axis=1, keepdims=True) + norm_eps)
    return (widened * inv_scale * gain).astype(jnp.bfloat16)


def layer_kernel(
    n_tp,
    n_ep,
    slot_most,
    tok_hbm,
    gain_hbm,
    sg_hbm,
    su_hbm,
    sd_hbm,
    eg_hbm,
    eu_hbm,
    down_hbm,
    chosen_hbm,
    gates_hbm,
    out_hbm,
    out_ref,
    gain_ref,
    chosen_ref,
    gates_ref,
    tok_all,
    own_rows,
    used_rows,
    sel,
    sg_in,
    su_in,
    sd_in,
    eg_ref,
    eu_ref,
    down_ref,
    hidden,
    acc,
    parts,
    in_up,
    in_down,
    stage,
    back,
    picker,
    ids_out,
    ids_in,
    chosen_col,
    gates_col,
    place_row,
    place_col,
    near_out,
    near_in,
    normed,
    ep_send,
    ep_recv,
    tp_send,
    tp_recv,
    disp_send,
    disp_recv,
    far_send,
    hid_send,
    hid_recv,
    up_send,
    up_recv,
    down_send,
    down_recv,
    ret_send,
    ret_recv,
    ids_send_sem,
    ids_recv_sem,
    near_send,
    near_recv,
    local_sem,
    *flat,
):
    tp = lax.axis_index("tp")
    ep = lax.axis_index("ep")
    f32, bf16, i32 = jnp.float32, jnp.bfloat16, jnp.int32
    n_exp, cap = chosen_ref.shape
    n_tok, width = tok_hbm.shape
    n_hid = eg_ref.shape[0]
    slot_pad = back.shape[2]
    split = n_tp // n_exp
    slot = tp // split
    orders = half_orders(n_ep)
    ep_levels = levels(n_ep)
    cut = max(128, cap * 2 // 3 // 128 * 128)
    chunks = [(0, cut), (cut, cap - cut)]
    direct = n_tp == 4 and split == 2
    at_end = jnp.logical_or(tp == 0, tp == n_tp - 1)
    far_end = n_tp - 1 - tp
    part = near_in.shape[2]
    whole = direct and part == width
    parts_of = range(len(chunks))

    own_loads = [
        (tok_hbm, tok_all.at[ep]),
        (sg_hbm, sg_in),
        (su_hbm, su_in),
        (sd_hbm, sd_in),
    ]

    def block_of(out, block, rows):
        if len(out.shape) == 3:
            return out.at[block, rows, :]
        cols = out.shape[1] // n_ep
        return out.at[rows, pl.ds(pl.multiple_of(block * cols, cols), cols)]

    def columns(ref, block):
        return ref.at[:, pl.ds(pl.multiple_of(block * width, width), width)]

    loads = []
    for i, (source, target) in enumerate(own_loads):
        if i > 0:
            target = block_of(target, ep, pl.ds(0, source.shape[0]))
        loads.append(pltpu.make_async_copy(source, target, local_sem.at[i]))
    loads.append(pltpu.make_async_copy(tok_hbm, columns(own_rows, tp), local_sem.at[4]))
    for i, (source, target) in enumerate(((eg_hbm, eg_ref), (eu_hbm, eu_ref), (down_hbm, down_ref))):
        loads.append(pltpu.make_async_copy(source, target, local_sem.at[5 + i]))
    small = ((chosen_hbm, chosen_ref), (gates_hbm, gates_ref), (gain_hbm, gain_ref))
    for i, (source, target) in enumerate(small):
        loads.append(pltpu.make_async_copy(source, target, local_sem.at[10 + i]))
    for load in loads:
        load.start()

    barrier = pltpu.get_barrier_semaphore()
    for mask in range(1, n_tp):
        pl.semaphore_signal(barrier, inc=1, device_id={"tp": flip(tp, mask)}, device_id_type=MESH)
    for mask in range(1, n_ep):
        pl.semaphore_signal(barrier, inc=1, device_id={"ep": flip(ep, mask)}, device_id_type=MESH)
    back[...] = jnp.zeros_like(back)
    ids_out[...] = jnp.zeros_like(ids_out)
    acc[...] = jnp.zeros_like(acc)
    pl.semaphore_wait(barrier, n_tp + n_ep - 2)

    def piece(w, block, h):
        half = own_loads[w][0].shape[0] // 2
        rows = pl.ds(h * half, half)
        if w == 0:
            return tok_all.at[block, rows, :]
        return block_of([None, sg_in, su_in, sd_in][w], block, rows)

    def remote(source, target, send, recv, axis, place):
        return pltpu.make_async_remote_copy(
            src_ref=source,
            dst_ref=target,
            send_sem=send,
            recv_sem=recv,
            device_id={axis: place},
            device_id_type=MESH,
        )

    def ep_copy(w, h, mask, hop):
        ref = piece(w, flip(ep, mask), h)
        sem = (w, h, (mask | hop) - 1)
        return remote(ref, ref, ep_send.at[w], ep_recv.at[sem], "ep", flip(ep, hop))

    def ep_wait(w, h, mask):
        hop = [b for b in orders[h] if mask & b][-1]
        ref = piece(w, flip(ep, mask), h)
        sem = (w, h, mask - 1)
        remote(ref, ref, ep_send.at[w], ep_recv.at[sem], "ep", flip(ep, hop)).wait_recv()

    def ep_start(w):
        for position in range(len(orders[0])):
            for h in (0, 1):
                ep_copy(w, h, 0, orders[h][position]).start()

    def ep_level(w, masks):
        for mask in masks:
            for h in (0, 1):
                ep_wait(w, h, mask)
                for hop in later_hops(mask, orders[h]):
                    ep_copy(w, h, mask, hop).start()

    def known(up, j):
        return tp >= j if up else tp < n_tp - j

    def ahead(up):
        return tp < n_tp - 1 if up else tp > 0

    def at_distance(up, j):
        return tp - j if up else tp + j

    def tok_ref(ref, block, h):
        half = n_tok // 2
        cols = pl.ds(pl.multiple_of(block * width, width), width)
        return ref.at[pl.ds(h * half, half), cols]

    def tok_copy(up, j, h):
        ref = tok_ref(own_rows, at_distance(up, j), h)
        source = tok_all.at[ep, pl.ds(h * (n_tok // 2), n_tok // 2), :] if j == 0 else ref
        sem = (up, j, h)
        return remote(
            source, ref, tp_send.at[up], tp_recv.at[sem], "tp", at_distance(1 - up, 1)
        )

    def tok_wait(up, j, h):
        ref = tok_ref(own_rows, at_distance(up, j), h)
        sem = (up, j - 1, h)
        remote(ref, ref, tp_send.at[up], tp_recv.at[sem], "tp", at_distance(up, 1)).wait_recv()

    def hid_copy(up, j, h):
        ref = hidden.at[at_distance(up, j), :, pl.ds(*chunks[h])]
        sem = (up, j, h)
        return remote(
            ref, ref, hid_send.at[up], hid_recv.at[sem], "tp", at_distance(1 - up, 1)
        )

    def hid_wait(up, j, h):
        ref = hidden.at[at_distance(up, j), :, pl.ds(*chunks[h])]
        sem = (up, j - 1, h)
        remote(ref, ref, hid_send.at[up], hid_recv.at[sem], "tp", at_distance(up, 1)).wait_recv()

    def line_start(copy, *rest):
        for up in (0, 1):

            @pl.when(ahead(up))
            def _():
                copy(up, 0, *rest).start()

    def line_pass(copy, wait, j, *rest, side=None):
        for up in (0, 1):
            here = known(up, j)
            if side is not None:
                near = tp < n_tp // 2 if up == side else tp >= n_tp // 2
                here = jnp.logical_and(here, near)

            @pl.when(here)
            def _():
                wait(up, j, *rest)

                @pl.when(ahead(up))
                def _():
                    copy(up, j, *rest).start()

    def hid_pass(j, side, h):
        line_pass(hid_copy, hid_wait, j, h, side=side)

    def tok_pass(j, h):
        line_pass(tok_copy, tok_wait, j, h)

    def ret_slot(k):
        return flip(tp, k * split) // split

    low = slot * split
    top = low + split - 1

    def in_group(up):
        return tp < top if up else tp > low

    def used_piece(block, h):
        cols = pl.ds(pl.multiple_of(block * width, width), width)
        return used_rows.at[pl.ds(*chunks[h]), cols]

    def rest_piece(block, h):
        cols = pl.ds(pl.multiple_of(block * width + part, 128), width - part)
        return used_rows.at[pl.ds(*chunks[h]), cols]

    def disp_copy(up, j, h):
        block = at_distance(up, j)
        ref = used_piece(block, h)
        if direct and j == n_tp - 2:
            ref = rest_piece(block, h)
        source = sel.at[slot, pl.ds(*chunks[h]), :] if j == 0 else ref
        return remote(
            source,
            ref,
            disp_send.at[up],
            disp_recv.at[block, h],
            "tp",
            at_distance(1 - up, 1),
        )

    def disp_wait(up, j, h):
        block = at_distance(up, j)
        ref = used_piece(block, h)
        if direct and j == n_tp - 1:
            ref = rest_piece(block, h)
        remote(
            ref, ref, disp_send.at[up], disp_recv.at[block, h], "tp", at_distance(up, 1)
        ).wait_recv()

    def far_copy(k, h, entry):
        return remote(
            sel.at[ret_slot(k), pl.ds(*chunks[h]), :],
            used_piece(tp, h),
            far_send.at[0],
            disp_recv.at[tp, h],
            "tp",
            entry,
        )

    def far_each(act, h):
        for k in range(1, n_exp):
            s = ret_slot(k)

            @pl.when(s > slot)
            def _():
                act(far_copy(k, h, s * split))

            @pl.when(s < slot)
            def _():
                act(far_copy(k, h, s * split + split - 1))

    def disp_start(h):
        for up in (0, 1):

            @pl.when(in_group(up))
            def _():
                disp_copy(up, 0, h).start()

    def disp_pass(j, h):
        for up in (0, 1):

            @pl.when(jnp.logical_and(known(up, j), in_group(up)))
            def _():
                disp_wait(up, j, h)
                if not (whole and j == n_tp - 2):
                    disp_copy(up, j, h).start()

    def disp_rest(h):
        for j in range(1, n_tp - 1 if whole else n_tp):
            for up in (0, 1):

                @pl.when(jnp.logical_and(known(up, j), jnp.logical_not(in_group(up))))
                def _():
                    disp_wait(up, j, h)

    def sum_rows(h):
        half = n_tok // 2
        return pl.ds(pl.multiple_of(h * half, half), half)

    def up_copy(d, h):
        rows = (d, sum_rows(h))
        return remote(
            parts.at[rows], in_up.at[rows], up_send.at[0], up_recv.at[d, h], "tp", tp + 1
        )

    def down_copy(d, h):
        rows = (d, sum_rows(h))
        return remote(
            parts.at[rows], in_down.at[rows], down_send.at[0], down_recv.at[d, h], "tp", tp - 1
        )

    def up_wait(d, h):
        ref = in_up.at[d, sum_rows(h)]
        remote(ref, ref, up_send.at[0], up_recv.at[d, h], "tp", tp - 1).wait_recv()

    def down_wait(d, h):
        ref = in_down.at[d, sum_rows(h)]
        remote(ref, ref, down_send.at[0], down_recv.at[d, h], "tp", tp + 1).wait_recv()

    def ret_copy(mask, k):
        rows = pl.ds(0, slot_most)
        return remote(
            stage.at[k, flip(ep, mask)],
            back.at[k, ep, rows, :],
            ret_send.at[k],
            ret_recv.at[k],
            "ep",
            flip(ep, mask),
        )

    def local_wait(ref, sem):
        pltpu.make_async_copy(ref, ref, sem).wait()

    def ret_wait(k):
        local_wait(back.at[k, pl.ds(0, n_ep - 1), pl.ds(0, slot_most), :], ret_recv.at[k])

    def near_copy(mask):
        return remote(
            near_out.at[flip(ep, mask)],
            near_in.at[ep],
            near_send.at[0],
            near_recv.at[0],
            "ep",
            flip(ep, mask),
        )

    def ids_copy(mask):
        return remote(
            ids_out.at[flip(ep, mask)],
            ids_in.at[ep],
            ids_send_sem.at[0],
            ids_recv_sem.at[0],
            "ep",
            flip(ep, mask),
        )

    def ids_wait():
        local_wait(ids_in.at[pl.ds(0, n_ep - 1)], ids_recv_sem.at[0])

    loads[0].wait()
    ep_start(0)
    for h in (0, 1):
        line_start(tok_copy, h)

    for load in loads[8:11]:
        load.wait()
    for s in range(n_exp):
        row = chosen_ref[pl.ds(s, 1), :]
        col = column_of(row.astype(f32), cap).astype(i32)
        chosen_col[s] = col
        gates_col[s] = column_of(gates_ref[pl.ds(s, 1), :], cap)
        row_from = jnp.zeros_like(row)
        col_from = jnp.zeros_like(col)
        for d in range(1, n_ep):
            row_from += jnp.where(row >= d * n_tok, 1, 0)
            col_from += jnp.where(col >= d * n_tok, 1, 0)
        before = jnp.where(col < row_from * n_tok, 1.0, 0.0)
        run_row = jnp.sum(before, axis=0, keepdims=True).astype(i32)
        before = jnp.where(row < col_from * n_tok, 1.0, 0.0)
        run_col = jnp.sum(before, axis=1, keepdims=True).astype(i32)
        lanes = lax.broadcasted_iota(i32, (1, cap), 1)
        rows = lax.broadcasted_iota(i32, (cap, 1), 0)
        place_row[s] = row_from * slot_most + lanes - run_row
        within = rows - run_col
        place_col[s] = col_from * slot_most + within

        def slot_ids(d, carry):
            slots = lax.broadcasted_iota(i32, (cap, slot_pad), 1)
            wanted = jnp.where(col_from == d, within, -1)
            value = (col - d * n_tok + 1).astype(f32)
            total = jnp.sum(jnp.where(slots == wanted, value, 0.0), axis=0, keepdims=True)
            ids_out[d, pl.ds(s, 1), :] = total.astype(i32) - 1
            return carry

        lax.fori_loop(0, n_ep, slot_ids, 0)

    def select(e):
        def one(s, carry):
            ids = lax.broadcasted_iota(i32, (cap, n_tok), 1) + e * n_tok
            hits = jnp.where(chosen_col[s] == ids, 1.0, 0.0).astype(bf16)
            acc[s] += jnp.dot(hits, tok_all[e], preferred_element_type=f32)
            return carry

        lax.fori_loop(0, n_exp, one, 0)

    ep_masks = sorted(range(1, n_ep), key=lambda m: -bin(m >> 1).count("1"))
    for mask in ep_masks:
        ids_copy(mask).start()
    ids_in[ep] = ids_out[ep]
    select(ep)
    if n_tp > 2:
        tok_pass(1, 0)
    def pick(k):
        for e in range(n_ep):
            ids = ids_in[e, pl.ds(ret_slot(k), 1), :]
            match = lax.broadcasted_iota(i32, (n_tok, slot_pad), 0) == ids
            picker[k, :, e * slot_pad : (e + 1) * slot_pad] = jnp.where(match, 1.0, 0.0).astype(bf16)

    ids_wait()
    pick(0)
    ep_level(0, ep_levels[0])
    for load in loads[1:4]:
        load.wait()
    ep_start(1)
    held = at_end if direct else tp < 0

    @pl.when(jnp.logical_not(held))
    def _():
        ep_start(2)
        ep_start(3)

    if n_tp > 2:
        tok_pass(1, 1)
    for mask in ep_levels[0]:
        select(flip(ep, mask))
    if n_tp > 3:
        tok_pass(2, 0)
    for masks in ep_levels[1:]:
        for mask in sorted(masks, key=lambda m: -(m % 2)):
            ep_level(0, [mask])
            select(flip(ep, mask))
    for s in range(n_exp):
        sel[s] = acc[s].astype(bf16)
    if n_tp > 3:
        tok_pass(2, 1)
    far_each(lambda copy: copy.start(), 0)
    own_used = pltpu.make_async_copy(sel.at[slot], columns(used_rows, tp), local_sem.at[8])
    own_used.start()
    acc[...] = jnp.zeros_like(acc)
    for j in range(3, n_tp - 1):
        for h in (0, 1):
            tok_pass(j, h)
    ep_level(1, ep_levels[0])

    @pl.when(held)
    def _():
        ep_start(2)

    far_each(lambda copy: copy.start(), 1)
    for h in parts_of:
        disp_start(h)
    for j in range(1, n_tp):
        disp_pass(j, 0)
    if direct:

        @pl.when(at_end)
        def _():
            for h in (0, 1):
                tok_pass(n_tp - 1, h)
            cols = pl.ds(pl.multiple_of(far_end * width, width), part)
            rows = lax.dot_general(
                picker[0], own_rows[:, cols], (((0,), (0,)), ((), ())), preferred_element_type=f32
            )
            near_out[...] = rows.reshape(n_ep, slot_pad, part)[:, :slot_most, :].astype(bf16)
            for mask in ep_masks:
                near_copy(mask).start()
            near_in[ep] = near_out[ep]


    @pl.when(held)
    def _():
        ep_start(3)

    ep_level(2, ep_levels[0])
    for j in range(1, n_tp):
        disp_pass(j, 1)
    for k in range(1, n_exp):
        pick(k)
    @pl.when(jnp.logical_not(held))
    def _():
        ep_level(3, ep_levels[0])

    if direct:

        @pl.when(at_end)
        def _():
            local_wait(near_in.at[pl.ds(0, n_ep - 1)], near_recv.at[0])
            slots = n_ep * slot_most
            match = lax.broadcasted_iota(i32, (cap, slots), 1) == place_col[slot]
            rows = jnp.dot(
                jnp.where(match, 1.0, 0.0).astype(bf16),
                near_in[...].reshape(slots, part),
                preferred_element_type=f32,
            )
            cols = pl.ds(pl.multiple_of(far_end * width, width), part)
            used_rows[:, cols] = rows.astype(bf16)

    own_used.wait()
    loads[5].wait()
    loads[6].wait()
    for h in parts_of:
        disp_rest(h)
        used = normalise(used_rows[pl.ds(*chunks[h]), :], gain_ref[...])
        contract = (((1,), (1,)), ((), ()))
        gate = lax.dot_general(eg_ref[...], used, contract, preferred_element_type=f32)
        up = lax.dot_general(eu_ref[...], used, contract, preferred_element_type=f32)
        hidden[tp, :, pl.ds(*chunks[h])] = (jax.nn.silu(gate) * up).astype(bf16)
        line_start(hid_copy, h)
    loads[4].wait()
    if not direct:
        for h in (0, 1):
            tok_pass(n_tp - 1, h)
    def norm_rows(i, carry):
        rows = sum_rows(i)
        normed[rows, :] = normalise(own_rows[rows, :], gain_ref[...])
        return carry

    lax.fori_loop(0, 2, norm_rows, 0)
    @pl.when(held)
    def _():
        ep_level(3, ep_levels[0])

    for masks in ep_levels[1:]:
        for w in (1, 2, 3):
            ep_level(w, masks)
    if flat:
        weights = flat
        cols = sg_hbm.shape[1]
        group = 128 // cols
        for ref, out in zip((sg_in, su_in, sd_in), flat):
            for j in range(n_ep // group):
                joined = jnp.concatenate([ref[j * group + i] for i in range(group)], axis=1)
                out[:, j * 128 : (j + 1) * 128] = joined
    else:
        weights = (sg_in, su_in, sd_in)
    sg_ref, su_ref, sd_ref = weights
    chunk = n_tok // 2

    def sums_first(h):
        @pl.when(tp == 0)
        def _():
            up_copy(n_tp - 1, h).start()

        @pl.when(tp == n_tp - 1)
        def _():
            down_copy(0, h).start()


    def shared_rows(i, carry):
        rows = pl.ds(pl.multiple_of(i * chunk, chunk), chunk)
        x = normed[rows, :]
        contract = (((1,), (1,)), ((), ()))
        gate = lax.dot_general(x, sg_ref[...], contract, preferred_element_type=f32)
        up = lax.dot_general(x, su_ref[...], contract, preferred_element_type=f32)
        mid = (jax.nn.silu(gate) * up).astype(bf16)
        for block in range(n_tp):
            cols = pl.ds(block * width, width)
            parts[block, rows, :] = jnp.dot(
                mid, sd_ref[:, cols], preferred_element_type=f32
            ).astype(bf16)
        sums_first(i)
        return carry

    lax.fori_loop(0, 2, shared_rows, 0)

    def sums_ends(j):
        @pl.when(tp == 0)
        def _():
            for h in (0, 1):
                up_copy(n_tp - 1 - j, h).start()

        @pl.when(tp == n_tp - 1)
        def _():
            for h in (0, 1):
                down_copy(j, h).start()

    def sums_up(j):
        d = n_tp - 1 - j

        @pl.when(jnp.logical_and(tp > 0, tp < d))
        def _():
            for h in (0, 1):
                rows = sum_rows(h)
                up_wait(d, h)
                parts[d, rows] = (parts[d, rows].astype(f32) + in_up[d, rows].astype(f32)).astype(bf16)
                up_copy(d, h).start()

    def sums_down(j):
        @pl.when(jnp.logical_and(tp < n_tp - 1, tp > j))
        def _():
            for h in (0, 1):
                rows = sum_rows(h)
                down_wait(j, h)
                parts[j, rows] = (parts[j, rows].astype(f32) + in_down[j, rows].astype(f32)).astype(bf16)
                down_copy(j, h).start()

    def sums_outer(j):
        @pl.when(tp < n_tp // 2)
        def _():
            sums_up(j)

        @pl.when(tp >= n_tp // 2)
        def _():
            sums_down(j)

    def sums_inner(j):
        @pl.when(tp < n_tp // 2)
        def _():
            sums_down(j)

        @pl.when(tp >= n_tp // 2)
        def _():
            sums_up(j)

    def add_block(mask, h):
        block = flip(tp, mask)
        rows = pl.ds(*chunks[h])
        acc[block // split, rows, :] += lax.dot_general(
            hidden[block, :, rows],
            down_ref[block],
            (((0,), (0,)), ((), ())),
            preferred_element_type=f32,
        )

    def give_back(k):
        s = ret_slot(k)
        weighted = (gates_col[s] * acc[s]).astype(bf16)
        slots = n_ep * slot_most
        placer = lax.broadcasted_iota(i32, (slots, cap), 0) == place_row[s]
        placer = jnp.where(placer, 1.0, 0.0).astype(bf16)
        placed = jnp.dot(placer, weighted, preferred_element_type=f32)
        stage[k] = placed.reshape(n_ep, slot_most, width).astype(bf16)
        for mask in ep_masks:
            ret_copy(mask, k).start()
        back[k, ep, :slot_most, :] = stage[k, ep]

    loads[7].wait()
    for h in parts_of:
        add_block(0, h)
    for h in parts_of:
        hid_pass(1, 0, h)
    for h in parts_of:
        hid_pass(1, 1, h)
    for j in range(1, n_tp):
        if j > 1:
            for h in parts_of:
                hid_pass(j, 0, h)
                hid_pass(j, 1, h)
                add_block(j, h)
        if j == 1:
            for h in parts_of:
                add_block(j, h)
        if (j + 1) % split == 0:
            give_back(j // split)
        if j > 1:
            sums_outer(j - 2)
        if j < n_tp - 1:
            sums_ends(j)
    sums_outer(n_tp - 2)
    for j in range(n_tp - 1):
        sums_inner(j)
    acc[0] = parts[tp].astype(f32)

    @pl.when(tp > 0)
    def _():
        for h in (0, 1):
            up_wait(tp, h)
        acc[0] += in_up[tp].astype(f32)

    @pl.when(tp < n_tp - 1)
    def _():
        for h in (0, 1):
            down_wait(tp, h)
        acc[0] += in_down[tp].astype(f32)

    for k in range(n_exp):
        ret_wait(k)
        for h in (0, 1):
            rows = sum_rows(h)
            value = acc[0, rows, :] + jnp.dot(
                picker[k, rows, :],
                back[k].reshape(n_ep * slot_pad, width),
                preferred_element_type=f32,
            )
            if k < n_exp - 1:
                acc[0, rows, :] = value
            else:
                out_ref[rows, :] = value.astype(bf16)
                result = pltpu.make_async_copy(
                    out_ref.at[rows, :], out_hbm.at[rows, :], local_sem.at[8 + h]
                )
                result.start()

    for w in range(4):
        if w == 0 or len(sg_in.shape) == 3:
            sent = [tok_all, sg_in, su_in, sd_in][w].at[pl.ds(0, n_ep - 1)]
        else:
            cols = sg_hbm.shape[1] * (n_ep - 1)
            sent = [None, sg_in, su_in, sd_in][w].at[:, pl.ds(0, cols)]
        local_wait(sent, ep_send.at[w])
    local_wait(sel.at[pl.ds(0, n_exp - 1)], far_send.at[0])
    if direct:

        @pl.when(at_end)
        def _():
            local_wait(near_out.at[pl.ds(0, n_ep - 1)], near_send.at[0])

    local_wait(ids_out.at[pl.ds(0, n_ep - 1)], ids_send_sem.at[0])
    for k in range(n_exp):
        local_wait(stage.at[k, pl.ds(0, n_ep - 1)], ret_send.at[k])
    for place in range(n_tp):
        for up in (0, 1):
            blocks = place + 1 if up else n_tp - place
            last = n_tp - 1 if up else 0
            if place != last:

                @pl.when(tp == place)
                def _():
                    local_wait(own_rows.at[:, pl.ds(0, blocks * width)], tp_send.at[up])
                    local_wait(hidden.at[pl.ds(0, blocks)], hid_send.at[up])
                    sums = up_send if up else down_send
                    local_wait(parts.at[pl.ds(0, n_tp - blocks)], sums.at[0])

            edge = place % split == (split - 1 if up else 0)
            if not edge:

                @pl.when(tp == place)
                def _():
                    sent = blocks * width
                    if direct and place == (n_tp - 2 if up else 1):
                        sent = sent - part
                    local_wait(used_rows.at[:, pl.ds(0, sent)], disp_send.at[up])

    for h in (0, 1):
        rows = sum_rows(h)
        pltpu.make_async_copy(
            out_ref.at[rows, :], out_hbm.at[rows, :], local_sem.at[8 + h]
        ).wait()


def on_device(
    tokens,
    norm_gain,
    shared_gate,
    shared_up,
    shared_down,
    expert_gate,
    expert_up,
    expert_down,
    chosen,
    gates,
):
    n_tp = lax.axis_size("tp")
    n_ep = lax.axis_size("ep")
    n_exp, cap = chosen.shape
    n_tok, width = tokens.shape
    model = n_tp * width
    bf16, f32, i32 = jnp.bfloat16, jnp.float32, jnp.int32
    slot_most = 2 * cap // n_ep
    slot_pad = -(-slot_most // 128) * 128
    n_hid = expert_gate.shape[2]
    near = width
    sg, su, sd = shared_gate.T, shared_up.T, shared_down
    rows, cols = sg.shape
    if cols % 128 == 0:
        joined, flat = (rows, n_ep * cols), []
    else:
        joined = (n_ep, rows, cols)
        flat = [pltpu.VMEM((rows, n_ep * cols), bf16)] * 3
    hbm = pl.BlockSpec(memory_space=pltpu.HBM)
    anywhere = pl.BlockSpec(memory_space=pl.ANY)
    dma = pltpu.SemaphoreType.DMA
    return pl.pallas_call(
        functools.partial(layer_kernel, n_tp, n_ep, slot_most),
        out_shape=jax.ShapeDtypeStruct((n_tok, width), bf16),
        in_specs=[hbm] * 10,
        out_specs=anywhere,
        scratch_shapes=[
            pltpu.VMEM((n_tok, width), bf16),
            pltpu.VMEM((1, model), f32),
            pltpu.VMEM(chosen.shape, i32),
            pltpu.VMEM(gates.shape, f32),
            pltpu.VMEM((n_ep, n_tok, width), bf16),
            pltpu.VMEM((n_tok, model), bf16),
            pltpu.VMEM((cap, model), bf16),
            pltpu.VMEM((n_exp, cap, width), bf16),
            pltpu.VMEM(joined, bf16),
            pltpu.VMEM(joined, bf16),
            pltpu.VMEM(joined, bf16),
            pltpu.VMEM((n_hid, model), bf16),
            pltpu.VMEM((n_hid, model), bf16),
            pltpu.VMEM((n_tp, n_hid, width), bf16),
            pltpu.VMEM((n_tp, n_hid, cap), bf16),
            pltpu.VMEM((n_exp, cap, width), f32),
            pltpu.VMEM((n_tp, n_tok, width), bf16),
            pltpu.VMEM((n_tp, n_tok, width), bf16),
            pltpu.VMEM((n_tp, n_tok, width), bf16),
            pltpu.VMEM((n_exp, n_ep, slot_most, width), bf16),
            pltpu.VMEM((n_exp, n_ep, slot_pad, width), bf16),
            pltpu.VMEM((n_exp, n_tok, n_ep * slot_pad), bf16),
            pltpu.VMEM((n_ep, 8, slot_pad), i32),
            pltpu.VMEM((n_ep, 8, slot_pad), i32),
            pltpu.VMEM((n_exp, cap, 1), i32),
            pltpu.VMEM((n_exp, cap, 1), f32),
            pltpu.VMEM((n_exp, 1, cap), i32),
            pltpu.VMEM((n_exp, cap, 1), i32),
            pltpu.VMEM((n_ep, slot_most, near), bf16),
            pltpu.VMEM((n_ep, slot_most, near), bf16),
            pltpu.VMEM((n_tok, model), bf16),
            dma((4,)),
            dma((4, 2, n_ep - 1)),
            dma((2,)),
            dma((2, n_tp - 1, 2)),
            dma((2,)),
            dma((n_tp, 2)),
            dma((1,)),
            dma((2,)),
            dma((2, n_tp - 1, 2)),
            dma((1,)),
            dma((n_tp, 2)),
            dma((1,)),
            dma((n_tp, 2)),
            dma((n_exp,)),
            dma((n_exp,)),
            dma((1,)),
            dma((1,)),
            dma((1,)),
            dma((1,)),
            dma((13,)),
        ]
        + flat,
        compiler_params=pltpu.CompilerParams(
            collective_id=0, has_side_effects=True, vmem_limit_bytes=62 * 1024 * 1024
        ),
    )(
        tokens,
        norm_gain.reshape(1, -1),
        sg,
        su,
        sd,
        expert_gate.reshape(n_hid, model),
        expert_up.reshape(n_hid, model),
        expert_down.reshape(n_tp, n_hid, width),
        chosen,
        gates,
    )


def solution(mesh):
    return jax.shard_map(
        on_device,
        mesh=mesh,
        in_specs=(
            P("ep", "tp"),
            P(),
            P("ep", "tp"),
            P("ep", "tp"),
            P("tp", "ep"),
            P("tp", "ep", None, None),
            P("tp", "ep", None, None),
            P("ep", None, "tp"),
            P("ep", None),
            P("ep", None),
        ),
        out_specs=P("ep", "tp"),
        check_vma=False,
    )
```

```python
import functools

import jax
import jax.numpy as jnp
from jax import lax
from jax.experimental import pallas as pl
from jax.experimental.pallas import tpu as pltpu
from jax.sharding import PartitionSpec as P

norm_eps = 1e-06
MESH = pl.DeviceIdType.MESH


def flip(index, mask):
    bit = 1
    result = index
    while bit <= mask:
        if mask & bit:
            result = result + bit - 2 * bit * ((index // bit) % 2)
        bit *= 2
    return result


def bits_below(count):
    return [1 << i for i in range(count.bit_length() - 1)]


def half_orders(count):
    bits = bits_below(count)
    upper = bits[1:]
    return [upper + bits[:1], upper[::-1] + bits[:1]]


def later_hops(mask, order):
    last = max([i for i, b in enumerate(order) if mask & b], default=-1)
    return order[last + 1 :]


def masks_by_level(count):
    return sorted(range(1, count), key=lambda m: (bin(m).count("1"), -m))


def levels(count):
    found = {}
    for m in masks_by_level(count):
        found.setdefault(bin(m).count("1"), []).append(m)
    return [found[k] for k in sorted(found)]


def column_of(row, count):
    same = lax.broadcasted_iota(jnp.int32, (count, count), 0) == lax.broadcasted_iota(
        jnp.int32, (count, count), 1
    )
    return jnp.sum(jnp.where(same, row, 0.0), axis=1, keepdims=True)


def normalise(rows, gain):
    widened = rows.astype(jnp.float32)
    inv_scale = lax.rsqrt(jnp.mean(widened * widened, axis=1, keepdims=True) + norm_eps)
    return (widened * inv_scale * gain).astype(jnp.bfloat16)


def layer_kernel(
    n_tp,
    n_ep,
    slot_most,
    tok_hbm,
    gain_hbm,
    sg_hbm,
    su_hbm,
    sd_hbm,
    eg_hbm,
    eu_hbm,
    down_hbm,
    chosen_hbm,
    gates_hbm,
    out_hbm,
    out_ref,
    gain_ref,
    chosen_ref,
    gates_ref,
    tok_all,
    own_rows,
    used_rows,
    sel,
    sg_in,
    su_in,
    sd_in,
    eg_ref,
    eu_ref,
    down_ref,
    hidden,
    acc,
    parts,
    in_up,
    in_down,
    stage,
    back,
    picker,
    ids_out,
    ids_in,
    chosen_col,
    gates_col,
    place_row,
    place_col,
    near_out,
    near_in,
    normed,
    mid_ref,
    ep_send,
    ep_recv,
    tp_send,
    tp_recv,
    disp_send,
    disp_recv,
    far_send,
    hid_send,
    hid_recv,
    up_send,
    up_recv,
    down_send,
    down_recv,
    ret_send,
    ret_recv,
    ids_send_sem,
    ids_recv_sem,
    near_send,
    near_recv,
    local_sem,
    *flat,
):
    tp = lax.axis_index("tp")
    ep = lax.axis_index("ep")
    f32, bf16, i32 = jnp.float32, jnp.bfloat16, jnp.int32
    n_exp, cap = chosen_ref.shape
    n_tok, width = tok_hbm.shape
    n_hid = eg_ref.shape[0]
    slot_pad = back.shape[2]
    split = n_tp // n_exp
    slot = tp // split
    orders = half_orders(n_ep)
    ep_levels = levels(n_ep)
    cut = max(128, cap * 2 // 3 // 128 * 128)
    chunks = [(0, cut), (cut, cap - cut)]
    direct = n_tp == 4 and split == 2
    at_end = jnp.logical_or(tp == 0, tp == n_tp - 1)
    far_end = n_tp - 1 - tp
    part = near_in.shape[2]
    whole = direct and part == width
    parts_of = range(len(chunks))

    own_loads = [
        (tok_hbm, tok_all.at[ep]),
        (sg_hbm, sg_in),
        (su_hbm, su_in),
        (sd_hbm, sd_in),
    ]

    def block_of(out, block, rows):
        if len(out.shape) == 3:
            return out.at[block, rows, :]
        cols = out.shape[1] // n_ep
        return out.at[rows, pl.ds(pl.multiple_of(block * cols, cols), cols)]

    def columns(ref, block):
        return ref.at[:, pl.ds(pl.multiple_of(block * width, width), width)]

    loads = []
    for i, (source, target) in enumerate(own_loads):
        if i > 0:
            target = block_of(target, ep, pl.ds(0, source.shape[0]))
        loads.append(pltpu.make_async_copy(source, target, local_sem.at[i]))
    loads.append(pltpu.make_async_copy(tok_hbm, columns(own_rows, tp), local_sem.at[4]))
    for i, (source, target) in enumerate(((eg_hbm, eg_ref), (eu_hbm, eu_ref), (down_hbm, down_ref))):
        loads.append(pltpu.make_async_copy(source, target, local_sem.at[5 + i]))
    small = ((chosen_hbm, chosen_ref), (gates_hbm, gates_ref), (gain_hbm, gain_ref))
    for i, (source, target) in enumerate(small):
        loads.append(pltpu.make_async_copy(source, target, local_sem.at[10 + i]))
    for load in loads:
        load.start()

    barrier = pltpu.get_barrier_semaphore()
    for mask in range(1, n_tp):
        pl.semaphore_signal(barrier, inc=1, device_id={"tp": flip(tp, mask)}, device_id_type=MESH)
    for mask in range(1, n_ep):
        pl.semaphore_signal(barrier, inc=1, device_id={"ep": flip(ep, mask)}, device_id_type=MESH)
    back[...] = jnp.zeros_like(back)
    ids_out[...] = jnp.zeros_like(ids_out)
    acc[...] = jnp.zeros_like(acc)
    pl.semaphore_wait(barrier, n_tp + n_ep - 2)

    def piece(w, block, h):
        half = own_loads[w][0].shape[0] // 2
        rows = pl.ds(h * half, half)
        if w == 0:
            return tok_all.at[block, rows, :]
        return block_of([None, sg_in, su_in, sd_in][w], block, rows)

    def remote(source, target, send, recv, axis, place):
        return pltpu.make_async_remote_copy(
            src_ref=source,
            dst_ref=target,
            send_sem=send,
            recv_sem=recv,
            device_id={axis: place},
            device_id_type=MESH,
        )

    def ep_copy(w, h, mask, hop):
        ref = piece(w, flip(ep, mask), h)
        sem = (w, h, (mask | hop) - 1)
        return remote(ref, ref, ep_send.at[w], ep_recv.at[sem], "ep", flip(ep, hop))

    def ep_wait(w, h, mask):
        hop = [b for b in orders[h] if mask & b][-1]
        ref = piece(w, flip(ep, mask), h)
        sem = (w, h, mask - 1)
        remote(ref, ref, ep_send.at[w], ep_recv.at[sem], "ep", flip(ep, hop)).wait_recv()

    def ep_start(w):
        for position in range(len(orders[0])):
            for h in (0, 1):
                ep_copy(w, h, 0, orders[h][position]).start()

    def ep_level(w, masks):
        for mask in masks:
            for h in (0, 1):
                ep_wait(w, h, mask)
                for hop in later_hops(mask, orders[h]):
                    ep_copy(w, h, mask, hop).start()

    def known(up, j):
        return tp >= j if up else tp < n_tp - j

    def ahead(up):
        return tp < n_tp - 1 if up else tp > 0

    def at_distance(up, j):
        return tp - j if up else tp + j

    def tok_ref(ref, block, h):
        half = n_tok // 2
        cols = pl.ds(pl.multiple_of(block * width, width), width)
        return ref.at[pl.ds(h * half, half), cols]

    def tok_copy(up, j, h):
        ref = tok_ref(own_rows, at_distance(up, j), h)
        source = tok_all.at[ep, pl.ds(h * (n_tok // 2), n_tok // 2), :] if j == 0 else ref
        sem = (up, j, h)
        return remote(
            source, ref, tp_send.at[up], tp_recv.at[sem], "tp", at_distance(1 - up, 1)
        )

    def tok_wait(up, j, h):
        ref = tok_ref(own_rows, at_distance(up, j), h)
        sem = (up, j - 1, h)
        remote(ref, ref, tp_send.at[up], tp_recv.at[sem], "tp", at_distance(up, 1)).wait_recv()

    def hid_copy(up, j, h):
        ref = hidden.at[at_distance(up, j), :, pl.ds(*chunks[h])]
        sem = (up, j, h)
        return remote(
            ref, ref, hid_send.at[up], hid_recv.at[sem], "tp", at_distance(1 - up, 1)
        )

    def hid_wait(up, j, h):
        ref = hidden.at[at_distance(up, j), :, pl.ds(*chunks[h])]
        sem = (up, j - 1, h)
        remote(ref, ref, hid_send.at[up], hid_recv.at[sem], "tp", at_distance(up, 1)).wait_recv()

    def line_start(copy, *rest):
        for up in (0, 1):

            @pl.when(ahead(up))
            def _():
                copy(up, 0, *rest).start()

    def line_pass(copy, wait, j, *rest, side=None):
        for up in (0, 1):
            here = known(up, j)
            if side is not None:
                near = tp < n_tp // 2 if up == side else tp >= n_tp // 2
                here = jnp.logical_and(here, near)

            @pl.when(here)
            def _():
                wait(up, j, *rest)

                @pl.when(ahead(up))
                def _():
                    copy(up, j, *rest).start()

    def hid_pass(j, side, h):
        line_pass(hid_copy, hid_wait, j, h, side=side)

    def tok_pass(j, h):
        line_pass(tok_copy, tok_wait, j, h)

    def ret_slot(k):
        return flip(tp, k * split) // split

    low = slot * split
    top = low + split - 1

    def in_group(up):
        return tp < top if up else tp > low

    def used_piece(block, h):
        cols = pl.ds(pl.multiple_of(block * width, width), width)
        return used_rows.at[pl.ds(*chunks[h]), cols]

    def rest_piece(block, h):
        cols = pl.ds(pl.multiple_of(block * width + part, 128), width - part)
        return used_rows.at[pl.ds(*chunks[h]), cols]

    def disp_copy(up, j, h):
        block = at_distance(up, j)
        ref = used_piece(block, h)
        if direct and j == n_tp - 2:
            ref = rest_piece(block, h)
        source = sel.at[slot, pl.ds(*chunks[h]), :] if j == 0 else ref
        return remote(
            source,
            ref,
            disp_send.at[up],
            disp_recv.at[block, h],
            "tp",
            at_distance(1 - up, 1),
        )

    def disp_wait(up, j, h):
        block = at_distance(up, j)
        ref = used_piece(block, h)
        if direct and j == n_tp - 1:
            ref = rest_piece(block, h)
        remote(
            ref, ref, disp_send.at[up], disp_recv.at[block, h], "tp", at_distance(up, 1)
        ).wait_recv()

    def far_copy(k, h, entry):
        return remote(
            sel.at[ret_slot(k), pl.ds(*chunks[h]), :],
            used_piece(tp, h),
            far_send.at[0],
            disp_recv.at[tp, h],
            "tp",
            entry,
        )

    def far_each(act, h):
        for k in range(1, n_exp):
            s = ret_slot(k)

            @pl.when(s > slot)
            def _():
                act(far_copy(k, h, s * split))

            @pl.when(s < slot)
            def _():
                act(far_copy(k, h, s * split + split - 1))

    def disp_start(h):
        for up in (0, 1):

            @pl.when(in_group(up))
            def _():
                disp_copy(up, 0, h).start()

    def disp_pass(j, h):
        for up in (0, 1):

            @pl.when(jnp.logical_and(known(up, j), in_group(up)))
            def _():
                disp_wait(up, j, h)
                if not (whole and j == n_tp - 2):
                    disp_copy(up, j, h).start()

    def disp_rest(h):
        for j in range(1, n_tp - 1 if whole else n_tp):
            for up in (0, 1):

                @pl.when(jnp.logical_and(known(up, j), jnp.logical_not(in_group(up))))
                def _():
                    disp_wait(up, j, h)

    def sum_rows(h):
        half = n_tok // 2
        return pl.ds(pl.multiple_of(h * half, half), half)

    def up_copy(d, h):
        rows = (d, sum_rows(h))
        return remote(
            parts.at[rows], in_up.at[rows], up_send.at[0], up_recv.at[d, h], "tp", tp + 1
        )

    def down_copy(d, h):
        rows = (d, sum_rows(h))
        return remote(
            parts.at[rows], in_down.at[rows], down_send.at[0], down_recv.at[d, h], "tp", tp - 1
        )

    def up_wait(d, h):
        ref = in_up.at[d, sum_rows(h)]
        remote(ref, ref, up_send.at[0], up_recv.at[d, h], "tp", tp - 1).wait_recv()

    def down_wait(d, h):
        ref = in_down.at[d, sum_rows(h)]
        remote(ref, ref, down_send.at[0], down_recv.at[d, h], "tp", tp + 1).wait_recv()

    def ret_copy(mask, k):
        rows = pl.ds(0, slot_most)
        return remote(
            stage.at[k, flip(ep, mask)],
            back.at[k, ep, rows, :],
            ret_send.at[k],
            ret_recv.at[k],
            "ep",
            flip(ep, mask),
        )

    def local_wait(ref, sem):
        pltpu.make_async_copy(ref, ref, sem).wait()

    def ret_wait(k):
        local_wait(back.at[k, pl.ds(0, n_ep - 1), pl.ds(0, slot_most), :], ret_recv.at[k])

    def near_copy(mask):
        return remote(
            near_out.at[flip(ep, mask)],
            near_in.at[ep],
            near_send.at[0],
            near_recv.at[0],
            "ep",
            flip(ep, mask),
        )

    def ids_copy(mask):
        return remote(
            ids_out.at[flip(ep, mask)],
            ids_in.at[ep],
            ids_send_sem.at[0],
            ids_recv_sem.at[0],
            "ep",
            flip(ep, mask),
        )

    def ids_wait():
        local_wait(ids_in.at[pl.ds(0, n_ep - 1)], ids_recv_sem.at[0])

    loads[0].wait()
    ep_start(0)
    for h in (0, 1):
        line_start(tok_copy, h)

    for load in loads[8:11]:
        load.wait()
    for s in range(n_exp):
        row = chosen_ref[pl.ds(s, 1), :]
        col = column_of(row.astype(f32), cap).astype(i32)
        chosen_col[s] = col
        gates_col[s] = column_of(gates_ref[pl.ds(s, 1), :], cap)
        row_from = jnp.zeros_like(row)
        col_from = jnp.zeros_like(col)
        for d in range(1, n_ep):
            row_from += jnp.where(row >= d * n_tok, 1, 0)
            col_from += jnp.where(col >= d * n_tok, 1, 0)
        before = jnp.where(col < row_from * n_tok, 1.0, 0.0)
        run_row = jnp.sum(before, axis=0, keepdims=True).astype(i32)
        before = jnp.where(row < col_from * n_tok, 1.0, 0.0)
        run_col = jnp.sum(before, axis=1, keepdims=True).astype(i32)
        lanes = lax.broadcasted_iota(i32, (1, cap), 1)
        rows = lax.broadcasted_iota(i32, (cap, 1), 0)
        place_row[s] = row_from * slot_most + lanes - run_row
        within = rows - run_col
        place_col[s] = col_from * slot_most + within

        def slot_ids(d, carry):
            slots = lax.broadcasted_iota(i32, (cap, slot_pad), 1)
            wanted = jnp.where(col_from == d, within, -1)
            value = (col - d * n_tok + 1).astype(f32)
            total = jnp.sum(jnp.where(slots == wanted, value, 0.0), axis=0, keepdims=True)
            ids_out[d, pl.ds(s, 1), :] = total.astype(i32) - 1
            return carry

        lax.fori_loop(0, n_ep, slot_ids, 0)

    def select(e):
        def one(s, carry):
            ids = lax.broadcasted_iota(i32, (cap, n_tok), 1) + e * n_tok
            hits = jnp.where(chosen_col[s] == ids, 1.0, 0.0).astype(bf16)
            acc[s] += jnp.dot(hits, tok_all[e], preferred_element_type=f32)
            return carry

        lax.fori_loop(0, n_exp, one, 0)

    ep_masks = sorted(range(1, n_ep), key=lambda m: -bin(m >> 1).count("1"))
    for mask in ep_masks:
        ids_copy(mask).start()
    ids_in[ep] = ids_out[ep]
    select(ep)
    if n_tp > 2:
        tok_pass(1, 0)
    def pick(k):
        for e in range(n_ep):
            ids = ids_in[e, pl.ds(ret_slot(k), 1), :]
            match = lax.broadcasted_iota(i32, (n_tok, slot_pad), 0) == ids
            picker[k, :, e * slot_pad : (e + 1) * slot_pad] = jnp.where(match, 1.0, 0.0).astype(bf16)

    ids_wait()
    pick(0)
    ep_level(0, ep_levels[0])
    for load in loads[1:4]:
        load.wait()
    ep_start(1)
    held = at_end if direct else tp < 0

    ep_start(2)

    @pl.when(jnp.logical_not(held))
    def _():
        ep_start(3)

    if n_tp > 2:
        tok_pass(1, 1)
    for mask in ep_levels[0]:
        select(flip(ep, mask))
    if n_tp > 3:
        tok_pass(2, 0)
    for masks in ep_levels[1:]:
        for mask in sorted(masks, key=lambda m: -(m % 2)):
            ep_level(0, [mask])
            select(flip(ep, mask))
    for s in range(n_exp):
        sel[s] = acc[s].astype(bf16)
    if n_tp > 3:
        tok_pass(2, 1)
    far_each(lambda copy: copy.start(), 0)
    own_used = pltpu.make_async_copy(sel.at[slot], columns(used_rows, tp), local_sem.at[8])
    own_used.start()
    acc[...] = jnp.zeros_like(acc)
    for j in range(3, n_tp - 1):
        for h in (0, 1):
            tok_pass(j, h)
    ep_level(1, ep_levels[0])

    far_each(lambda copy: copy.start(), 1)
    for h in parts_of:
        disp_start(h)
    for j in range(1, n_tp):
        disp_pass(j, 0)
    if direct:

        @pl.when(at_end)
        def _():
            for h in (0, 1):
                tok_pass(n_tp - 1, h)
            cols = pl.ds(pl.multiple_of(far_end * width, width), part)
            rows = lax.dot_general(
                picker[0], own_rows[:, cols], (((0,), (0,)), ((), ())), preferred_element_type=f32
            )
            near_out[...] = rows.reshape(n_ep, slot_pad, part)[:, :slot_most, :].astype(bf16)
            for mask in ep_masks:
                near_copy(mask).start()
            near_in[ep] = near_out[ep]


    @pl.when(held)
    def _():
        ep_start(3)

    ep_level(2, ep_levels[0])
    for j in range(1, n_tp):
        disp_pass(j, 1)
    for k in range(1, n_exp):
        pick(k)
    @pl.when(jnp.logical_not(held))
    def _():
        ep_level(3, ep_levels[0])

    if direct:

        @pl.when(at_end)
        def _():
            local_wait(near_in.at[pl.ds(0, n_ep - 1)], near_recv.at[0])
            slots = n_ep * slot_most
            match = lax.broadcasted_iota(i32, (cap, slots), 1) == place_col[slot]
            rows = jnp.dot(
                jnp.where(match, 1.0, 0.0).astype(bf16),
                near_in[...].reshape(slots, part),
                preferred_element_type=f32,
            )
            cols = pl.ds(pl.multiple_of(far_end * width, width), part)
            used_rows[:, cols] = rows.astype(bf16)

    own_used.wait()
    loads[5].wait()
    loads[6].wait()
    for h in parts_of:
        disp_rest(h)
        used = normalise(used_rows[pl.ds(*chunks[h]), :], gain_ref[...])
        contract = (((1,), (1,)), ((), ()))
        gate = lax.dot_general(eg_ref[...], used, contract, preferred_element_type=f32)
        up = lax.dot_general(eu_ref[...], used, contract, preferred_element_type=f32)
        hidden[tp, :, pl.ds(*chunks[h])] = (jax.nn.silu(gate) * up).astype(bf16)
        line_start(hid_copy, h)
    loads[4].wait()
    if not direct:
        for h in (0, 1):
            tok_pass(n_tp - 1, h)
    def norm_rows(i, carry):
        rows = sum_rows(i)
        normed[rows, :] = normalise(own_rows[rows, :], gain_ref[...])
        return carry

    lax.fori_loop(0, 2, norm_rows, 0)
    @pl.when(held)
    def _():
        ep_level(3, ep_levels[0])

    for masks in ep_levels[1:]:
        for w in (1, 2):
            ep_level(w, masks)
    def join(k):
        if not flat:
            return (sg_in, su_in, sd_in)[k]
        group = 128 // sg_hbm.shape[1]
        blocks, out = (sg_in, su_in, sd_in)[k], flat[k]
        for j in range(n_ep // group):
            joined = jnp.concatenate([blocks[j * group + i] for i in range(group)], axis=1)
            out[:, j * 128 : (j + 1) * 128] = joined
        return out

    sg_ref, su_ref = join(0), join(1)

    def shared_up(i, carry):
        rows = sum_rows(i)
        x = normed[rows, :]
        contract = (((1,), (1,)), ((), ()))
        gate = lax.dot_general(x, sg_ref[...], contract, preferred_element_type=f32)
        up = lax.dot_general(x, su_ref[...], contract, preferred_element_type=f32)
        mid_ref[rows, :] = (jax.nn.silu(gate) * up).astype(bf16)
        return carry

    lax.fori_loop(0, 2, shared_up, 0)
    for masks in ep_levels[1:]:
        ep_level(3, masks)
    sd_ref = join(2)

    def sums_first(h):
        @pl.when(tp == 0)
        def _():
            up_copy(n_tp - 1, h).start()

        @pl.when(tp == n_tp - 1)
        def _():
            down_copy(0, h).start()


    def shared_rows(i, carry):
        rows = sum_rows(i)
        mid = mid_ref[rows, :]
        for block in range(n_tp):
            cols = pl.ds(block * width, width)
            parts[block, rows, :] = jnp.dot(
                mid, sd_ref[:, cols], preferred_element_type=f32
            ).astype(bf16)
        sums_first(i)
        return carry

    lax.fori_loop(0, 2, shared_rows, 0)

    def sums_ends(j):
        @pl.when(tp == 0)
        def _():
            for h in (0, 1):
                up_copy(n_tp - 1 - j, h).start()

        @pl.when(tp == n_tp - 1)
        def _():
            for h in (0, 1):
                down_copy(j, h).start()

    def sums_up(j):
        d = n_tp - 1 - j

        @pl.when(jnp.logical_and(tp > 0, tp < d))
        def _():
            for h in (0, 1):
                rows = sum_rows(h)
                up_wait(d, h)
                parts[d, rows] = (parts[d, rows].astype(f32) + in_up[d, rows].astype(f32)).astype(bf16)
                up_copy(d, h).start()

    def sums_down(j):
        @pl.when(jnp.logical_and(tp < n_tp - 1, tp > j))
        def _():
            for h in (0, 1):
                rows = sum_rows(h)
                down_wait(j, h)
                parts[j, rows] = (parts[j, rows].astype(f32) + in_down[j, rows].astype(f32)).astype(bf16)
                down_copy(j, h).start()

    def sums_outer(j):
        @pl.when(tp < n_tp // 2)
        def _():
            sums_up(j)

        @pl.when(tp >= n_tp // 2)
        def _():
            sums_down(j)

    def sums_inner(j):
        @pl.when(tp < n_tp // 2)
        def _():
            sums_down(j)

        @pl.when(tp >= n_tp // 2)
        def _():
            sums_up(j)

    def add_block(mask, h):
        block = flip(tp, mask)
        rows = pl.ds(*chunks[h])
        acc[block // split, rows, :] += lax.dot_general(
            hidden[block, :, rows],
            down_ref[block],
            (((0,), (0,)), ((), ())),
            preferred_element_type=f32,
        )

    def give_back(k):
        s = ret_slot(k)
        weighted = (gates_col[s] * acc[s]).astype(bf16)
        slots = n_ep * slot_most
        placer = lax.broadcasted_iota(i32, (slots, cap), 0) == place_row[s]
        placer = jnp.where(placer, 1.0, 0.0).astype(bf16)
        placed = jnp.dot(placer, weighted, preferred_element_type=f32)
        stage[k] = placed.reshape(n_ep, slot_most, width).astype(bf16)
        for mask in ep_masks:
            ret_copy(mask, k).start()
        back[k, ep, :slot_most, :] = stage[k, ep]

    loads[7].wait()
    for h in parts_of:
        add_block(0, h)
    for h in parts_of:
        hid_pass(1, 0, h)
    for h in parts_of:
        hid_pass(1, 1, h)
    for j in range(1, n_tp):
        if j > 1:
            for h in parts_of:
                hid_pass(j, 0, h)
                hid_pass(j, 1, h)
                add_block(j, h)
        if j == 1:
            for h in parts_of:
                add_block(j, h)
        if (j + 1) % split == 0:
            give_back(j // split)
        if j > 1:
            sums_outer(j - 2)
        if j < n_tp - 1:
            sums_ends(j)
    sums_outer(n_tp - 2)
    for j in range(n_tp - 1):
        sums_inner(j)
    acc[0] = parts[tp].astype(f32)

    @pl.when(tp > 0)
    def _():
        for h in (0, 1):
            up_wait(tp, h)
        acc[0] += in_up[tp].astype(f32)

    @pl.when(tp < n_tp - 1)
    def _():
        for h in (0, 1):
            down_wait(tp, h)
        acc[0] += in_down[tp].astype(f32)

    for k in range(n_exp):
        ret_wait(k)
        for h in (0, 1):
            rows = sum_rows(h)
            value = acc[0, rows, :] + jnp.dot(
                picker[k, rows, :],
                back[k].reshape(n_ep * slot_pad, width),
                preferred_element_type=f32,
            )
            if k < n_exp - 1:
                acc[0, rows, :] = value
            else:
                out_ref[rows, :] = value.astype(bf16)
                result = pltpu.make_async_copy(
                    out_ref.at[rows, :], out_hbm.at[rows, :], local_sem.at[8 + h]
                )
                result.start()

    for w in range(4):
        if w == 0 or len(sg_in.shape) == 3:
            sent = [tok_all, sg_in, su_in, sd_in][w].at[pl.ds(0, n_ep - 1)]
        else:
            cols = sg_hbm.shape[1] * (n_ep - 1)
            sent = [None, sg_in, su_in, sd_in][w].at[:, pl.ds(0, cols)]
        local_wait(sent, ep_send.at[w])
    local_wait(sel.at[pl.ds(0, n_exp - 1)], far_send.at[0])
    if direct:

        @pl.when(at_end)
        def _():
            local_wait(near_out.at[pl.ds(0, n_ep - 1)], near_send.at[0])

    local_wait(ids_out.at[pl.ds(0, n_ep - 1)], ids_send_sem.at[0])
    for k in range(n_exp):
        local_wait(stage.at[k, pl.ds(0, n_ep - 1)], ret_send.at[k])
    for place in range(n_tp):
        for up in (0, 1):
            blocks = place + 1 if up else n_tp - place
            last = n_tp - 1 if up else 0
            if place != last:

                @pl.when(tp == place)
                def _():
                    local_wait(own_rows.at[:, pl.ds(0, blocks * width)], tp_send.at[up])
                    local_wait(hidden.at[pl.ds(0, blocks)], hid_send.at[up])
                    sums = up_send if up else down_send
                    local_wait(parts.at[pl.ds(0, n_tp - blocks)], sums.at[0])

            edge = place % split == (split - 1 if up else 0)
            if not edge:

                @pl.when(tp == place)
                def _():
                    sent = blocks * width
                    if direct and place == (n_tp - 2 if up else 1):
                        sent = sent - part
                    local_wait(used_rows.at[:, pl.ds(0, sent)], disp_send.at[up])

    for h in (0, 1):
        rows = sum_rows(h)
        pltpu.make_async_copy(
            out_ref.at[rows, :], out_hbm.at[rows, :], local_sem.at[8 + h]
        ).wait()


def on_device(
    tokens,
    norm_gain,
    shared_gate,
    shared_up,
    shared_down,
    expert_gate,
    expert_up,
    expert_down,
    chosen,
    gates,
):
    n_tp = lax.axis_size("tp")
    n_ep = lax.axis_size("ep")
    n_exp, cap = chosen.shape
    n_tok, width = tokens.shape
    model = n_tp * width
    bf16, f32, i32 = jnp.bfloat16, jnp.float32, jnp.int32
    slot_most = 2 * cap // n_ep
    slot_pad = -(-slot_most // 128) * 128
    n_hid = expert_gate.shape[2]
    near = width
    sg, su, sd = shared_gate.T, shared_up.T, shared_down
    rows, cols = sg.shape
    if cols % 128 == 0:
        joined, flat = (rows, n_ep * cols), []
    else:
        joined = (n_ep, rows, cols)
        flat = [pltpu.VMEM((rows, n_ep * cols), bf16)] * 3
    hbm = pl.BlockSpec(memory_space=pltpu.HBM)
    anywhere = pl.BlockSpec(memory_space=pl.ANY)
    dma = pltpu.SemaphoreType.DMA
    return pl.pallas_call(
        functools.partial(layer_kernel, n_tp, n_ep, slot_most),
        out_shape=jax.ShapeDtypeStruct((n_tok, width), bf16),
        in_specs=[hbm] * 10,
        out_specs=anywhere,
        scratch_shapes=[
            pltpu.VMEM((n_tok, width), bf16),
            pltpu.VMEM((1, model), f32),
            pltpu.VMEM(chosen.shape, i32),
            pltpu.VMEM(gates.shape, f32),
            pltpu.VMEM((n_ep, n_tok, width), bf16),
            pltpu.VMEM((n_tok, model), bf16),
            pltpu.VMEM((cap, model), bf16),
            pltpu.VMEM((n_exp, cap, width), bf16),
            pltpu.VMEM(joined, bf16),
            pltpu.VMEM(joined, bf16),
            pltpu.VMEM(joined, bf16),
            pltpu.VMEM((n_hid, model), bf16),
            pltpu.VMEM((n_hid, model), bf16),
            pltpu.VMEM((n_tp, n_hid, width), bf16),
            pltpu.VMEM((n_tp, n_hid, cap), bf16),
            pltpu.VMEM((n_exp, cap, width), f32),
            pltpu.VMEM((n_tp, n_tok, width), bf16),
            pltpu.VMEM((n_tp, n_tok, width), bf16),
            pltpu.VMEM((n_tp, n_tok, width), bf16),
            pltpu.VMEM((n_exp, n_ep, slot_most, width), bf16),
            pltpu.VMEM((n_exp, n_ep, slot_pad, width), bf16),
            pltpu.VMEM((n_exp, n_tok, n_ep * slot_pad), bf16),
            pltpu.VMEM((n_ep, 8, slot_pad), i32),
            pltpu.VMEM((n_ep, 8, slot_pad), i32),
            pltpu.VMEM((n_exp, cap, 1), i32),
            pltpu.VMEM((n_exp, cap, 1), f32),
            pltpu.VMEM((n_exp, 1, cap), i32),
            pltpu.VMEM((n_exp, cap, 1), i32),
            pltpu.VMEM((n_ep, slot_most, near), bf16),
            pltpu.VMEM((n_ep, slot_most, near), bf16),
            pltpu.VMEM((n_tok, model), bf16),
            pltpu.VMEM((n_tok, rows), bf16),
            dma((4,)),
            dma((4, 2, n_ep - 1)),
            dma((2,)),
            dma((2, n_tp - 1, 2)),
            dma((2,)),
            dma((n_tp, 2)),
            dma((1,)),
            dma((2,)),
            dma((2, n_tp - 1, 2)),
            dma((1,)),
            dma((n_tp, 2)),
            dma((1,)),
            dma((n_tp, 2)),
            dma((n_exp,)),
            dma((n_exp,)),
            dma((1,)),
            dma((1,)),
            dma((1,)),
            dma((1,)),
            dma((13,)),
        ]
        + flat,
        compiler_params=pltpu.CompilerParams(
            collective_id=0, has_side_effects=True, vmem_limit_bytes=62 * 1024 * 1024
        ),
    )(
        tokens,
        norm_gain.reshape(1, -1),
        sg,
        su,
        sd,
        expert_gate.reshape(n_hid, model),
        expert_up.reshape(n_hid, model),
        expert_down.reshape(n_tp, n_hid, width),
        chosen,
        gates,
    )


def solution(mesh):
    return jax.shard_map(
        on_device,
        mesh=mesh,
        in_specs=(
            P("ep", "tp"),
            P(),
            P("ep", "tp"),
            P("ep", "tp"),
            P("tp", "ep"),
            P("tp", "ep", None, None),
            P("tp", "ep", None, None),
            P("ep", None, "tp"),
            P("ep", None),
            P("ep", None),
        ),
        out_specs=P("ep", "tp"),
        check_vma=False,
    )
```

```python
import functools

import jax
import jax.numpy as jnp
from jax import lax
from jax.experimental import pallas as pl
from jax.experimental.pallas import tpu as pltpu
from jax.sharding import PartitionSpec as P

norm_eps = 1e-06
MESH = pl.DeviceIdType.MESH


def flip(index, mask):
    bit = 1
    result = index
    while bit <= mask:
        if mask & bit:
            result = result + bit - 2 * bit * ((index // bit) % 2)
        bit *= 2
    return result


def bits_below(count):
    return [1 << i for i in range(count.bit_length() - 1)]


def half_orders(count):
    bits = bits_below(count)
    upper = bits[1:]
    return [upper + bits[:1], upper[::-1] + bits[:1]]


def later_hops(mask, order):
    last = max([i for i, b in enumerate(order) if mask & b], default=-1)
    return order[last + 1 :]


def masks_by_level(count):
    return sorted(range(1, count), key=lambda m: (bin(m).count("1"), -m))


def levels(count):
    found = {}
    for m in masks_by_level(count):
        found.setdefault(bin(m).count("1"), []).append(m)
    return [found[k] for k in sorted(found)]


def column_of(row, count):
    same = lax.broadcasted_iota(jnp.int32, (count, count), 0) == lax.broadcasted_iota(
        jnp.int32, (count, count), 1
    )
    return jnp.sum(jnp.where(same, row, 0.0), axis=1, keepdims=True)


def normalise(rows, gain):
    widened = rows.astype(jnp.float32)
    inv_scale = lax.rsqrt(jnp.mean(widened * widened, axis=1, keepdims=True) + norm_eps)
    return (widened * inv_scale * gain).astype(jnp.bfloat16)


def layer_kernel(
    n_tp,
    n_ep,
    slot_most,
    tok_hbm,
    gain_hbm,
    sg_hbm,
    su_hbm,
    sd_hbm,
    eg_hbm,
    eu_hbm,
    down_hbm,
    chosen_hbm,
    gates_hbm,
    out_hbm,
    out_ref,
    gain_ref,
    chosen_ref,
    gates_ref,
    tok_all,
    own_rows,
    used_rows,
    sel,
    sg_in,
    su_in,
    sd_in,
    eg_ref,
    eu_ref,
    down_ref,
    hidden,
    acc,
    parts,
    in_up,
    in_down,
    stage,
    back,
    picker,
    ids_out,
    ids_in,
    chosen_col,
    gates_col,
    place_row,
    place_col,
    near_out,
    near_in,
    normed,
    mid_ref,
    ep_send,
    ep_recv,
    tp_send,
    tp_recv,
    disp_send,
    disp_recv,
    far_send,
    hid_send,
    hid_recv,
    up_send,
    up_recv,
    down_send,
    down_recv,
    ret_send,
    ret_recv,
    ids_send_sem,
    ids_recv_sem,
    near_send,
    near_recv,
    local_sem,
    *flat,
):
    tp = lax.axis_index("tp")
    ep = lax.axis_index("ep")
    f32, bf16, i32 = jnp.float32, jnp.bfloat16, jnp.int32
    n_exp, cap = chosen_ref.shape
    n_tok, width = tok_hbm.shape
    n_hid = eg_ref.shape[0]
    slot_pad = back.shape[2]
    split = n_tp // n_exp
    slot = tp // split
    orders = half_orders(n_ep)
    ep_levels = levels(n_ep)
    cut = max(128, cap * 2 // 3 // 128 * 128)
    chunks = [(0, cut), (cut, cap - cut)]
    direct = n_tp == 4 and split == 2
    at_end = jnp.logical_or(tp == 0, tp == n_tp - 1)
    far_end = n_tp - 1 - tp
    part = near_in.shape[2]
    whole = direct and part == width
    parts_of = range(len(chunks))

    own_loads = [
        (tok_hbm, tok_all.at[ep]),
        (sg_hbm, sg_in),
        (su_hbm, su_in),
        (sd_hbm, sd_in),
    ]

    def block_of(out, block, rows):
        if len(out.shape) == 3:
            return out.at[block, rows, :]
        cols = out.shape[1] // n_ep
        return out.at[rows, pl.ds(pl.multiple_of(block * cols, cols), cols)]

    def columns(ref, block):
        return ref.at[:, pl.ds(pl.multiple_of(block * width, width), width)]

    loads = []
    for i, (source, target) in enumerate(own_loads):
        if i > 0:
            target = block_of(target, ep, pl.ds(0, source.shape[0]))
        loads.append(pltpu.make_async_copy(source, target, local_sem.at[i]))
    loads.append(pltpu.make_async_copy(tok_hbm, columns(own_rows, tp), local_sem.at[4]))
    for i, (source, target) in enumerate(((eg_hbm, eg_ref), (eu_hbm, eu_ref), (down_hbm, down_ref))):
        loads.append(pltpu.make_async_copy(source, target, local_sem.at[5 + i]))
    small = ((chosen_hbm, chosen_ref), (gates_hbm, gates_ref), (gain_hbm, gain_ref))
    for i, (source, target) in enumerate(small):
        loads.append(pltpu.make_async_copy(source, target, local_sem.at[10 + i]))
    for load in loads:
        load.start()

    barrier = pltpu.get_barrier_semaphore()
    for mask in range(1, n_tp):
        pl.semaphore_signal(barrier, inc=1, device_id={"tp": flip(tp, mask)}, device_id_type=MESH)
    for mask in range(1, n_ep):
        pl.semaphore_signal(barrier, inc=1, device_id={"ep": flip(ep, mask)}, device_id_type=MESH)
    back[...] = jnp.zeros_like(back)
    ids_out[...] = jnp.zeros_like(ids_out)
    acc[...] = jnp.zeros_like(acc)
    pl.semaphore_wait(barrier, n_tp + n_ep - 2)

    def piece(w, block, h):
        half = own_loads[w][0].shape[0] // 2
        rows = pl.ds(h * half, half)
        if w == 0:
            return tok_all.at[block, rows, :]
        return block_of([None, sg_in, su_in, sd_in][w], block, rows)

    def remote(source, target, send, recv, axis, place):
        return pltpu.make_async_remote_copy(
            src_ref=source,
            dst_ref=target,
            send_sem=send,
            recv_sem=recv,
            device_id={axis: place},
            device_id_type=MESH,
        )

    def ep_copy(w, h, mask, hop):
        ref = piece(w, flip(ep, mask), h)
        sem = (w, h, (mask | hop) - 1)
        return remote(ref, ref, ep_send.at[w], ep_recv.at[sem], "ep", flip(ep, hop))

    def ep_wait(w, h, mask):
        hop = [b for b in orders[h] if mask & b][-1]
        ref = piece(w, flip(ep, mask), h)
        sem = (w, h, mask - 1)
        remote(ref, ref, ep_send.at[w], ep_recv.at[sem], "ep", flip(ep, hop)).wait_recv()

    def ep_start(w):
        for position in range(len(orders[0])):
            for h in (0, 1):
                ep_copy(w, h, 0, orders[h][position]).start()

    def ep_level(w, masks):
        for mask in masks:
            for h in (0, 1):
                ep_wait(w, h, mask)
                for hop in later_hops(mask, orders[h]):
                    ep_copy(w, h, mask, hop).start()

    def known(up, j):
        return tp >= j if up else tp < n_tp - j

    def ahead(up):
        return tp < n_tp - 1 if up else tp > 0

    def at_distance(up, j):
        return tp - j if up else tp + j

    def tok_ref(ref, block, h):
        half = n_tok // 2
        cols = pl.ds(pl.multiple_of(block * width, width), width)
        return ref.at[pl.ds(h * half, half), cols]

    def tok_copy(up, j, h):
        ref = tok_ref(own_rows, at_distance(up, j), h)
        source = tok_all.at[ep, pl.ds(h * (n_tok // 2), n_tok // 2), :] if j == 0 else ref
        sem = (up, j, h)
        return remote(
            source, ref, tp_send.at[up], tp_recv.at[sem], "tp", at_distance(1 - up, 1)
        )

    def tok_wait(up, j, h):
        ref = tok_ref(own_rows, at_distance(up, j), h)
        sem = (up, j - 1, h)
        remote(ref, ref, tp_send.at[up], tp_recv.at[sem], "tp", at_distance(up, 1)).wait_recv()

    def hid_copy(up, j, h):
        ref = hidden.at[at_distance(up, j), :, pl.ds(*chunks[h])]
        sem = (up, j, h)
        return remote(
            ref, ref, hid_send.at[up], hid_recv.at[sem], "tp", at_distance(1 - up, 1)
        )

    def hid_wait(up, j, h):
        ref = hidden.at[at_distance(up, j), :, pl.ds(*chunks[h])]
        sem = (up, j - 1, h)
        remote(ref, ref, hid_send.at[up], hid_recv.at[sem], "tp", at_distance(up, 1)).wait_recv()

    def line_start(copy, *rest):
        for up in (0, 1):

            @pl.when(ahead(up))
            def _():
                copy(up, 0, *rest).start()

    def line_pass(copy, wait, j, *rest, side=None):
        for up in (0, 1):
            here = known(up, j)
            if side is not None:
                near = tp < n_tp // 2 if up == side else tp >= n_tp // 2
                here = jnp.logical_and(here, near)

            @pl.when(here)
            def _():
                wait(up, j, *rest)

                @pl.when(ahead(up))
                def _():
                    copy(up, j, *rest).start()

    def hid_pass(j, side, h):
        line_pass(hid_copy, hid_wait, j, h, side=side)

    def tok_pass(j, h):
        line_pass(tok_copy, tok_wait, j, h)

    def ret_slot(k):
        return flip(tp, k * split) // split

    low = slot * split
    top = low + split - 1

    def in_group(up):
        return tp < top if up else tp > low

    def used_piece(block, h):
        cols = pl.ds(pl.multiple_of(block * width, width), width)
        return used_rows.at[pl.ds(*chunks[h]), cols]

    def rest_piece(block, h):
        cols = pl.ds(pl.multiple_of(block * width + part, 128), width - part)
        return used_rows.at[pl.ds(*chunks[h]), cols]

    def disp_copy(up, j, h):
        block = at_distance(up, j)
        ref = used_piece(block, h)
        if direct and j == n_tp - 2:
            ref = rest_piece(block, h)
        source = sel.at[slot, pl.ds(*chunks[h]), :] if j == 0 else ref
        return remote(
            source,
            ref,
            disp_send.at[up],
            disp_recv.at[block, h],
            "tp",
            at_distance(1 - up, 1),
        )

    def disp_wait(up, j, h):
        block = at_distance(up, j)
        ref = used_piece(block, h)
        if direct and j == n_tp - 1:
            ref = rest_piece(block, h)
        remote(
            ref, ref, disp_send.at[up], disp_recv.at[block, h], "tp", at_distance(up, 1)
        ).wait_recv()

    def far_copy(k, h, entry):
        return remote(
            sel.at[ret_slot(k), pl.ds(*chunks[h]), :],
            used_piece(tp, h),
            far_send.at[0],
            disp_recv.at[tp, h],
            "tp",
            entry,
        )

    def far_each(act, h):
        for k in range(1, n_exp):
            s = ret_slot(k)

            @pl.when(s > slot)
            def _():
                act(far_copy(k, h, s * split))

            @pl.when(s < slot)
            def _():
                act(far_copy(k, h, s * split + split - 1))

    def disp_start(h):
        for up in (0, 1):

            @pl.when(in_group(up))
            def _():
                disp_copy(up, 0, h).start()

    def disp_pass(j, h):
        for up in (0, 1):

            @pl.when(jnp.logical_and(known(up, j), in_group(up)))
            def _():
                disp_wait(up, j, h)
                if not (whole and j == n_tp - 2):
                    disp_copy(up, j, h).start()

    def disp_rest(h):
        for j in range(1, n_tp - 1 if whole else n_tp):
            for up in (0, 1):

                @pl.when(jnp.logical_and(known(up, j), jnp.logical_not(in_group(up))))
                def _():
                    disp_wait(up, j, h)

    def sum_rows(h):
        half = n_tok // 2
        return pl.ds(pl.multiple_of(h * half, half), half)

    def up_copy(d, h):
        rows = (d, sum_rows(h))
        return remote(
            parts.at[rows], in_up.at[rows], up_send.at[0], up_recv.at[d, h], "tp", tp + 1
        )

    def down_copy(d, h):
        rows = (d, sum_rows(h))
        return remote(
            parts.at[rows], in_down.at[rows], down_send.at[0], down_recv.at[d, h], "tp", tp - 1
        )

    def up_wait(d, h):
        ref = in_up.at[d, sum_rows(h)]
        remote(ref, ref, up_send.at[0], up_recv.at[d, h], "tp", tp - 1).wait_recv()

    def down_wait(d, h):
        ref = in_down.at[d, sum_rows(h)]
        remote(ref, ref, down_send.at[0], down_recv.at[d, h], "tp", tp + 1).wait_recv()

    def ret_copy(mask, k):
        rows = pl.ds(0, slot_most)
        return remote(
            stage.at[k, flip(ep, mask)],
            back.at[k, ep, rows, :],
            ret_send.at[k],
            ret_recv.at[k],
            "ep",
            flip(ep, mask),
        )

    def local_wait(ref, sem):
        pltpu.make_async_copy(ref, ref, sem).wait()

    def ret_wait(k):
        local_wait(back.at[k, pl.ds(0, n_ep - 1), pl.ds(0, slot_most), :], ret_recv.at[k])

    def near_copy(mask):
        return remote(
            near_out.at[flip(ep, mask)],
            near_in.at[ep],
            near_send.at[0],
            near_recv.at[0],
            "ep",
            flip(ep, mask),
        )

    def ids_copy(mask):
        return remote(
            ids_out.at[flip(ep, mask)],
            ids_in.at[ep],
            ids_send_sem.at[0],
            ids_recv_sem.at[0],
            "ep",
            flip(ep, mask),
        )

    def ids_wait():
        local_wait(ids_in.at[pl.ds(0, n_ep - 1)], ids_recv_sem.at[0])

    loads[0].wait()
    ep_start(0)
    for h in (0, 1):
        line_start(tok_copy, h)

    for load in loads[8:11]:
        load.wait()
    for s in range(n_exp):
        row = chosen_ref[pl.ds(s, 1), :]
        col = column_of(row.astype(f32), cap).astype(i32)
        chosen_col[s] = col
        gates_col[s] = column_of(gates_ref[pl.ds(s, 1), :], cap)
        row_from = jnp.zeros_like(row)
        col_from = jnp.zeros_like(col)
        for d in range(1, n_ep):
            row_from += jnp.where(row >= d * n_tok, 1, 0)
            col_from += jnp.where(col >= d * n_tok, 1, 0)
        before = jnp.where(col < row_from * n_tok, 1.0, 0.0)
        run_row = jnp.sum(before, axis=0, keepdims=True).astype(i32)
        before = jnp.where(row < col_from * n_tok, 1.0, 0.0)
        run_col = jnp.sum(before, axis=1, keepdims=True).astype(i32)
        lanes = lax.broadcasted_iota(i32, (1, cap), 1)
        rows = lax.broadcasted_iota(i32, (cap, 1), 0)
        place_row[s] = row_from * slot_most + lanes - run_row
        within = rows - run_col
        place_col[s] = col_from * slot_most + within

        def slot_ids(d, carry):
            slots = lax.broadcasted_iota(i32, (cap, slot_pad), 1)
            wanted = jnp.where(col_from == d, within, -1)
            value = (col - d * n_tok + 1).astype(f32)
            total = jnp.sum(jnp.where(slots == wanted, value, 0.0), axis=0, keepdims=True)
            ids_out[d, pl.ds(s, 1), :] = total.astype(i32) - 1
            return carry

        lax.fori_loop(0, n_ep, slot_ids, 0)

    def select(e):
        def one(s, carry):
            ids = lax.broadcasted_iota(i32, (cap, n_tok), 1) + e * n_tok
            hits = jnp.where(chosen_col[s] == ids, 1.0, 0.0).astype(bf16)
            acc[s] += jnp.dot(hits, tok_all[e], preferred_element_type=f32)
            return carry

        lax.fori_loop(0, n_exp, one, 0)

    ep_masks = sorted(range(1, n_ep), key=lambda m: -bin(m >> 1).count("1"))
    for mask in ep_masks:
        ids_copy(mask).start()
    ids_in[ep] = ids_out[ep]
    select(ep)
    if n_tp > 2:
        tok_pass(1, 0)
    def pick(k):
        for e in range(n_ep):
            ids = ids_in[e, pl.ds(ret_slot(k), 1), :]
            match = lax.broadcasted_iota(i32, (n_tok, slot_pad), 0) == ids
            picker[k, :, e * slot_pad : (e + 1) * slot_pad] = jnp.where(match, 1.0, 0.0).astype(bf16)

    ids_wait()
    pick(0)
    ep_level(0, ep_levels[0])
    for load in loads[1:4]:
        load.wait()
    ep_start(1)
    held = at_end if direct else tp < 0

    ep_start(2)

    @pl.when(jnp.logical_not(held))
    def _():
        ep_start(3)

    if n_tp > 2:
        tok_pass(1, 1)
    for mask in ep_levels[0]:
        select(flip(ep, mask))
    if n_tp > 3:
        tok_pass(2, 0)
    for masks in ep_levels[1:]:
        for mask in sorted(masks, key=lambda m: -(m % 2)):
            ep_level(0, [mask])
            select(flip(ep, mask))
    for s in range(n_exp):
        sel[s] = acc[s].astype(bf16)
    if n_tp > 3:
        tok_pass(2, 1)
    far_each(lambda copy: copy.start(), 0)
    own_used = pltpu.make_async_copy(sel.at[slot], columns(used_rows, tp), local_sem.at[8])
    own_used.start()
    acc[...] = jnp.zeros_like(acc)
    for j in range(3, n_tp - 1):
        for h in (0, 1):
            tok_pass(j, h)
    ep_level(1, ep_levels[0])

    far_each(lambda copy: copy.start(), 1)
    for h in parts_of:
        disp_start(h)
    for j in range(1, n_tp):
        disp_pass(j, 0)
    if direct:

        @pl.when(at_end)
        def _():
            for h in (0, 1):
                tok_pass(n_tp - 1, h)
            cols = pl.ds(pl.multiple_of(far_end * width, width), part)
            rows = lax.dot_general(
                picker[0], own_rows[:, cols], (((0,), (0,)), ((), ())), preferred_element_type=f32
            )
            near_out[...] = rows.reshape(n_ep, slot_pad, part)[:, :slot_most, :].astype(bf16)
            for mask in ep_masks:
                near_copy(mask).start()
            near_in[ep] = near_out[ep]


    @pl.when(held)
    def _():
        ep_start(3)

    ep_level(2, ep_levels[0])
    for j in range(1, n_tp):
        disp_pass(j, 1)
    for k in range(1, n_exp):
        pick(k)
    @pl.when(jnp.logical_not(held))
    def _():
        ep_level(3, ep_levels[0])

    if direct:

        @pl.when(at_end)
        def _():
            local_wait(near_in.at[pl.ds(0, n_ep - 1)], near_recv.at[0])
            slots = n_ep * slot_most
            match = lax.broadcasted_iota(i32, (cap, slots), 1) == place_col[slot]
            rows = jnp.dot(
                jnp.where(match, 1.0, 0.0).astype(bf16),
                near_in[...].reshape(slots, part),
                preferred_element_type=f32,
            )
            cols = pl.ds(pl.multiple_of(far_end * width, width), part)
            used_rows[:, cols] = rows.astype(bf16)

    own_used.wait()
    loads[5].wait()
    loads[6].wait()
    for h in parts_of:
        disp_rest(h)
        used = normalise(used_rows[pl.ds(*chunks[h]), :], gain_ref[...])
        contract = (((1,), (1,)), ((), ()))
        gate = lax.dot_general(eg_ref[...], used, contract, preferred_element_type=f32)
        up = lax.dot_general(eu_ref[...], used, contract, preferred_element_type=f32)
        hidden[tp, :, pl.ds(*chunks[h])] = (jax.nn.silu(gate) * up).astype(bf16)
        line_start(hid_copy, h)
    loads[4].wait()
    if not direct:
        for h in (0, 1):
            tok_pass(n_tp - 1, h)
    def norm_rows(i, carry):
        rows = sum_rows(i)
        normed[rows, :] = normalise(own_rows[rows, :], gain_ref[...])
        return carry

    lax.fori_loop(0, 2, norm_rows, 0)
    @pl.when(held)
    def _():
        ep_level(3, ep_levels[0])

    for masks in ep_levels[1:]:
        for w in (1, 2):
            ep_level(w, masks)
    def join(k):
        if not flat:
            return (sg_in, su_in, sd_in)[k]
        group = 128 // sg_hbm.shape[1]
        blocks, out = (sg_in, su_in, sd_in)[k], flat[k]
        for j in range(n_ep // group):
            joined = jnp.concatenate([blocks[j * group + i] for i in range(group)], axis=1)
            out[:, j * 128 : (j + 1) * 128] = joined
        return out

    sg_ref, su_ref = join(0), join(1)

    def shared_up(i, carry):
        rows = sum_rows(i)
        x = normed[rows, :]
        contract = (((1,), (1,)), ((), ()))
        gate = lax.dot_general(x, sg_ref[...], contract, preferred_element_type=f32)
        up = lax.dot_general(x, su_ref[...], contract, preferred_element_type=f32)
        mid_ref[rows, :] = (jax.nn.silu(gate) * up).astype(bf16)
        return carry

    lax.fori_loop(0, 2, shared_up, 0)
    for masks in ep_levels[1:]:
        ep_level(3, masks)
    sd_ref = join(2)

    def sums_first(h):
        @pl.when(tp == 0)
        def _():
            up_copy(n_tp - 1, h).start()

        @pl.when(tp == n_tp - 1)
        def _():
            down_copy(0, h).start()


    def shared_rows(i, carry):
        rows = sum_rows(i)
        mid = mid_ref[rows, :]
        for block in range(n_tp):
            cols = pl.ds(block * width, width)
            parts[block, rows, :] = jnp.dot(
                mid, sd_ref[:, cols], preferred_element_type=f32
            ).astype(bf16)
        sums_first(i)
        return carry

    lax.fori_loop(0, 2, shared_rows, 0)

    def sums_ends(j):
        @pl.when(tp == 0)
        def _():
            for h in (0, 1):
                up_copy(n_tp - 1 - j, h).start()

        @pl.when(tp == n_tp - 1)
        def _():
            for h in (0, 1):
                down_copy(j, h).start()

    def sums_up(j, h):
        d = n_tp - 1 - j

        @pl.when(jnp.logical_and(tp > 0, tp < d))
        def _():
            rows = sum_rows(h)
            up_wait(d, h)
            parts[d, rows] = (parts[d, rows].astype(f32) + in_up[d, rows].astype(f32)).astype(bf16)
            up_copy(d, h).start()

    def sums_down(j, h):
        @pl.when(jnp.logical_and(tp < n_tp - 1, tp > j))
        def _():
            rows = sum_rows(h)
            down_wait(j, h)
            parts[j, rows] = (parts[j, rows].astype(f32) + in_down[j, rows].astype(f32)).astype(bf16)
            down_copy(j, h).start()

    def sums_outer(j, h):
        @pl.when(tp < n_tp // 2)
        def _():
            sums_up(j, h)

        @pl.when(tp >= n_tp // 2)
        def _():
            sums_down(j, h)

    def sums_inner(j, h):
        @pl.when(tp < n_tp // 2)
        def _():
            sums_down(j, h)

        @pl.when(tp >= n_tp // 2)
        def _():
            sums_up(j, h)

    def add_block(mask, h):
        block = flip(tp, mask)
        rows = pl.ds(*chunks[h])
        acc[block // split, rows, :] += lax.dot_general(
            hidden[block, :, rows],
            down_ref[block],
            (((0,), (0,)), ((), ())),
            preferred_element_type=f32,
        )

    def give_back(k):
        s = ret_slot(k)
        weighted = (gates_col[s] * acc[s]).astype(bf16)
        slots = n_ep * slot_most
        placer = lax.broadcasted_iota(i32, (slots, cap), 0) == place_row[s]
        placer = jnp.where(placer, 1.0, 0.0).astype(bf16)
        placed = jnp.dot(placer, weighted, preferred_element_type=f32)
        stage[k] = placed.reshape(n_ep, slot_most, width).astype(bf16)
        for mask in ep_masks:
            ret_copy(mask, k).start()
        back[k, ep, :slot_most, :] = stage[k, ep]

    loads[7].wait()
    for h in parts_of:
        add_block(0, h)
    for h in parts_of:
        hid_pass(1, 0, h)
    for h in parts_of:
        hid_pass(1, 1, h)
    for j in range(1, n_tp):
        if j > 1:
            for h in parts_of:
                hid_pass(j, 0, h)
                hid_pass(j, 1, h)
                add_block(j, h)
        if j == 1:
            for h in parts_of:
                add_block(j, h)
        if (j + 1) % split == 0:
            give_back(j // split)
        if j > 1:
            for h in (0, 1):
                sums_outer(j - 2, h)
                if j > 2:
                    sums_inner(j - 3, h)
        if j < n_tp - 1:
            sums_ends(j)
    for j in (n_tp - 3, n_tp - 2):
        for h in (0, 1):
            if j == n_tp - 2:
                sums_outer(j, h)
            sums_inner(j, h)
    acc[0] = parts[tp].astype(f32)

    @pl.when(tp > 0)
    def _():
        for h in (0, 1):
            up_wait(tp, h)
        acc[0] += in_up[tp].astype(f32)

    @pl.when(tp < n_tp - 1)
    def _():
        for h in (0, 1):
            down_wait(tp, h)
        acc[0] += in_down[tp].astype(f32)

    for k in range(n_exp):
        ret_wait(k)
        for h in (0, 1):
            rows = sum_rows(h)
            value = acc[0, rows, :] + jnp.dot(
                picker[k, rows, :],
                back[k].reshape(n_ep * slot_pad, width),
                preferred_element_type=f32,
            )
            if k < n_exp - 1:
                acc[0, rows, :] = value
            else:
                out_ref[rows, :] = value.astype(bf16)
                result = pltpu.make_async_copy(
                    out_ref.at[rows, :], out_hbm.at[rows, :], local_sem.at[8 + h]
                )
                result.start()

    for w in range(4):
        if w == 0 or len(sg_in.shape) == 3:
            sent = [tok_all, sg_in, su_in, sd_in][w].at[pl.ds(0, n_ep - 1)]
        else:
            cols = sg_hbm.shape[1] * (n_ep - 1)
            sent = [None, sg_in, su_in, sd_in][w].at[:, pl.ds(0, cols)]
        local_wait(sent, ep_send.at[w])
    local_wait(sel.at[pl.ds(0, n_exp - 1)], far_send.at[0])
    if direct:

        @pl.when(at_end)
        def _():
            local_wait(near_out.at[pl.ds(0, n_ep - 1)], near_send.at[0])

    local_wait(ids_out.at[pl.ds(0, n_ep - 1)], ids_send_sem.at[0])
    for k in range(n_exp):
        local_wait(stage.at[k, pl.ds(0, n_ep - 1)], ret_send.at[k])
    for place in range(n_tp):
        for up in (0, 1):
            blocks = place + 1 if up else n_tp - place
            last = n_tp - 1 if up else 0
            if place != last:

                @pl.when(tp == place)
                def _():
                    local_wait(own_rows.at[:, pl.ds(0, blocks * width)], tp_send.at[up])
                    local_wait(hidden.at[pl.ds(0, blocks)], hid_send.at[up])
                    sums = up_send if up else down_send
                    local_wait(parts.at[pl.ds(0, n_tp - blocks)], sums.at[0])

            edge = place % split == (split - 1 if up else 0)
            if not edge:

                @pl.when(tp == place)
                def _():
                    sent = blocks * width
                    if direct and place == (n_tp - 2 if up else 1):
                        sent = sent - part
                    local_wait(used_rows.at[:, pl.ds(0, sent)], disp_send.at[up])

    for h in (0, 1):
        rows = sum_rows(h)
        pltpu.make_async_copy(
            out_ref.at[rows, :], out_hbm.at[rows, :], local_sem.at[8 + h]
        ).wait()


def on_device(
    tokens,
    norm_gain,
    shared_gate,
    shared_up,
    shared_down,
    expert_gate,
    expert_up,
    expert_down,
    chosen,
    gates,
):
    n_tp = lax.axis_size("tp")
    n_ep = lax.axis_size("ep")
    n_exp, cap = chosen.shape
    n_tok, width = tokens.shape
    model = n_tp * width
    bf16, f32, i32 = jnp.bfloat16, jnp.float32, jnp.int32
    slot_most = 2 * cap // n_ep
    slot_pad = -(-slot_most // 128) * 128
    n_hid = expert_gate.shape[2]
    near = width
    sg, su, sd = shared_gate.T, shared_up.T, shared_down
    rows, cols = sg.shape
    if cols % 128 == 0:
        joined, flat = (rows, n_ep * cols), []
    else:
        joined = (n_ep, rows, cols)
        flat = [pltpu.VMEM((rows, n_ep * cols), bf16)] * 3
    hbm = pl.BlockSpec(memory_space=pltpu.HBM)
    anywhere = pl.BlockSpec(memory_space=pl.ANY)
    dma = pltpu.SemaphoreType.DMA
    return pl.pallas_call(
        functools.partial(layer_kernel, n_tp, n_ep, slot_most),
        out_shape=jax.ShapeDtypeStruct((n_tok, width), bf16),
        in_specs=[hbm] * 10,
        out_specs=anywhere,
        scratch_shapes=[
            pltpu.VMEM((n_tok, width), bf16),
            pltpu.VMEM((1, model), f32),
            pltpu.VMEM(chosen.shape, i32),
            pltpu.VMEM(gates.shape, f32),
            pltpu.VMEM((n_ep, n_tok, width), bf16),
            pltpu.VMEM((n_tok, model), bf16),
            pltpu.VMEM((cap, model), bf16),
            pltpu.VMEM((n_exp, cap, width), bf16),
            pltpu.VMEM(joined, bf16),
            pltpu.VMEM(joined, bf16),
            pltpu.VMEM(joined, bf16),
            pltpu.VMEM((n_hid, model), bf16),
            pltpu.VMEM((n_hid, model), bf16),
            pltpu.VMEM((n_tp, n_hid, width), bf16),
            pltpu.VMEM((n_tp, n_hid, cap), bf16),
            pltpu.VMEM((n_exp, cap, width), f32),
            pltpu.VMEM((n_tp, n_tok, width), bf16),
            pltpu.VMEM((n_tp, n_tok, width), bf16),
            pltpu.VMEM((n_tp, n_tok, width), bf16),
            pltpu.VMEM((n_exp, n_ep, slot_most, width), bf16),
            pltpu.VMEM((n_exp, n_ep, slot_pad, width), bf16),
            pltpu.VMEM((n_exp, n_tok, n_ep * slot_pad), bf16),
            pltpu.VMEM((n_ep, 8, slot_pad), i32),
            pltpu.VMEM((n_ep, 8, slot_pad), i32),
            pltpu.VMEM((n_exp, cap, 1), i32),
            pltpu.VMEM((n_exp, cap, 1), f32),
            pltpu.VMEM((n_exp, 1, cap), i32),
            pltpu.VMEM((n_exp, cap, 1), i32),
            pltpu.VMEM((n_ep, slot_most, near), bf16),
            pltpu.VMEM((n_ep, slot_most, near), bf16),
            pltpu.VMEM((n_tok, model), bf16),
            pltpu.VMEM((n_tok, rows), bf16),
            dma((4,)),
            dma((4, 2, n_ep - 1)),
            dma((2,)),
            dma((2, n_tp - 1, 2)),
            dma((2,)),
            dma((n_tp, 2)),
            dma((1,)),
            dma((2,)),
            dma((2, n_tp - 1, 2)),
            dma((1,)),
            dma((n_tp, 2)),
            dma((1,)),
            dma((n_tp, 2)),
            dma((n_exp,)),
            dma((n_exp,)),
            dma((1,)),
            dma((1,)),
            dma((1,)),
            dma((1,)),
            dma((13,)),
        ]
        + flat,
        compiler_params=pltpu.CompilerParams(
            collective_id=0, has_side_effects=True, vmem_limit_bytes=62 * 1024 * 1024
        ),
    )(
        tokens,
        norm_gain.reshape(1, -1),
        sg,
        su,
        sd,
        expert_gate.reshape(n_hid, model),
        expert_up.reshape(n_hid, model),
        expert_down.reshape(n_tp, n_hid, width),
        chosen,
        gates,
    )


def solution(mesh):
    return jax.shard_map(
        on_device,
        mesh=mesh,
        in_specs=(
            P("ep", "tp"),
            P(),
            P("ep", "tp"),
            P("ep", "tp"),
            P("tp", "ep"),
            P("tp", "ep", None, None),
            P("tp", "ep", None, None),
            P("ep", None, "tp"),
            P("ep", None),
            P("ep", None),
        ),
        out_specs=P("ep", "tp"),
        check_vma=False,
    )
```
